256 devices in a mesh: tm: 32 (over z_hi, x, core), space: 8 (over y, z_lo).
Axes of the slice: x: 4, y: 4, z: 8 (z_hi: 4, z_lo: 2; z = z_hi * 2 + z_lo), core: 2. Of those that a mesh axis runs over, the one named last changes fastest.
Arguments:
- fine_nodes: float32 [32, 3, 3, 128, 4096], P('tm', None, None, 'space'), may hold values from -6 to 6
- init_state: float32 [3, 128, 4096], P(None, 'space'), may hold values from -6 to 6
- mean_depth: float32 [128, 4096], P('space'), may hold values from 0.5 to 2
Outputs:
- new_nodes: float32 [32, 3, 3, 128, 4096], P('tm', None, None, 'space')
The draws below stay inside these ranges and needn't reach their ends.
All inputs are finite; a program needn't handle non-finite values.
Results may differ from the reference program's by a relative error of at most 0.00002.
Values sent between devices are 32-bit elements; how exact they have to be, the bound alone decides.
A program may use at most 64 MiB of HBM per device.

```python
import math
import jax
import jax.numpy as jnp
from jax import lax

NX = 4096
NODES = 3
FIELDS = 3
NY = 128
SLICES = 32


def steps_of(rng, shape, pieces, least, largest):
    level, own = 1.0, jax.random.fold_in(rng, 6)
    for position, parts in pieces:
        heights = jnp.exp(jax.random.uniform(jax.random.fold_in(own, position), (parts,), jnp.float32, least / len(pieces), largest / len(pieces)))
        level = level * jnp.repeat(heights, shape[position] // parts).reshape([-1 if axis == position else 1 for axis in range(len(shape))])
    return level


def noise(key, extent, scale, limit, split=(), held_as=jnp.bfloat16):
    array = scale * jax.random.normal(key, extent, jnp.float32)
    if split:
        array = array * steps_of(key, extent, split, -0.22, 0.18)
    return jnp.clip(array, -limit, limit).astype(held_as)


def setup_inputs(seed: int = 0) -> dict:
    seeds = jax.random.split(jax.random.key(seed), 4)
    return {
        "fine_nodes": noise(seeds[0], (SLICES, NODES, FIELDS, NY, NX), 1.0, 6.0, ((0, 32), (3, 8)), jnp.float32),
        "init_state": noise(seeds[1], (FIELDS, NY, NX), 1.0, 6.0, ((1, 8),), jnp.float32),
        "mean_depth": jnp.clip(jnp.exp(math.log(2.0) - 1.3862944 * jax.random.uniform(seeds[2], (NY, NX), jnp.float32) ** steps_of(seeds[2], (NY, NX), ((0, 8),), -0.2, 0.2)), 0.5, 2.0),
    }


step_size = 0.3
viscosity = 1.0 / 3.0
coriolis = 0.5
quad_near = 5.0 / 24.0
quad_mid = 1.0 / 3.0
quad_far = -1.0 / 24.0


def column_slope(values):
    return (jnp.roll(values, -1, -1) - jnp.roll(values, 1, -1)) * 0.5


def row_slope(values):
    return (values[..., 2:, :] - values[..., :-2, :]) * 0.5


def diffuse(values, centre):
    return values[..., 2:, :] + values[..., :-2, :] + jnp.roll(centre, -1, -1) + jnp.roll(centre, 1, -1) - 4.0 * centre


def tendency(padded, depth_rows):
    height = padded[..., 0, :, :]
    east_flow = padded[..., 1, :, :]
    north_flow = padded[..., 2, :, :]
    centre = padded[..., 1:-1, :]
    height_c = centre[..., 0, :, :]
    east_c = centre[..., 1, :, :]
    north_c = centre[..., 2, :, :]
    depth_c = depth_rows[1:-1]
    height_rate = -column_slope(depth_c * east_c) - row_slope(depth_rows * north_flow) + viscosity * diffuse(height, height_c)
    east_rate = -column_slope(height_c) + coriolis * north_c + viscosity * diffuse(east_flow, east_c)
    north_rate = -row_slope(height) - coriolis * east_c + viscosity * diffuse(north_flow, north_c)
    return jnp.stack([height_rate, east_rate, north_rate], axis=-3)


def padded_rows(values):
    return jnp.concatenate([values[..., -1:, :], values, values[..., :1, :]], axis=-2)


def full_rate(values, mean_depth):
    return tendency(padded_rows(values), padded_rows(mean_depth))


def reference(fine_nodes, init_state, mean_depth):
    half_step = step_size * 0.5
    starts = jnp.concatenate([init_state[None], fine_nodes[:-1, 2]], axis=0)
    first_flags = jnp.arange(fine_nodes.shape[0], dtype=jnp.int32) == 0

    def slice_work(slice_items):
        points, section_zero, is_first = slice_items
        old_rates = full_rate(points, mean_depth)
        rate_zero = full_rate(section_zero, mean_depth)
        section_one = section_zero + half_step * (rate_zero - old_rates[0]) + step_size * (quad_near * old_rates[0] + quad_mid * old_rates[1] + quad_far * old_rates[2])
        rate_one = full_rate(section_one, mean_depth)
        section_two = section_one + half_step * (rate_one - old_rates[1]) + step_size * (quad_far * old_rates[0] + quad_mid * old_rates[1] + quad_near * old_rates[2])
        rate_two = full_rate(section_two, mean_depth)
        fas_term = -(step_size / 3.0) * (rate_zero - 2.0 * rate_one + rate_two)
        drift_total = half_step * (rate_two - rate_zero) + fas_term
        boosted = drift_total + jnp.where(is_first, section_zero + step_size * rate_zero, 0.0)
        return section_one, section_two, boosted

    section_ones, section_twos, boosts = lax.map(slice_work, (fine_nodes, starts, first_flags))

    def chain_turn(current, boosted):
        updated = boosted + (current + step_size * full_rate(current, mean_depth))
        return updated, updated

    _, coarse_end = lax.scan(chain_turn, jnp.zeros_like(init_state), boosts)
    coarse_begin = jnp.concatenate([init_state[None], coarse_end[:-1]], axis=0)
    middle = section_ones + 0.5 * ((coarse_begin - starts) + (coarse_end - section_twos))
    return jnp.stack([coarse_begin, middle, coarse_end], axis=1)
```

```python
import functools

import jax
import jax.numpy as jnp
from jax import lax
from jax.experimental import pallas as pl
from jax.experimental.pallas import tpu as pltpu
from jax.sharding import PartitionSpec as P

MESH = pl.DeviceIdType.MESH
F32 = jnp.float32

step_size = 0.3
viscosity = 1.0 / 3.0
coriolis = 0.5
quad_near = 5.0 / 24.0
quad_mid = 1.0 / 3.0
quad_far = -1.0 / 24.0
half_step = 0.5 * step_size

ROWS = 16
COLS = 4096
SPACE = 8
CHIPS = 16
PART = 256
OWN = 16
HALO = 32
WIDE = OWN + 2 * HALO


def rates(h, u, v, de, dn, left, right, up, down, centre):
    nh, nu, nv = viscosity * h, viscosity * u, viscosity * v
    he, hn, hh = 0.5 * de, 0.5 * dn, 0.5 * h
    nhc, nuc, nvc = centre(nh), centre(nu), centre(nv)
    hr = right(nh - he) + left(nh + he) + down(centre(nh - hn)) + up(centre(nh + hn)) - 4.0 * nhc
    ur = right(nu - hh) + left(nu + hh) + down(nuc) + up(nuc) - 4.0 * nuc + coriolis * centre(v)
    vr = right(nv) + left(nv) + down(centre(nv - hh)) + up(centre(nv + hh)) - 4.0 * nvc - coriolis * centre(u)
    return hr, ur, vr


CHUNK = 512


def fine_kernel(fine, fine_halo, start, start_halo, depth, depth_halo, item, boosted, partial, g1, g2, s1, acc, bst):
    slot = lax.axis_index("tm")
    first = jnp.where(slot == 0, 1.0, 0.0).astype(F32)
    even = jnp.where(lax.rem(slot, 2) == 0, step_size, 0.0).astype(F32)

    def ring(main, halo, idx, cols):
        return jnp.concatenate([main[idx + (slice(None), cols)], halo[idx + (slice(None), cols)]], axis=0)

    def edges(base):
        lo = pl.multiple_of(lax.rem(base + COLS - 128, COLS), 128)
        hi = pl.multiple_of(lax.rem(base + CHUNK, COLS), 128)
        return pl.ds(lo, 128), pl.ds(base, CHUNK), pl.ds(hi, 128)

    def wide(get, base):
        return jnp.concatenate([get(c) for c in edges(base)], axis=1)

    n = CHUNK + 256

    def right(x):
        return pltpu.roll(x, n - 1, 1)[:, 128 : 128 + CHUNK]

    def left(x):
        return pltpu.roll(x, 1, 1)[:, 128 : 128 + CHUNK]

    def down(x):
        return pltpu.roll(x, 23, 0)

    def up(x):
        return pltpu.roll(x, 1, 0)

    def centre(x):
        return x[:, 128 : 128 + CHUNK]

    def rate(get, base):
        h, u, v = (wide(functools.partial(get, f), base) for f in range(3))
        d = wide(lambda c: ring(depth, depth_halo, (), c), base)
        return rates(h, u, v, d * u, d * v, left, right, up, down, centre)

    def loop(body):
        @pl.loop(0, COLS // CHUNK)
        def _(i):
            body(pl.multiple_of(i * CHUNK, CHUNK))

    def old(base):
        cols = pl.ds(base, CHUNK)
        r = [rate(lambda f, c, m=m: ring(fine, fine_halo, (3 * m + f,), c), base) for m in range(3)]
        for f in range(3):
            near, mid, far = r[0][f], r[1][f], r[2][f]
            g1[f, :, cols] = step_size * (quad_near * near + quad_mid * mid + quad_far * far) - half_step * near
            g2[f, :, cols] = step_size * (quad_far * near + quad_mid * mid + quad_near * far) - half_step * mid

    loop(old)

    def zero(base):
        cols = pl.ds(base, CHUNK)
        r = rate(lambda f, c: ring(start, start_halo, (f,), c), base)
        for f in range(3):
            sz = ring(start, start_halo, (f,), cols)
            s1[f, :, cols] = sz + half_step * r[f] + g1[f, :, cols]
            acc[f, :, cols] = first * (sz + step_size * r[f]) - (half_step + step_size / 3.0) * r[f]

    loop(zero)

    def one(base):
        cols = pl.ds(base, CHUNK)
        r = rate(lambda f, c: s1[f, :, c], base)
        for f in range(3):
            g2[f, :, cols] = s1[f, :, cols] + half_step * r[f] + g2[f, :, cols]
            acc[f, :, cols] += (2.0 * step_size / 3.0) * r[f]

    loop(one)

    def two(base):
        cols = pl.ds(base, CHUNK)
        r = rate(lambda f, c: g2[f, :, c], base)
        for f in range(3):
            b = acc[f, :, cols] + (half_step - step_size / 3.0) * r[f]
            bst[f, :, cols] = b
            boosted[f, :, cols] = b[:ROWS]
            partial[f, :, cols] = s1[f, :ROWS, cols] - 0.5 * (start[f, :, cols] + g2[f, :ROWS, cols])

    loop(two)

    def push(base):
        cols = pl.ds(base, CHUNK)
        r = rate(lambda f, c: bst[f, :, c], base)
        for f in range(3):
            item[f, :, cols] = boosted[f, :, cols] + even * r[f][:ROWS]

    loop(push)


def ring_place(k, chip):
    z, x = chip // 4, lax.rem(chip, 4)
    r = z * 4 + jnp.where(lax.rem(z, 2) == 0, x, 3 - x)
    return jnp.where(k == 0, r, CHIPS - 1 - r)


def ring_chip(k, r):
    r = jnp.where(k == 0, r, CHIPS - 1 - r)
    z, x = r // 4, lax.rem(r, 4)
    return z * 4 + jnp.where(lax.rem(z, 2) == 0, x, 3 - x)


def coarse_kernel(
    item, boosted, depth, esum, other, vout, ritem, rt, et, dr, dt, ex, vx, vt, vr,
    pair_s, pair_r, one_s, one_r, dep_s, dep_r, two_s, two_r, halo_s, halo_r,
    ret_s, ret_r, row_s, row_r, fin_s, fin_r,
):
    tm = lax.axis_index("tm")
    s = lax.axis_index("space")
    chip, k = tm // 2, lax.rem(tm, 2)
    place = ring_place(k, chip)
    q = (s * 2 + k) * CHIPS + place
    partner = {"tm": chip * 2 + 1 - k, "space": s}

    def at(c, sp):
        return {"tm": c * 2 + k, "space": sp}

    def near(step):
        p = lax.rem(q + step + 256, 256)
        kk = lax.rem(p // CHIPS, 2)
        return {"tm": ring_chip(kk, lax.rem(p, CHIPS)) * 2 + kk, "space": p // 32}

    rows_of = [at(chip, lax.rem(s + d, SPACE)) for d in range(1, SPACE)]
    chips_of = [at(lax.rem(chip + d, CHIPS), s) for d in range(1, CHIPS)]
    rings = [near(1), near(-1), near(2), near(-2)]
    vt[...] = jnp.zeros_like(vt)
    barrier = pltpu.get_barrier_semaphore()
    peers = [partner] + rows_of + chips_of + rings
    for p in peers:
        pl.semaphore_signal(barrier, inc=1, device_id=p, device_id_type=MESH)
    pl.semaphore_wait(barrier, len(peers))

    def copy(src, dst, ss, rs, dev):
        return pltpu.make_async_remote_copy(src_ref=src, dst_ref=dst, send_sem=ss, recv_sem=rs, device_id=dev, device_id_type=MESH)

    def block(sp, kk=None):
        return pl.ds(pl.multiple_of(512 * sp + 256 * (k if kk is None else kk), PART), PART)

    def rows(sp, n=ROWS):
        return pl.ds(pl.multiple_of(sp, 8), n)

    pair = [copy(item, ritem, pair_s.at[0], pair_r.at[0], partner), copy(boosted, other, pair_s.at[1], pair_r.at[1], partner)]
    for c in pair:
        c.start()

    def depth_parts(sp):
        base = 512 * sp + 256 * k
        return (
            (pl.ds(pl.multiple_of(base, 128), PART), pl.ds(128, PART)),
            (pl.ds(pl.multiple_of(lax.rem(base + COLS - 128, COLS), 128), 128), pl.ds(0, 128)),
            (pl.ds(pl.multiple_of(lax.rem(base + PART, COLS), 128), 128), pl.ds(384, 128)),
        )

    def depth_copy(d, n, send):
        sp = lax.rem(s + d, SPACE) if send else lax.rem(s + SPACE - d, SPACE)
        src, dst = depth_parts(sp if send else s)[n]
        return copy(depth.at[:, src], dr.at[rows(ROWS * (s if send else sp)), dst], dep_s.at[n, d], dep_r.at[n, d], at(chip, sp))

    for d in range(1, SPACE):
        for n in range(3):
            depth_copy(d, n, True).start()
    for src, dst in depth_parts(s):
        dr[rows(ROWS * s), dst] = depth[:, src]

    pair[0].wait_recv()
    for f in range(3):
        esum[f] = item[f] + ritem[f]

    def one_copy(d, send):
        sp = lax.rem(s + d, SPACE) if send else lax.rem(s + SPACE - d, SPACE)
        return copy(
            esum.at[:, :, block(sp if send else s)], rt.at[:, rows(ROWS * (s if send else sp)), :], one_s.at[d], one_r.at[d], at(chip, sp)
        )

    for d in range(1, SPACE):
        one_copy(d, True).start()
    rt[:, rows(ROWS * s), :] = esum[:, :, block(s)]

    for d in range(1, SPACE):
        for n in range(3):
            depth_copy(d, n, False).wait_recv()
    for t in range(4):
        dt[128 * t : 128 * t + 128, :] = dr[:, 128 * t : 128 * t + 128].T

    for d in range(1, SPACE):
        one_copy(d, False).wait_recv()
    for f in range(3):
        for t in range(2):
            et[f, 128 * t : 128 * t + 128, :] = rt[f, :, 128 * t : 128 * t + 128].T

    def two_copy(d, send):
        c = lax.rem(chip + d, CHIPS) if send else lax.rem(chip + CHIPS - d, CHIPS)
        src = et.at[:, rows(OWN * (ring_place(k, c) if send else place), OWN), :]
        return copy(src, ex.at[chip if send else c, :, pl.ds(HALO, OWN), :], two_s.at[d], two_r.at[d], at(c, s))

    for d in range(1, CHIPS):
        two_copy(d, True).start()
    ex[chip, :, HALO : HALO + OWN, :] = et[:, rows(OWN * place, OWN), :]
    for d in range(1, CHIPS):
        two_copy(d, False).wait_recv()

    halos = []
    for hop, lo, hi, width in ((1, 0, 10, 16), (1, 10, 14, 8), (2, 0, 2, 16), (2, 2, 6, 8)):
        far = OWN * (hop - 1)
        halos.append((lo, hi, HALO + OWN - width, HALO - far - width, width, hop))
        halos.append((lo, hi, HALO, HALO + OWN + far, width, -hop))

    def halo_copy(i):
        lo, hi, src, dst, width, hop = halos[i]
        to = rings[{1: 0, -1: 1, 2: 2, -2: 3}[hop]]
        return copy(ex.at[lo:hi, :, pl.ds(src, width), :], ex.at[lo:hi, :, pl.ds(dst, width), :], halo_s.at[i], halo_r.at[i], to)

    for i in range(len(halos)):
        halo_copy(i).start()
    for i in range(len(halos)):
        halo_copy(i).wait_recv()

    d_own = dt[rows(96 + OWN * place, WIDE), :]

    def same(x):
        return x

    def stepped(state):
        h, u, v = state
        r = rates(
            h, u, v, d_own * u, d_own * v,
            lambda x: pltpu.roll(x, 1, 0), lambda x: pltpu.roll(x, WIDE - 1, 0),
            lambda x: pltpu.roll(x, 1, 1), lambda x: pltpu.roll(x, 127, 1), same,
        )
        return tuple(x + step_size * y for x, y in zip(state, r))

    def ret_copy(j):
        return copy(vx.at[j], vt.at[:, rows(OWN * place, OWN), :], ret_s.at[j], ret_r.at[chip], at(j, s))

    def body(j, state):
        state = stepped(stepped(state))
        state = tuple(x + ex[j, f] for f, x in enumerate(state))
        for f in range(3):
            vx[j + 1, f] = state[f][HALO : HALO + OWN]

        @pl.when(chip != j + 1)
        def _():
            ret_copy(j + 1).start()

        return state

    empty = jnp.zeros((WIDE, 128), F32)
    lax.fori_loop(0, CHIPS - 1, body, (empty, empty, empty))

    @pl.when(chip > 0)
    def _():
        vt[:, rows(OWN * place, OWN), :] = vx[chip]
        for d in range(1, CHIPS):
            c = lax.rem(chip + CHIPS - d, CHIPS)
            dst = vt.at[:, rows(OWN * ring_place(k, c), OWN), :]
            copy(vx.at[0], dst, ret_s.at[0], ret_r.at[c], at(c, s)).wait_recv()

    for f in range(3):
        for t in range(2):
            vr[f, :, 128 * t : 128 * t + 128] = vt[f, 128 * t : 128 * t + 128, :].T

    def row_parts(sp):
        return (
            (rows(ROWS * sp), pl.ds(0, 16)),
            (rows(lax.rem(ROWS * sp + 16, 128), 8), pl.ds(16, 8)),
            (rows(lax.rem(ROWS * sp + 120, 128), 8), pl.ds(24, 8)),
        )

    def row_copy(d, n, send):
        sp = lax.rem(s + d, SPACE) if send else lax.rem(s + SPACE - d, SPACE)
        src, dst = row_parts(sp if send else s)[n]
        return copy(vr.at[:, src, :], vout.at[:, dst, block(s if send else sp)], row_s.at[n, d], row_r.at[n, d], at(chip, sp))

    for d in range(1, SPACE):
        for n in range(3):
            row_copy(d, n, True).start()
    for src, dst in row_parts(s):
        vout[:, dst, block(s)] = vr[:, src, :]

    def fin_copy(d, send):
        cols = block(lax.rem(s + SPACE - d, SPACE), k if send else 1 - k)
        return copy(vout.at[:, :, cols], vout.at[:, :, cols], fin_s.at[d], fin_r.at[d], partner)

    fin_copy(0, True).start()
    for d in range(1, SPACE):
        for n in range(3):
            row_copy(d, n, False).wait_recv()
        fin_copy(d, True).start()
    pair[1].wait_recv()
    for d in range(SPACE):
        fin_copy(d, False).wait_recv()

    for c in pair:
        c.wait_send()
    for d in range(1, SPACE):
        for n in range(3):
            depth_copy(d, n, True).wait_send()
            row_copy(d, n, True).wait_send()
        one_copy(d, True).wait_send()
    for d in range(1, CHIPS):
        two_copy(d, True).wait_send()
    for i in range(len(halos)):
        halo_copy(i).wait_send()
    for d in range(SPACE):
        fin_copy(d, True).wait_send()

    @pl.loop(1, CHIPS)
    def _(j):
        @pl.when(chip != j)
        def _():
            ret_copy(j).wait_send()


def final_kernel(v, boosted, other, esum, partial, init, depth, depth_halo, out):
    slot = lax.axis_index("tm")
    even = lax.rem(slot, 2) == 0
    first = slot == 0
    n = CHUNK + 256

    def right(x):
        return pltpu.roll(x, x.shape[1] - 1, 1)

    def left(x):
        return pltpu.roll(x, 1, 1)

    def down(x):
        return pltpu.roll(x, 23, 0)

    def up(x):
        return pltpu.roll(x, 1, 0)

    low = lax.broadcasted_iota(jnp.int32, (8, n), 0) < 4

    @pl.loop(0, COLS // CHUNK)
    def _(i):
        base = pl.multiple_of(i * CHUNK, CHUNK)
        lo = pl.multiple_of(lax.rem(base + COLS - 128, COLS), 128)
        hi = pl.multiple_of(lax.rem(base + CHUNK, COLS), 128)
        parts = (pl.ds(lo, 128), pl.ds(base, CHUNK), pl.ds(hi, 128))
        cols = pl.ds(base, CHUNK)

        def ring(f):
            x = jnp.concatenate([v[f, :, c] for c in parts], axis=1)
            return jnp.concatenate([x[:16], jnp.where(low, x[16:24], x[24:32])], axis=0)

        d = jnp.concatenate([jnp.concatenate([depth[:, c], depth_halo[:, c]], axis=0) for c in parts], axis=1)

        def stepped(state):
            h, u, w = state
            r = rates(h, u, w, d * u, d * w, left, right, up, down, lambda x: x)
            return [x + step_size * y for x, y in zip(state, r)]

        state = [ring(f) for f in range(3)]
        a = stepped(state)
        b = stepped(a)
        for f in range(3):
            begin = state[f][:16, 128 : 128 + CHUNK]
            ours = jnp.where(even, boosted[f, :, cols], other[f, :, cols])
            y1 = ours + a[f][:16, 128 : 128 + CHUNK]
            y2 = esum[f, :, cols] + b[f][:16, 128 : 128 + CHUNK]
            start = jnp.where(even, jnp.where(first, init[f, :, cols], begin), y1)
            end = jnp.where(even, y1, y2)
            out[0, f, :, cols] = start
            out[1, f, :, cols] = partial[f, :, cols] + 0.5 * (start + end)
            out[2, f, :, cols] = end


VM = pl.BlockSpec(memory_space=pltpu.VMEM)


def per_device(fine_nodes, init_state, mean_depth):
    points = fine_nodes[0].reshape(9, ROWS, COLS)
    slot = lax.axis_index("tm")
    last = slot == 31
    is_first = slot == 0
    ring_next = [((i + 1) % SPACE, i) for i in range(SPACE)]
    ring_prev = [(i, (i + 1) % SPACE) for i in range(SPACE)]

    stacked = jnp.concatenate([points, mean_depth[None]], axis=0)
    after = lax.ppermute(stacked[:, :4], "space", ring_next)
    before = lax.ppermute(stacked[:, ROWS - 4 :], "space", ring_prev)
    halo = jnp.concatenate([after, before], axis=1)

    end = points[6:9]
    shifted = lax.ppermute(end, "tm", [(i, i + 1) for i in range(31)])
    start = jnp.where(is_first, init_state, shifted)
    flat = lambda t, sp: (t % 32) * SPACE + sp % SPACE
    edge = jnp.where(last, init_state, end)
    start_after = lax.ppermute(
        edge[:, :4], ("tm", "space"), [(flat(t, sp + 1), flat(t + 1, sp)) for t in range(32) for sp in range(SPACE)]
    )
    start_before = lax.ppermute(
        edge[:, ROWS - 4 :], ("tm", "space"), [(flat(t, sp), flat(t + 1, sp + 1)) for t in range(32) for sp in range(SPACE)]
    )
    start_halo = jnp.concatenate([start_after, start_before], axis=1)

    state = jax.ShapeDtypeStruct((3, ROWS, COLS), F32)
    ringed = pltpu.VMEM((3, 24, COLS), F32)
    item, boosted, partial = pl.pallas_call(
        fine_kernel,
        out_shape=[state] * 3,
        in_specs=[VM] * 6,
        out_specs=[VM] * 3,
        scratch_shapes=[ringed] * 5,
        name="fine",
    )(points, halo[:9], start, start_halo, mean_depth, halo[9])

    dma = pltpu.SemaphoreType.DMA
    esum, other, v = pl.pallas_call(
        coarse_kernel,
        out_shape=[state, state, jax.ShapeDtypeStruct((3, 32, COLS), F32)],
        in_specs=[VM] * 3,
        out_specs=[VM] * 3,
        scratch_shapes=[
            pltpu.VMEM((3, ROWS, COLS), F32),
            pltpu.VMEM((3, 128, PART), F32),
            pltpu.VMEM((3, PART, 128), F32),
            pltpu.VMEM((128, 512), F32),
            pltpu.VMEM((512, 128), F32),
            pltpu.VMEM((CHIPS, 3, WIDE, 128), F32),
            pltpu.VMEM((CHIPS, 3, OWN, 128), F32),
            pltpu.VMEM((3, PART, 128), F32),
            pltpu.VMEM((3, 128, PART), F32),
            dma((2,)), dma((2,)), dma((8,)), dma((8,)), dma((3, 8)), dma((3, 8)), dma((16,)), dma((16,)),
            dma((8,)), dma((8,)), dma((16,)), dma((16,)), dma((3, 8)), dma((3, 8)), dma((8,)), dma((8,)),
        ],
        compiler_params=pltpu.CompilerParams(collective_id=0, has_side_effects=True),
        name="coarse",
    )(item, boosted, mean_depth)

    out = pl.pallas_call(
        final_kernel,
        out_shape=jax.ShapeDtypeStruct((3, 3, ROWS, COLS), F32),
        in_specs=[VM] * 8,
        out_specs=VM,
        name="final",
    )(v, boosted, other, esum, partial, init_state, mean_depth, halo[9])
    return out[None]


def solution(mesh):
    placed = (P("tm", None, None, "space", None), P(None, "space", None), P("space", None))
    return jax.shard_map(
        per_device,
        mesh=mesh,
        in_specs=placed,
        out_specs=P("tm", None, None, "space", None),
        check_vma=False,
    )
```

```python
import functools

import jax
import jax.numpy as jnp
from jax import lax
from jax.experimental import pallas as pl
from jax.experimental.pallas import tpu as pltpu
from jax.sharding import PartitionSpec as P

MESH = pl.DeviceIdType.MESH
F32 = jnp.float32

step_size = 0.3
viscosity = 1.0 / 3.0
coriolis = 0.5
quad_near = 5.0 / 24.0
quad_mid = 1.0 / 3.0
quad_far = -1.0 / 24.0
half_step = 0.5 * step_size
start_share = -(half_step + step_size / 3.0)
one_share = 2.0 * step_size / 3.0
two_share = half_step - step_size / 3.0

ROWS = 16
COLS = 4096
SPACE = 8
CHIPS = 16
PART = 256
OWN = 16
HALO = 32
WIDE = OWN + 2 * HALO


def rates(h, u, v, de, dn, left, right, up, down, centre):
    nh, nu, nv = viscosity * h, viscosity * u, viscosity * v
    he, hn, hh = 0.5 * de, 0.5 * dn, 0.5 * h
    nhc, nuc, nvc = centre(nh), centre(nu), centre(nv)
    hr = right(nh - he) + left(nh + he) + down(centre(nh - hn)) + up(centre(nh + hn)) - 4.0 * nhc
    ur = right(nu - hh) + left(nu + hh) + down(nuc) + up(nuc) - 4.0 * nuc + coriolis * centre(v)
    vr = right(nv) + left(nv) + down(centre(nv - hh)) + up(centre(nv + hh)) - 4.0 * nvc - coriolis * centre(u)
    return hr, ur, vr


CHUNK = 512
RING = 24


def edges(base):
    lo = pl.multiple_of(lax.rem(base + COLS - 128, COLS), 128)
    hi = pl.multiple_of(lax.rem(base + CHUNK, COLS), 128)
    return pl.ds(lo, 128), pl.ds(base, CHUNK), pl.ds(hi, 128)


def wide(get, base):
    return jnp.concatenate([get(c) for c in edges(base)], axis=1)


def right(x):
    return pltpu.roll(x, x.shape[1] - 1, 1)


def left(x):
    return pltpu.roll(x, 1, 1)


def down(x):
    return pltpu.roll(x, RING - 1, 0)


def up(x):
    return pltpu.roll(x, 1, 0)


def inner(x):
    return x[:, 128 : 128 + CHUNK]


def ring_rates(q, depth, base):
    h, u, v = (wide(lambda c, f=f: q[f, :, c], base) for f in range(3))
    d = wide(lambda c: depth[:, c], base)
    return rates(h, u, v, d * u, d * v, lambda x: inner(left(x)), lambda x: inner(right(x)), up, down, inner)


def chunks(body):
    @pl.loop(0, COLS // CHUNK)
    def _(i):
        body(pl.multiple_of(i * CHUNK, CHUNK))


def sub_roll(x, by):
    by %= 8
    return x if by == 0 else pltpu.roll(x, by, 0)


def pack(parts, at):
    row = lax.broadcasted_iota(jnp.int32, parts[0].shape, 0)
    tile = sub_roll(parts[0], -at)
    for i in range(1, len(parts)):
        tile = jnp.where(row >= 2 * i, sub_roll(parts[i], 2 * i - at), tile)
    return tile


def unpack(after, before, i):
    row = lax.broadcasted_iota(jnp.int32, after.shape, 0)
    return jnp.where(row < 4, sub_roll(after, -2 * i), sub_roll(before, 6 - 2 * i))


def snake(chip):
    z, x = chip // 4, lax.rem(chip, 4)
    return z * 4 + jnp.where(lax.rem(z, 2) == 0, x, 3 - x)


def owner(s, i):
    o = jnp.where(lax.rem(s, 2) == 0, i, 31 - i)
    return snake(o // 2) * 2 + lax.rem(o, 2)


def owned(s, tm):
    o = snake(tm // 2) * 2 + lax.rem(tm, 2)
    return jnp.where(lax.rem(s, 2) == 0, o, 31 - o)


def coarse_kernel(
    points, init, depth,
    boosted, other, esum, partial, vout, drow,
    s0, a1, a2, ps, pr, fs, fr, s0r, q1, s1, q2, q3, q3s, q3r, br, item, ritem,
    rt, et, dr, dt, ex, vx, vt, vr,
    st_s, st_r, pk_s, pk_r, q3_ss, q3_rs, it_s, it_r, oth_s, oth_r, one_s, one_r, dep_s, dep_r, two_s, two_r,
    halo_s, halo_r, ret_s, ret_r, row_s, row_r, fin_s, fin_r,
):
    tm = lax.axis_index("tm")
    s = lax.axis_index("space")
    chip, k = tm // 2, lax.rem(tm, 2)
    mine = owned(s, tm)
    half, spot = mine // 16, lax.rem(mine, 16)
    s_next, s_prev = lax.rem(s + 1, SPACE), lax.rem(s + SPACE - 1, SPACE)
    tm_next, tm_prev = lax.rem(tm + 1, 32), lax.rem(tm + 31, 32)
    first = jnp.where(tm == 0, 1.0, 0.0).astype(F32)
    even = jnp.where(k == 0, step_size, 0.0).astype(F32)

    def at(t, sp):
        return {"tm": t, "space": sp}

    def near(step):
        p = lax.rem(32 * s + mine + step + 256, 256)
        return at(owner(p // 32, lax.rem(p, 32)), p // 32)

    partner = at(chip * 2 + 1 - k, s)
    nears = [near(1), near(-1), near(2), near(-2)]

    vt[...] = jnp.zeros_like(vt)
    barrier = pltpu.get_barrier_semaphore()
    peers = [at(lax.rem(tm + d, 32), s) for d in range(1, 32)]
    peers += [at(tm, lax.rem(s + d, SPACE)) for d in range(1, SPACE)]
    peers += [at(t, sp) for t in (tm_next, tm_prev) for sp in (s_next, s_prev)]
    peers += nears
    for p in peers:
        pl.semaphore_signal(barrier, inc=1, device_id=p, device_id_type=MESH)
    pl.semaphore_wait(barrier, len(peers))

    def copy(src, dst, ss, rs, dev):
        return pltpu.make_async_remote_copy(src_ref=src, dst_ref=dst, send_sem=ss, recv_sem=rs, device_id=dev, device_id_type=MESH)

    def block(sp, kk):
        return pl.ds(pl.multiple_of(512 * sp + 256 * kk, PART), PART)

    def rows(start, n=ROWS):
        return pl.ds(pl.multiple_of(start, 8), n)

    start = copy(points.at[6:9], s0, st_s.at[0], st_r.at[0], at(tm_next, s))

    @pl.when(tm < 31)
    def _():
        start.start()

    def prepare(base):
        cols = pl.ds(base, CHUNK)
        top, bottom = [], []
        for f in range(3):
            p0, p1, p2 = (points[3 * m + f, :, cols] for m in range(3))
            x = (step_size * quad_near - half_step) * p0 + (step_size * quad_mid) * p1 + (step_size * quad_far) * p2
            y = (step_size * quad_far) * p0 + (step_size * quad_mid - half_step) * p1 + (step_size * quad_near) * p2
            a1[f, :, cols] = x
            a2[f, :, cols] = y
            top.append((x[:8], y[:8]))
            bottom.append((x[8:], y[8:]))
        for n, (parts, row) in enumerate(((bottom, 6), (top, 0))):
            ps[n, 0, :, cols] = pack([p[0] for p in parts] + [parts[0][1]], row)
            ps[n, 1, :, cols] = pack([parts[1][1], parts[2][1]], row)
            tile = pl.ds(8, 8) if n == 0 else pl.ds(0, 8)
            ends = [jnp.where(tm == 31, init[f, tile, cols], points[6 + f, tile, cols]) for f in range(3)]
            fs[n, :, cols] = pack(ends + [depth[tile, cols]], row)

    chunks(prepare)
    packs = [
        (ps.at[0], pr.at[0], at(tm, s_next)),
        (ps.at[1], pr.at[1], at(tm, s_prev)),
        (fs.at[0], fr.at[0], at(tm_next, s_next)),
        (fs.at[1], fr.at[1], at(tm_next, s_prev)),
    ]
    packs = [copy(src, dst, pk_s.at[n], pk_r.at[n], dev) for n, (src, dst, dev) in enumerate(packs)]
    for c in packs:
        c.start()

    def depth_pieces(base):
        return (
            (pl.ds(pl.multiple_of(base, 128), PART), pl.ds(128, PART)),
            (pl.ds(pl.multiple_of(lax.rem(base + COLS - 128, COLS), 128), 128), pl.ds(0, 128)),
            (pl.ds(pl.multiple_of(lax.rem(base + PART, COLS), 128), 128), pl.ds(384, 128)),
        )

    def depth_copy(d, n, send):
        sp = lax.rem(s + d, SPACE) if send else lax.rem(s + SPACE - d, SPACE)
        to = sp if send else s
        src, dst = depth_pieces(512 * to + 256 * (owned(to, tm) // 16))[n]
        return copy(depth.at[:, src], dr.at[rows(ROWS * (s if send else sp)), dst], dep_s.at[n, d], dep_r.at[n, d], at(tm, sp))

    for d in range(1, SPACE):
        for n in range(3):
            depth_copy(d, n, True).start()
    for src, dst in depth_pieces(512 * s + 256 * half):
        dr[rows(ROWS * s), dst] = depth[:, src]

    for n, dev in enumerate((at(tm, s_prev), at(tm, s_next), at(tm_prev, s_prev), at(tm_prev, s_next))):
        src, dst = ((ps.at[n], pr.at[n]), (fs.at[n - 2], fr.at[n - 2]))[n // 2]
        copy(src, dst, pk_s.at[n], pk_r.at[n], dev).wait_recv()

    @pl.when(tm > 0)
    def _():
        copy(points.at[6:9], s0, st_s.at[0], st_r.at[0], at(tm_prev, s)).wait_recv()

    def ringed(base):
        cols = pl.ds(base, CHUNK)
        drow[:, cols] = jnp.concatenate([depth[:, cols], unpack(fr[1, :, cols], fr[0, :, cols], 3)], axis=0)
        for f in range(3):
            main = jnp.where(tm == 0, init[f, :, cols], s0[f, :, cols])
            x = jnp.concatenate([main, unpack(fr[1, :, cols], fr[0, :, cols], f)], axis=0)
            y = jnp.concatenate([a1[f, :, cols], unpack(pr[1, 0, :, cols], pr[0, 0, :, cols], f)], axis=0)
            s0r[f, :, cols] = x
            q1[f, :, cols] = half_step * x + y

    chunks(ringed)

    def one(base):
        cols = pl.ds(base, CHUNK)
        r = ring_rates(q1, drow, base)
        for f in range(3):
            x = s0r[f, :, cols] + r[f]
            tile, i = (0, 3) if f == 0 else (1, f - 1)
            y = jnp.concatenate([a2[f, :, cols], unpack(pr[1, tile, :, cols], pr[0, tile, :, cols], i)], axis=0)
            s1[f, :, cols] = x
            q2[f, :, cols] = half_step * x + y

    chunks(one)

    def two(base):
        cols = pl.ds(base, CHUNK)
        r = ring_rates(q2, drow, base)
        top, bottom = [], []
        for f in range(3):
            x, y = s0r[f, :ROWS, cols], s1[f, :ROWS, cols]
            z = y + r[f][:ROWS]
            partial[f, :, cols] = y - 0.5 * (x + z)
            q = (step_size * first + start_share) * x + one_share * y + two_share * z
            q3[f, :ROWS, cols] = q
            top.append(q[:8])
            bottom.append(q[8:])
        q3s[0, :, cols] = pack(bottom, 6)
        q3s[1, :, cols] = pack(top, 0)

    chunks(two)
    for n, sp in enumerate((s_next, s_prev)):
        copy(q3s.at[n], q3r.at[n], q3_ss.at[n], q3_rs.at[n], at(tm, sp)).start()

    for d in range(1, SPACE):
        for n in range(3):
            depth_copy(d, n, False).wait_recv()
    for t in range(4):
        dt[128 * t : 128 * t + 128, :] = dr[:, 128 * t : 128 * t + 128].T

    for n, sp in enumerate((s_prev, s_next)):
        copy(q3s.at[n], q3r.at[n], q3_ss.at[n], q3_rs.at[n], at(tm, sp)).wait_recv()

    def edge_rows(base):
        cols = pl.ds(base, CHUNK)
        for f in range(3):
            q3[f, ROWS:, cols] = unpack(q3r[1, :, cols], q3r[0, :, cols], f)

    chunks(edge_rows)

    def three(base):
        cols = pl.ds(base, CHUNK)
        r = ring_rates(q3, drow, base)
        for f in range(3):
            x = r[f] + first * s0r[f, :, cols]
            br[f, :, cols] = x
            boosted[f, :, cols] = x[:ROWS]

    chunks(three)
    give = copy(boosted, other, oth_s.at[0], oth_r.at[0], partner)
    give.start()

    def item_copy(i):
        cols = pl.ds(pl.multiple_of(i * CHUNK, CHUNK), CHUNK)
        return copy(item.at[:, :, cols], ritem.at[:, :, cols], it_s.at[i], it_r.at[i], partner)

    @pl.loop(0, COLS // CHUNK)
    def _(i):
        base = pl.multiple_of(i * CHUNK, CHUNK)
        cols = pl.ds(base, CHUNK)
        r = ring_rates(br, drow, base)
        for f in range(3):
            item[f, :, cols] = br[f, :ROWS, cols] + even * r[f][:ROWS]
        item_copy(i).start()

    def one_copy(sp, send):
        to, by = (sp, s) if send else (s, sp)
        n = to if send else by
        return copy(esum.at[:, :, block(to, k)], rt.at[:, rows(ROWS * by), :], one_s.at[n], one_r.at[by], at(tm, sp))

    @pl.loop(0, SPACE)
    def _(d):
        sp = lax.rem(s + d + 1, SPACE)
        cols = pl.ds(pl.multiple_of(sp * CHUNK, CHUNK), CHUNK)
        item_copy(sp).wait_recv()
        for f in range(3):
            esum[f, :, cols] = item[f, :, cols] + ritem[f, :, cols]

        @pl.when(sp != s)
        def _():
            one_copy(sp, True).start()

    rt[:, rows(ROWS * s), :] = esum[:, :, block(s, k)]
    for d in range(1, SPACE):
        one_copy(lax.rem(s + SPACE - d, SPACE), False).wait_recv()
    for f in range(3):
        for t in range(2):
            et[f, 128 * t : 128 * t + 128, :] = rt[f, :, 128 * t : 128 * t + 128].T

    def two_copy(n):
        return copy(et.at[:, rows(OWN * n, OWN), :], ex.at[chip, :, pl.ds(HALO, OWN), :], two_s.at[n], two_r.at[chip], at(owner(s, 16 * k + n), s))

    @pl.loop(0, 16)
    def _(m):
        n = lax.rem(m + spot, 16)
        to = owner(s, 16 * k + n)

        @pl.when(to != tm)
        def _():
            two_copy(n).start()

    @pl.when(half == k)
    def _():
        ex[chip, :, HALO : HALO + OWN, :] = et[:, rows(OWN * spot, OWN), :]

    def halo_copy(n, j, width):
        hop, sign = n // 2 + 1, 1 - 2 * (n % 2)
        far = OWN * (hop - 1)
        if sign > 0:
            src, dst = HALO + OWN - width, HALO - far - width
        else:
            src, dst = HALO, HALO + OWN + far
        return copy(ex.at[j, :, pl.ds(src, width), :], ex.at[j, :, pl.ds(dst, width), :], halo_s.at[n, j], halo_r.at[n, j], nears[n])

    def each_halo(j, act):
        for lo, hi, ns, width in ((0, 10, (0, 1), 16), (10, 14, (0, 1), 8), (0, 2, (2, 3), 16), (2, 6, (2, 3), 8)):
            @pl.when((j >= lo) & (j < hi))
            def _():
                for n in ns:
                    act(halo_copy(n, j, width))

    @pl.loop(0, CHIPS)
    def _(d):
        c = lax.rem(chip + d, CHIPS)

        @pl.when((c != chip) | (half != k))
        def _():
            src = et.at[:, rows(OWN * spot, OWN), :]
            copy(src, ex.at[c, :, pl.ds(HALO, OWN), :], two_s.at[0], two_r.at[c], at(c * 2 + half, s)).wait_recv()

        each_halo(c, lambda x: x.start())

    d_own = dt[rows(96 + OWN * spot, WIDE), :]

    def stepped(state):
        h, u, v = state
        r = rates(
            h, u, v, d_own * u, d_own * v,
            lambda x: pltpu.roll(x, 1, 0), lambda x: pltpu.roll(x, WIDE - 1, 0),
            lambda x: pltpu.roll(x, 1, 1), lambda x: pltpu.roll(x, 127, 1), lambda x: x,
        )
        return tuple(x + step_size * y for x, y in zip(state, r))

    def ret_copy(j):
        return copy(vx.at[j], vt.at[:, rows(OWN * spot, OWN), :], ret_s.at[j], ret_r.at[spot], at(j * 2 + half, s))

    def body(j, state):
        state = stepped(stepped(state))
        each_halo(j, lambda x: x.wait_recv())
        state = tuple(x + ex[j, f] for f, x in enumerate(state))
        for f in range(3):
            vx[j + 1, f] = state[f][HALO : HALO + OWN]

        @pl.when((chip != j + 1) | (half != k))
        def _():
            ret_copy(j + 1).start()

        return state

    empty = jnp.zeros((WIDE, 128), F32)
    lax.fori_loop(0, CHIPS - 1, body, (empty, empty, empty))

    @pl.when(chip > 0)
    def _():
        @pl.when(half == k)
        def _():
            vt[:, rows(OWN * spot, OWN), :] = vx[chip]

        @pl.loop(0, 16)
        def _(n):
            t = owner(s, 16 * k + n)

            @pl.when(t != tm)
            def _():
                copy(vx.at[0], vt.at[:, rows(OWN * n, OWN), :], ret_s.at[0], ret_r.at[n], at(t, s)).wait_recv()

    low = lax.broadcasted_iota(jnp.int32, (8, 128), 0) < 4
    for f in range(3):
        for t in range(2):
            cols = slice(128 * t, 128 * t + 128)
            x = vt[f, cols, :].T
            for sp in range(SPACE):
                vr[sp, f, :ROWS, cols] = x[16 * sp : 16 * sp + 16]
                a, b = (16 * sp + 16) % 128, (16 * sp + 120) % 128
                vr[sp, f, ROWS:, cols] = jnp.where(low, x[a : a + 8], x[b : b + 8])

    def row_copy(sp, send):
        to, by = (sp, s) if send else (s, sp)
        return copy(vr.at[to], vout.at[:, :, block(by, k)], row_s.at[sp], row_r.at[by], at(tm, sp))

    def fin_copy(sp, send):
        cols = block(sp, k if send else 1 - k)
        return copy(vout.at[:, :, cols], vout.at[:, :, cols], fin_s.at[sp], fin_r.at[sp], partner)

    for d in range(1, SPACE):
        row_copy(lax.rem(s + d, SPACE), True).start()
    vout[:, :, block(s, k)] = vr[s]
    fin_copy(s, True).start()
    for d in range(1, SPACE):
        sp = lax.rem(s + SPACE - d, SPACE)
        row_copy(sp, False).wait_recv()
        fin_copy(sp, True).start()
    give.wait_recv()
    for sp in range(SPACE):
        fin_copy(sp, False).wait_recv()

    @pl.when(tm < 31)
    def _():
        start.wait_send()

    for c in packs:
        c.wait_send()
    for n, sp in enumerate((s_next, s_prev)):
        copy(q3s.at[n], q3r.at[n], q3_ss.at[n], q3_rs.at[n], at(tm, sp)).wait_send()
    give.wait_send()
    for i in range(COLS // CHUNK):
        item_copy(i).wait_send()
    for d in range(1, SPACE):
        for n in range(3):
            depth_copy(d, n, True).wait_send()
        one_copy(lax.rem(s + d, SPACE), True).wait_send()
        row_copy(lax.rem(s + d, SPACE), True).wait_send()
    for sp in range(SPACE):
        fin_copy(sp, True).wait_send()

    @pl.loop(0, 16)
    def _(n):
        @pl.when(owner(s, 16 * k + n) != tm)
        def _():
            two_copy(n).wait_send()

        each_halo(n, lambda x: x.wait_send())

        @pl.when((n > 0) & ((chip != n) | (half != k)))
        def _():
            ret_copy(n).wait_send()


def final_kernel(v, boosted, other, esum, partial, init, depth, out):
    slot = lax.axis_index("tm")
    even = lax.rem(slot, 2) == 0
    first = slot == 0

    def body(base):
        cols = pl.ds(base, CHUNK)
        d = wide(lambda c: depth[:, c], base)

        def stepped(state):
            h, u, w = state
            r = rates(h, u, w, d * u, d * w, left, right, up, down, lambda x: x)
            return [x + step_size * y for x, y in zip(state, r)]

        state = [wide(lambda c, f=f: v[f, :, c], base) for f in range(3)]
        a = stepped(state)
        b = stepped(a)
        for f in range(3):
            begin = inner(state[f])[:ROWS]
            ours = jnp.where(even, boosted[f, :, cols], other[f, :, cols])
            y1 = ours + inner(a[f])[:ROWS]
            y2 = esum[f, :, cols] + inner(b[f])[:ROWS]
            start = jnp.where(even, jnp.where(first, init[f, :, cols], begin), y1)
            end = jnp.where(even, y1, y2)
            out[0, f, :, cols] = start
            out[1, f, :, cols] = partial[f, :, cols] + 0.5 * (start + end)
            out[2, f, :, cols] = end

    chunks(body)


VM = pl.BlockSpec(memory_space=pltpu.VMEM)


def per_device(fine_nodes, init_state, mean_depth):
    points = fine_nodes[0].reshape(9, ROWS, COLS)
    state = jax.ShapeDtypeStruct((3, ROWS, COLS), F32)
    ring = jax.ShapeDtypeStruct((3, RING, COLS), F32)

    def vm(*shape):
        return pltpu.VMEM(shape, F32)

    def sems(*shape):
        return [pltpu.SemaphoreType.DMA(shape)] * 2

    flat, ringed = vm(3, ROWS, COLS), vm(3, RING, COLS)
    boosted, other, esum, partial, v, depth = pl.pallas_call(
        coarse_kernel,
        out_shape=[state, state, state, state, ring, jax.ShapeDtypeStruct((RING, COLS), F32)],
        in_specs=[VM] * 3,
        out_specs=[VM] * 6,
        scratch_shapes=[
            flat, flat, flat, vm(2, 2, 8, COLS), vm(2, 2, 8, COLS), vm(2, 8, COLS), vm(2, 8, COLS),
            ringed, ringed, ringed, ringed, ringed, vm(2, 8, COLS), vm(2, 8, COLS), ringed, flat, flat,
            vm(3, 128, PART), vm(3, PART, 128), vm(128, 512), vm(512, 128),
            vm(CHIPS, 3, WIDE, 128), vm(CHIPS, 3, OWN, 128), vm(3, PART, 128), vm(SPACE, 3, RING, PART),
            *sems(1), *sems(4), *sems(2), *sems(8), *sems(1), *sems(8), *sems(3, 8), *sems(16),
            *sems(4, 16), *sems(16), *sems(8), *sems(8),
        ],
        compiler_params=pltpu.CompilerParams(collective_id=0, has_side_effects=True),
        name="sweep",
    )(points, init_state, mean_depth)

    out = pl.pallas_call(
        final_kernel,
        out_shape=jax.ShapeDtypeStruct((3, 3, ROWS, COLS), F32),
        in_specs=[VM] * 7,
        out_specs=VM,
        name="final",
    )(v, boosted, other, esum, partial, init_state, depth)
    return out[None]


def solution(mesh):
    placed = (P("tm", None, None, "space", None), P(None, "space", None), P("space", None))
    return jax.shard_map(
        per_device,
        mesh=mesh,
        in_specs=placed,
        out_specs=P("tm", None, None, "space", None),
        check_vma=False,
    )
```

```python
import functools

import jax
import jax.numpy as jnp
from jax import lax
from jax.experimental import pallas as pl
from jax.experimental.pallas import tpu as pltpu
from jax.sharding import PartitionSpec as P

MESH = pl.DeviceIdType.MESH
F32 = jnp.float32

step_size = 0.3
viscosity = 1.0 / 3.0
coriolis = 0.5
quad_near = 5.0 / 24.0
quad_mid = 1.0 / 3.0
quad_far = -1.0 / 24.0
half_step = 0.5 * step_size
start_share = -(half_step + step_size / 3.0)
one_share = 2.0 * step_size / 3.0
two_share = half_step - step_size / 3.0

ROWS = 16
COLS = 4096
SPACE = 8
CHIPS = 16
PART = 256
OWN = 16
HALO = 32
WIDE = OWN + 2 * HALO


def rates(h, u, v, de, dn, left, right, up, down, centre):
    nh, nu, nv = viscosity * h, viscosity * u, viscosity * v
    he, hn, hh = 0.5 * de, 0.5 * dn, 0.5 * h
    nhc, nuc, nvc = centre(nh), centre(nu), centre(nv)
    hr = right(nh - he) + left(nh + he) + down(centre(nh - hn)) + up(centre(nh + hn)) - 4.0 * nhc
    ur = right(nu - hh) + left(nu + hh) + down(nuc) + up(nuc) - 4.0 * nuc + coriolis * centre(v)
    vr = right(nv) + left(nv) + down(centre(nv - hh)) + up(centre(nv + hh)) - 4.0 * nvc - coriolis * centre(u)
    return hr, ur, vr


CHUNK = 512
RING = 24


def edges(base):
    lo = pl.multiple_of(lax.rem(base + COLS - 128, COLS), 128)
    hi = pl.multiple_of(lax.rem(base + CHUNK, COLS), 128)
    return pl.ds(lo, 128), pl.ds(base, CHUNK), pl.ds(hi, 128)


def wide(get, base):
    return jnp.concatenate([get(c) for c in edges(base)], axis=1)


def right(x):
    return pltpu.roll(x, x.shape[1] - 1, 1)


def left(x):
    return pltpu.roll(x, 1, 1)


def down(x):
    return pltpu.roll(x, RING - 1, 0)


def up(x):
    return pltpu.roll(x, 1, 0)


def inner(x):
    return x[:, 128 : 128 + CHUNK]


def ring_rates(q, depth, base):
    h, u, v = (wide(lambda c, f=f: q[f, :, c], base) for f in range(3))
    d = wide(lambda c: depth[:, c], base)
    return rates(h, u, v, d * u, d * v, lambda x: inner(left(x)), lambda x: inner(right(x)), up, down, inner)


def chunks(body):
    @pl.loop(0, COLS // CHUNK)
    def _(i):
        body(pl.multiple_of(i * CHUNK, CHUNK))


PAIRS = COLS // CHUNK // 2
FOLD = COLS // 2


def pairs(body):
    @pl.loop(0, PAIRS)
    def _(j):
        base = pl.multiple_of(j * CHUNK, CHUNK)
        body(j, pl.ds(base, CHUNK), [base, pl.multiple_of(base + FOLD, CHUNK)])


def sub_roll(x, by):
    by %= 8
    return x if by == 0 else pltpu.roll(x, by, 0)


def pack(parts, at):
    row = lax.broadcasted_iota(jnp.int32, parts[0].shape, 0)
    tile = sub_roll(parts[0], -at)
    for i in range(1, len(parts)):
        tile = jnp.where(row >= 2 * i, sub_roll(parts[i], 2 * i - at), tile)
    return tile


def place(parts, at):
    row = lax.broadcasted_iota(jnp.int32, parts[0].shape, 0)
    tile = sub_roll(parts[0], -at[0])
    for i in range(1, len(parts)):
        tile = jnp.where(row >= i, sub_roll(parts[i], i - at[i]), tile)
    return tile


def fold(first, second):
    row = lax.broadcasted_iota(jnp.int32, first.shape, 0)
    return jnp.where(row < 4, first, sub_roll(second, 4))


def unfold(after, before, i):
    row = lax.broadcasted_iota(jnp.int32, after.shape, 0)
    return jnp.where(row < 4, sub_roll(after, -i), sub_roll(before, 7 - i))


def unpack(after, before, i):
    row = lax.broadcasted_iota(jnp.int32, after.shape, 0)
    return jnp.where(row < 4, sub_roll(after, -2 * i), sub_roll(before, 6 - 2 * i))


def snake(chip):
    z, x = chip // 4, lax.rem(chip, 4)
    return z * 4 + jnp.where(lax.rem(z, 2) == 0, x, 3 - x)


def owner(s, i):
    o = jnp.where(lax.rem(s, 2) == 0, i, 31 - i)
    return snake(o // 2) * 2 + lax.rem(o, 2)


def owned(s, tm):
    o = snake(tm // 2) * 2 + lax.rem(tm, 2)
    return jnp.where(lax.rem(s, 2) == 0, o, 31 - o)


def coarse_kernel(
    points, init, depth,
    boosted, other, esum, partial, vout, drow,
    s0, a1, a2, ps, pr, fs, fr, s0r, q1, s1, q2, q2s, q2r, q3, q3s, q3r, br, item, ritem, relay,
    rt, et, dr, dt, ex, vx, vt, vr,
    st_s, st_r, rl_s, rl_r, pk_s, pk_r, q2_ss, q2_rs, q3_ss, q3_rs, it_s, it_r, oth_s, oth_r, one_s, one_r, dep_s, dep_r, two_s, two_r,
    halo_s, halo_r, ret_s, ret_r, row_s, row_r, fin_s, fin_r,
):
    tm = lax.axis_index("tm")
    s = lax.axis_index("space")
    chip, k = tm // 2, lax.rem(tm, 2)
    mine = owned(s, tm)
    half, spot = mine // 16, lax.rem(mine, 16)
    s_next, s_prev = lax.rem(s + 1, SPACE), lax.rem(s + SPACE - 1, SPACE)
    tm_next, tm_prev = lax.rem(tm + 1, 32), lax.rem(tm + 31, 32)
    first = jnp.where(tm == 0, 1.0, 0.0).astype(F32)
    even = jnp.where(k == 0, step_size, 0.0).astype(F32)

    def at(t, sp):
        return {"tm": t, "space": sp}

    def near(step):
        p = lax.rem(32 * s + mine + step + 256, 256)
        return at(owner(p // 32, lax.rem(p, 32)), p // 32)

    partner = at(chip * 2 + 1 - k, s)
    nears = [near(1), near(-1), near(2), near(-2)]

    vt[...] = jnp.zeros_like(vt)
    barrier = pltpu.get_barrier_semaphore()
    peers = [at(lax.rem(tm + d, 32), s) for d in range(1, 32)]
    peers += [at(tm, lax.rem(s + d, SPACE)) for d in range(1, SPACE)]
    peers += [at(t, sp) for t in (tm_next, tm_prev) for sp in (s_next, s_prev)]
    peers += nears
    for p in peers:
        pl.semaphore_signal(barrier, inc=1, device_id=p, device_id_type=MESH)
    pl.semaphore_wait(barrier, len(peers))

    def copy(src, dst, ss, rs, dev):
        return pltpu.make_async_remote_copy(src_ref=src, dst_ref=dst, send_sem=ss, recv_sem=rs, device_id=dev, device_id_type=MESH)

    def block(sp, kk):
        return pl.ds(pl.multiple_of(512 * sp + 256 * kk, PART), PART)

    def rows(start, n=ROWS):
        return pl.ds(pl.multiple_of(start, 8), n)

    z_place = lax.rem(tm, 8)
    far_end = (z_place == 7) & (tm < 31)
    relays = (z_place == 1) & (tm < 24)
    QUARTER = COLS // 4

    def start_copy(n, to, via=False):
        cols = pl.ds(QUARTER * n, QUARTER)
        if via:
            return copy(points.at[6:9, :, cols], relay.at[n - 2], st_s.at[n], rl_r.at[n - 2], at(to, s))
        return copy(points.at[6:9, :, cols], s0.at[:, :, cols], st_s.at[n], st_r.at[n], at(to, s))

    def pass_copy(n):
        return copy(relay.at[n], s0.at[:, :, pl.ds(QUARTER * (n + 2), QUARTER)], rl_s.at[n], st_r.at[n + 2], at(lax.rem(tm + 7, 32), s))

    @pl.when(tm < 31)
    def _():
        for n in range(2):
            start_copy(n, tm_next).start()

    @pl.when((tm < 31) & (z_place != 7))
    def _():
        for n in range(2, 4):
            start_copy(n, tm_next).start()

    @pl.when(far_end)
    def _():
        for n in range(2, 4):
            start_copy(n, lax.rem(tm + 26, 32), True).start()

    def pack_copy(n, j, send):
        up_down = lax.rem(s + (1 if (n % 2 == 0) == send else SPACE - 1), SPACE)
        slot = tm if n < 2 else (tm_next if send else tm_prev)
        cols = pl.ds(pl.multiple_of(j * CHUNK, CHUNK), CHUNK)
        src, dst = (ps, pr) if n < 2 else (fs, fr)
        return copy(src.at[n % 2, :, cols], dst.at[n % 2, :, cols], pk_s.at[n, j], pk_r.at[n, j], at(slot, up_down))

    def prepare(j, folded, bases):
        tiles = [[], []], [[], []]
        for base in bases:
            cols = pl.ds(base, CHUNK)
            top, bottom = [], []
            for f in range(3):
                p0, p1, p2 = (points[3 * m + f, :, cols] for m in range(3))
                x = (step_size * quad_near - half_step) * p0 + (step_size * quad_mid) * p1 + (step_size * quad_far) * p2
                y = (step_size * quad_far) * p0 + (step_size * quad_mid - half_step) * p1 + (step_size * quad_near) * p2
                a1[f, :, cols] = x
                a2[f, :, cols] = y
                top.append(x[:8])
                bottom.append(x[8:])
            for n, (parts, tile, row, inside) in enumerate(((bottom, 8, 7, 6), (top, 0, 0, 1))):
                d = depth[tile : tile + 8, cols]
                ends = [
                    jnp.where(tm == 31, init[f, tile : tile + 8, cols], points[6 + f, tile : tile + 8, cols]) for f in range(3)
                ]
                tiles[0][n].append(place(parts + [d], [row] * 4))
                tiles[1][n].append(place(ends + [d], [row] * 3 + [inside]))
        for n in range(2):
            ps[n, :, folded] = fold(*tiles[0][n])
            fs[n, :, folded] = fold(*tiles[1][n])
        for n in range(4):
            pack_copy(n, j, True).start()

    pairs(prepare)

    def depth_pieces(base):
        return (
            (pl.ds(pl.multiple_of(base, 128), PART), pl.ds(128, PART)),
            (pl.ds(pl.multiple_of(lax.rem(base + COLS - 128, COLS), 128), 128), pl.ds(0, 128)),
            (pl.ds(pl.multiple_of(lax.rem(base + PART, COLS), 128), 128), pl.ds(384, 128)),
        )

    def depth_copy(d, n, send):
        sp = lax.rem(s + d, SPACE) if send else lax.rem(s + SPACE - d, SPACE)
        to = sp if send else s
        src, dst = depth_pieces(512 * to + 256 * (owned(to, tm) // 16))[n]
        return copy(depth.at[:, src], dr.at[rows(ROWS * (s if send else sp)), dst], dep_s.at[n, d], dep_r.at[n, d], at(tm, sp))

    for d in range(1, SPACE):
        for n in range(3):
            depth_copy(d, n, True).start()
    for src, dst in depth_pieces(512 * s + 256 * half):
        dr[rows(ROWS * s), dst] = depth[:, src]

    @pl.when(relays)
    def _():
        for n in range(2):
            start_copy(n + 2, lax.rem(tm + 6, 32), True).wait_recv()
            pass_copy(n).start()

    for n in range(4):
        for j in range(PAIRS):
            pack_copy(n, j, False).wait_recv()

    @pl.when(tm > 0)
    def _():
        for n in range(4):
            start_copy(n, tm_prev).wait_recv()

    def ringed(j, folded, bases):
        row = lax.broadcasted_iota(jnp.int32, (8, CHUNK), 0)
        for h, base in enumerate(bases):
            cols = pl.ds(base, CHUNK)
            pa, pb, fa, fb = pr[1, :, folded], pr[0, :, folded], fr[1, :, folded], fr[0, :, folded]
            i = 4 * h + 3
            d = jnp.where(row < 4, sub_roll(fa, 1 - i), sub_roll(fb, 6 - i))
            d = jnp.where((row == 0) | (row == 7), unfold(pa, pb, i), d)
            drow[:, cols] = jnp.concatenate([depth[:, cols], d], axis=0)
            for f in range(3):
                main = jnp.where(tm == 0, init[f, :, cols], s0[f, :, cols])
                x = jnp.concatenate([main, unfold(fa, fb, 4 * h + f)], axis=0)
                y = jnp.concatenate([a1[f, :, cols], unfold(pa, pb, 4 * h + f)], axis=0)
                s0r[f, :, cols] = x
                q1[f, :, cols] = half_step * x + y

    pairs(ringed)

    def q2_copy(n, j, send):
        up_down = lax.rem(s + (1 if (n == 0) == send else SPACE - 1), SPACE)
        cols = pl.ds(pl.multiple_of(j * CHUNK, CHUNK), CHUNK)
        return copy(q2s.at[n, :, cols], q2r.at[n, :, cols], q2_ss.at[n, j], q2_rs.at[n, j], at(tm, up_down))

    def one(j, folded, bases):
        tiles = [[], []]
        for base in bases:
            cols = pl.ds(base, CHUNK)
            r = ring_rates(q1, drow, base)
            q = []
            for f in range(3):
                x = s0r[f, :ROWS, cols] + r[f][:ROWS]
                s1[f, :, cols] = x
                q.append(half_step * x + a2[f, :, cols])
                q2[f, :ROWS, cols] = q[f]
            tiles[0].append(place([x[8:] for x in q], [7] * 3))
            tiles[1].append(place([x[:8] for x in q], [0] * 3))
        for n in range(2):
            q2s[n, :, folded] = fold(*tiles[n])
            q2_copy(n, j, True).start()

    pairs(one)
    for n in range(2):
        for j in range(PAIRS):
            q2_copy(n, j, False).wait_recv()

    def q2_rows(j, folded, bases):
        for h, base in enumerate(bases):
            for f in range(3):
                q2[f, ROWS:, pl.ds(base, CHUNK)] = unfold(q2r[1, :, folded], q2r[0, :, folded], 4 * h + f)

    pairs(q2_rows)

    def q3_copy(n, i, send):
        up_down = lax.rem(s + (1 if (n == 0) == send else SPACE - 1), SPACE)
        cols = pl.ds(pl.multiple_of(i * CHUNK, CHUNK), CHUNK)
        return copy(q3s.at[n, :, cols], q3r.at[n, :, cols], q3_ss.at[n, i], q3_rs.at[n, i], at(tm, up_down))

    @pl.loop(0, COLS // CHUNK)
    def _(i):
        base = pl.multiple_of(i * CHUNK, CHUNK)
        cols = pl.ds(base, CHUNK)
        r = ring_rates(q2, drow, base)
        top, bottom = [], []
        for f in range(3):
            x, y = s0r[f, :ROWS, cols], s1[f, :, cols]
            z = y + r[f][:ROWS]
            partial[f, :, cols] = y - 0.5 * (x + z)
            q = (step_size * first + start_share) * x + one_share * y + two_share * z
            q3[f, :ROWS, cols] = q
            top.append(q[:8])
            bottom.append(q[8:])
        q3s[0, :, cols] = pack(bottom, 6)
        q3s[1, :, cols] = pack(top, 0)
        for n in range(2):
            q3_copy(n, i, True).start()

    for d in range(1, SPACE):
        for n in range(3):
            depth_copy(d, n, False).wait_recv()
    for t in range(4):
        dt[128 * t : 128 * t + 128, :] = dr[:, 128 * t : 128 * t + 128].T

    for i in range(COLS // CHUNK):
        for n in range(2):
            q3_copy(n, i, False).wait_recv()

    def edge_rows(base):
        cols = pl.ds(base, CHUNK)
        for f in range(3):
            q3[f, ROWS:, cols] = unpack(q3r[1, :, cols], q3r[0, :, cols], f)

    chunks(edge_rows)

    def three(base):
        cols = pl.ds(base, CHUNK)
        r = ring_rates(q3, drow, base)
        for f in range(3):
            x = r[f] + first * s0r[f, :, cols]
            br[f, :, cols] = x
            boosted[f, :, cols] = x[:ROWS]

    chunks(three)
    give = copy(boosted, other, oth_s.at[0], oth_r.at[0], partner)
    give.start()

    def item_copy(i):
        cols = pl.ds(pl.multiple_of(i * CHUNK, CHUNK), CHUNK)
        return copy(item.at[:, :, cols], ritem.at[:, :, cols], it_s.at[i], it_r.at[i], partner)

    @pl.loop(0, COLS // CHUNK)
    def _(i):
        base = pl.multiple_of(i * CHUNK, CHUNK)
        cols = pl.ds(base, CHUNK)
        r = ring_rates(br, drow, base)
        for f in range(3):
            item[f, :, cols] = br[f, :ROWS, cols] + even * r[f][:ROWS]
        item_copy(i).start()

    def one_copy(f, sp, send):
        to, by = (sp, s) if send else (s, sp)
        n = to if send else by
        return copy(esum.at[f, :, block(to, k)], rt.at[f, rows(ROWS * by), :], one_s.at[f, n], one_r.at[f, by], at(tm, sp))

    for i in range(COLS // CHUNK):
        item_copy(i).wait_recv()

    def summed(base):
        cols = pl.ds(base, CHUNK)
        for f in range(3):
            esum[f, :, cols] = item[f, :, cols] + ritem[f, :, cols]

    chunks(summed)
    for f in range(3):
        for d in range(1, SPACE):
            one_copy(f, lax.rem(s + d, SPACE), True).start()
    rt[:, rows(ROWS * s), :] = esum[:, :, block(s, k)]

    def two_copy(f, n):
        src, dst = et.at[f, rows(OWN * n, OWN), :], ex.at[chip, f, pl.ds(HALO, OWN), :]
        return copy(src, dst, two_s.at[f, n], two_r.at[f, chip], at(owner(s, 16 * k + n), s))

    for f in range(3):
        for d in range(1, SPACE):
            one_copy(f, lax.rem(s + SPACE - d, SPACE), False).wait_recv()
        for t in range(2):
            et[f, 128 * t : 128 * t + 128, :] = rt[f, :, 128 * t : 128 * t + 128].T

        @pl.loop(0, 16)
        def _(m, f=f):
            n = lax.rem(m + spot, 16)

            @pl.when(owner(s, 16 * k + n) != tm)
            def _():
                two_copy(f, n).start()

    @pl.when(half == k)
    def _():
        ex[chip, :, HALO : HALO + OWN, :] = et[:, rows(OWN * spot, OWN), :]

    def halo_copy(n, j, width):
        hop, sign = n // 2 + 1, 1 - 2 * (n % 2)
        far = OWN * (hop - 1)
        if sign > 0:
            src, dst = HALO + OWN - width, HALO - far - width
        else:
            src, dst = HALO, HALO + OWN + far
        return copy(ex.at[j, :, pl.ds(src, width), :], ex.at[j, :, pl.ds(dst, width), :], halo_s.at[n, j], halo_r.at[n, j], nears[n])

    def each_halo(j, act):
        for lo, hi, ns, width in ((0, 10, (0, 1), 16), (10, 14, (0, 1), 8), (0, 2, (2, 3), 16), (2, 6, (2, 3), 8)):
            @pl.when((j >= lo) & (j < hi))
            def _():
                for n in ns:
                    act(halo_copy(n, j, width))

    @pl.loop(0, CHIPS)
    def _(d):
        c = lax.rem(chip + d, CHIPS)

        @pl.when((c != chip) | (half != k))
        def _():
            for f in range(3):
                src, dst = et.at[f, rows(OWN * spot, OWN), :], ex.at[c, f, pl.ds(HALO, OWN), :]
                copy(src, dst, two_s.at[f, 0], two_r.at[f, c], at(c * 2 + half, s)).wait_recv()

        each_halo(c, lambda x: x.start())

    def scanned(lo, hi, halo, state):
        count = OWN + 2 * halo
        d_own = dt[rows(128 - halo + OWN * spot, count), :]

        def stepped(state):
            h, u, v = state
            r = rates(
                h, u, v, d_own * u, d_own * v,
                lambda x: pltpu.roll(x, 1, 0), lambda x: pltpu.roll(x, count - 1, 0),
                lambda x: pltpu.roll(x, 1, 1), lambda x: pltpu.roll(x, 127, 1), lambda x: x,
            )
            return tuple(x + step_size * y for x, y in zip(state, r))

        def body(j, state):
            state = stepped(stepped(state))
            each_halo(j, lambda x: x.wait_recv())
            state = tuple(x + ex[j, f, HALO - halo : HALO + OWN + halo] for f, x in enumerate(state))
            for f in range(3):
                vx[j + 1, f] = state[f][halo : halo + OWN]

            @pl.when((chip != j + 1) | (half != k))
            def _():
                ret_copy(j + 1).start()

            return state

        return lax.fori_loop(lo, hi, body, state)

    def ret_copy(j):
        return copy(vx.at[j], vt.at[:, rows(OWN * spot, OWN), :], ret_s.at[j], ret_r.at[spot], at(j * 2 + half, s))

    state = scanned(0, 7, 32, (jnp.zeros((WIDE, 128), F32),) * 3)
    state = scanned(7, 11, 16, tuple(x[16:64] for x in state))
    scanned(11, CHIPS - 1, 8, tuple(x[8:40] for x in state))

    @pl.when(chip > 0)
    def _():
        @pl.when(half == k)
        def _():
            vt[:, rows(OWN * spot, OWN), :] = vx[chip]

        @pl.loop(0, 16)
        def _(n):
            t = owner(s, 16 * k + n)

            @pl.when(t != tm)
            def _():
                copy(vx.at[0], vt.at[:, rows(OWN * n, OWN), :], ret_s.at[0], ret_r.at[n], at(t, s)).wait_recv()

    low = lax.broadcasted_iota(jnp.int32, (8, 128), 0) < 4
    for f in range(3):
        for t in range(2):
            cols = slice(128 * t, 128 * t + 128)
            x = vt[f, cols, :].T
            for sp in range(SPACE):
                vr[sp, f, :ROWS, cols] = x[16 * sp : 16 * sp + 16]
                a, b = (16 * sp + 16) % 128, (16 * sp + 120) % 128
                vr[sp, f, ROWS:, cols] = jnp.where(low, x[a : a + 8], x[b : b + 8])

    def row_copy(sp, send):
        to, by = (sp, s) if send else (s, sp)
        return copy(vr.at[to], vout.at[:, :, block(by, k)], row_s.at[sp], row_r.at[by], at(tm, sp))

    def fin_copy(sp, send):
        cols = block(sp, k if send else 1 - k)
        return copy(vout.at[:, :, cols], vout.at[:, :, cols], fin_s.at[sp], fin_r.at[sp], partner)

    for d in range(1, SPACE):
        row_copy(lax.rem(s + d, SPACE), True).start()
    vout[:, :, block(s, k)] = vr[s]
    fin_copy(s, True).start()
    for d in range(1, SPACE):
        sp = lax.rem(s + SPACE - d, SPACE)
        row_copy(sp, False).wait_recv()
        fin_copy(sp, True).start()
    give.wait_recv()
    for sp in range(SPACE):
        fin_copy(sp, False).wait_recv()

    @pl.when(tm < 31)
    def _():
        for n in range(4):
            start_copy(n, tm_next).wait_send()

    @pl.when(relays)
    def _():
        for n in range(2):
            pass_copy(n).wait_send()

    for n in range(4):
        for j in range(PAIRS):
            pack_copy(n, j, True).wait_send()
    for n in range(2):
        for j in range(PAIRS):
            q2_copy(n, j, True).wait_send()
        for i in range(COLS // CHUNK):
            q3_copy(n, i, True).wait_send()
    give.wait_send()
    for i in range(COLS // CHUNK):
        item_copy(i).wait_send()
    for d in range(1, SPACE):
        for n in range(3):
            depth_copy(d, n, True).wait_send()
        for f in range(3):
            one_copy(f, lax.rem(s + d, SPACE), True).wait_send()
        row_copy(lax.rem(s + d, SPACE), True).wait_send()
    for sp in range(SPACE):
        fin_copy(sp, True).wait_send()

    @pl.loop(0, 16)
    def _(n):
        @pl.when(owner(s, 16 * k + n) != tm)
        def _():
            for f in range(3):
                two_copy(f, n).wait_send()

        each_halo(n, lambda x: x.wait_send())

        @pl.when((n > 0) & ((chip != n) | (half != k)))
        def _():
            ret_copy(n).wait_send()


def final_kernel(v, boosted, other, esum, partial, init, depth, out):
    slot = lax.axis_index("tm")
    even = lax.rem(slot, 2) == 0
    first = slot == 0

    def body(base):
        cols = pl.ds(base, CHUNK)
        d = wide(lambda c: depth[:, c], base)

        def stepped(state):
            h, u, w = state
            r = rates(h, u, w, d * u, d * w, left, right, up, down, lambda x: x)
            return [x + step_size * y for x, y in zip(state, r)]

        state = [wide(lambda c, f=f: v[f, :, c], base) for f in range(3)]
        a = stepped(state)
        b = stepped(a)
        for f in range(3):
            begin = inner(state[f])[:ROWS]
            ours = jnp.where(even, boosted[f, :, cols], other[f, :, cols])
            y1 = ours + inner(a[f])[:ROWS]
            y2 = esum[f, :, cols] + inner(b[f])[:ROWS]
            start = jnp.where(even, jnp.where(first, init[f, :, cols], begin), y1)
            end = jnp.where(even, y1, y2)
            out[0, f, :, cols] = start
            out[1, f, :, cols] = partial[f, :, cols] + 0.5 * (start + end)
            out[2, f, :, cols] = end

    chunks(body)


VM = pl.BlockSpec(memory_space=pltpu.VMEM)


def per_device(fine_nodes, init_state, mean_depth):
    points = fine_nodes[0].reshape(9, ROWS, COLS)
    state = jax.ShapeDtypeStruct((3, ROWS, COLS), F32)
    ring = jax.ShapeDtypeStruct((3, RING, COLS), F32)

    def vm(*shape):
        return pltpu.VMEM(shape, F32)

    def sems(*shape):
        return [pltpu.SemaphoreType.DMA(shape)] * 2

    flat, ringed = vm(3, ROWS, COLS), vm(3, RING, COLS)
    boosted, other, esum, partial, v, depth = pl.pallas_call(
        coarse_kernel,
        out_shape=[state, state, state, state, ring, jax.ShapeDtypeStruct((RING, COLS), F32)],
        in_specs=[VM] * 3,
        out_specs=[VM] * 6,
        scratch_shapes=[
            flat, flat, flat, vm(2, 8, FOLD), vm(2, 8, FOLD), vm(2, 8, FOLD), vm(2, 8, FOLD),
            ringed, ringed, flat, ringed, vm(2, 8, FOLD), vm(2, 8, FOLD), ringed, vm(2, 8, COLS), vm(2, 8, COLS),
            ringed, flat, flat, vm(2, 3, ROWS, COLS // 4),
            vm(3, 128, PART), vm(3, PART, 128), vm(128, 512), vm(512, 128),
            vm(CHIPS, 3, WIDE, 128), vm(CHIPS, 3, OWN, 128), vm(3, PART, 128), vm(SPACE, 3, RING, PART),
            *sems(4), *sems(2), *sems(4, 4), *sems(2, 4), *sems(2, 8), *sems(8), *sems(1), *sems(3, 8), *sems(3, 8), *sems(3, 16),
            *sems(4, 16), *sems(16), *sems(8), *sems(8),
        ],
        compiler_params=pltpu.CompilerParams(collective_id=0, has_side_effects=True, vmem_limit_bytes=36 << 20),
        name="sweep",
    )(points, init_state, mean_depth)

    out = pl.pallas_call(
        final_kernel,
        out_shape=jax.ShapeDtypeStruct((3, 3, ROWS, COLS), F32),
        in_specs=[VM] * 7,
        out_specs=VM,
        compiler_params=pltpu.CompilerParams(vmem_limit_bytes=24 << 20),
        name="final",
    )(v, boosted, other, esum, partial, init_state, depth)
    return out[None]


def solution(mesh):
    placed = (P("tm", None, None, "space", None), P(None, "space", None), P("space", None))
    return jax.shard_map(
        per_device,
        mesh=mesh,
        in_specs=placed,
        out_specs=P("tm", None, None, "space", None),
        check_vma=False,
    )
```

```python
import functools

import jax
import jax.numpy as jnp
from jax import lax
from jax.experimental import pallas as pl
from jax.experimental.pallas import tpu as pltpu
from jax.sharding import PartitionSpec as P

MESH = pl.DeviceIdType.MESH
F32 = jnp.float32

step_size = 0.3
viscosity = 1.0 / 3.0
coriolis = 0.5
quad_near = 5.0 / 24.0
quad_mid = 1.0 / 3.0
quad_far = -1.0 / 24.0
half_step = 0.5 * step_size
start_share = -(half_step + step_size / 3.0)
one_share = 2.0 * step_size / 3.0
two_share = half_step - step_size / 3.0

ROWS = 16
COLS = 4096
SPACE = 8
CHIPS = 16
PART = 256
OWN = 16
HALO = 32
WIDE = OWN + 2 * HALO


def rates(h, u, v, de, dn, left, right, up, down, centre):
    nh, nu, nv = viscosity * h, viscosity * u, viscosity * v
    he, hn, hh = 0.5 * de, 0.5 * dn, 0.5 * h
    nhc, nuc, nvc = centre(nh), centre(nu), centre(nv)
    hr = right(nh - he) + left(nh + he) + down(centre(nh - hn)) + up(centre(nh + hn)) - 4.0 * nhc
    ur = right(nu - hh) + left(nu + hh) + down(nuc) + up(nuc) - 4.0 * nuc + coriolis * centre(v)
    vr = right(nv) + left(nv) + down(centre(nv - hh)) + up(centre(nv + hh)) - 4.0 * nvc - coriolis * centre(u)
    return hr, ur, vr


CHUNK = 512
RING = 24


def edges(base):
    lo = pl.multiple_of(lax.rem(base + COLS - 128, COLS), 128)
    hi = pl.multiple_of(lax.rem(base + CHUNK, COLS), 128)
    return pl.ds(lo, 128), pl.ds(base, CHUNK), pl.ds(hi, 128)


def wide(get, base):
    return jnp.concatenate([get(c) for c in edges(base)], axis=1)


def right(x):
    return pltpu.roll(x, x.shape[1] - 1, 1)


def left(x):
    return pltpu.roll(x, 1, 1)


def down(x):
    return pltpu.roll(x, RING - 1, 0)


def up(x):
    return pltpu.roll(x, 1, 0)


def inner(x):
    return x[:, 128 : 128 + CHUNK]


def ring_rates(q, depth, base):
    h, u, v = (wide(lambda c, f=f: q[f, :, c], base) for f in range(3))
    d = wide(lambda c: depth[:, c], base)
    return rates(h, u, v, d * u, d * v, lambda x: inner(left(x)), lambda x: inner(right(x)), up, down, inner)


def chunks(body):
    @pl.loop(0, COLS // CHUNK)
    def _(i):
        body(pl.multiple_of(i * CHUNK, CHUNK))


PAIRS = COLS // CHUNK // 2
FOLD = COLS // 2


def pairs(body):
    @pl.loop(0, PAIRS)
    def _(j):
        base = pl.multiple_of(j * CHUNK, CHUNK)
        body(j, pl.ds(base, CHUNK), [base, pl.multiple_of(base + FOLD, CHUNK)])


def sub_roll(x, by):
    by %= 8
    return x if by == 0 else pltpu.roll(x, by, 0)


def pack(parts, at):
    row = lax.broadcasted_iota(jnp.int32, parts[0].shape, 0)
    tile = sub_roll(parts[0], -at)
    for i in range(1, len(parts)):
        tile = jnp.where(row >= 2 * i, sub_roll(parts[i], 2 * i - at), tile)
    return tile


def place(parts, at):
    row = lax.broadcasted_iota(jnp.int32, parts[0].shape, 0)
    tile = sub_roll(parts[0], -at[0])
    for i in range(1, len(parts)):
        tile = jnp.where(row >= i, sub_roll(parts[i], i - at[i]), tile)
    return tile


def fold(first, second):
    row = lax.broadcasted_iota(jnp.int32, first.shape, 0)
    return jnp.where(row < 4, first, sub_roll(second, 4))


def unfold(after, before, i):
    row = lax.broadcasted_iota(jnp.int32, after.shape, 0)
    return jnp.where(row < 4, sub_roll(after, -i), sub_roll(before, 7 - i))


def unpack(after, before, i):
    row = lax.broadcasted_iota(jnp.int32, after.shape, 0)
    return jnp.where(row < 4, sub_roll(after, -2 * i), sub_roll(before, 6 - 2 * i))


def snake(n):
    z, x = n // 4, lax.rem(n, 4)
    return z * 4 + jnp.where(lax.rem(z, 2) == 0, x, 3 - x)


def turned(s, chip):
    return chip // 4 * 4 + lax.rem(chip + 2 * lax.rem(s, 2), 4)


def owner(s, i):
    o = jnp.where(lax.rem(s, 2) == 0, i, 31 - i)
    return turned(s, snake(o // 2)) * 2 + lax.rem(o, 2)


def owned(s, tm):
    o = snake(turned(s, tm // 2)) * 2 + lax.rem(tm, 2)
    return jnp.where(lax.rem(s, 2) == 0, o, 31 - o)


def coarse_kernel(
    points_hbm, init_hbm, depth_hbm,
    boosted, other, esum, partial, vout, drow,
    points, init, depth, s0, a1, a2, ps, pr, fs, fr, s0r, q1, s1, q2, q2s, q2r, q3, q3s, q3r, br, item, ritem, relay_a, relay_b,
    rt, et, dr, dt, ex, vx, vt, vr,
    in_sem, st_s, st_r, rl_s, rl_r, pk_s, pk_r, q2_ss, q2_rs, q3_ss, q3_rs, it_s, it_r, oth_s, oth_r, one_s, one_r, dep_s, dep_r, two_s, two_r,
    halo_s, halo_r, ret_s, ret_r, row_s, row_r, fin_s, fin_r,
):
    tm = lax.axis_index("tm")
    s = lax.axis_index("space")
    chip, k = tm // 2, lax.rem(tm, 2)
    mine = owned(s, tm)
    half, spot = mine // 16, lax.rem(mine, 16)
    s_next, s_prev = lax.rem(s + 1, SPACE), lax.rem(s + SPACE - 1, SPACE)
    tm_next, tm_prev = lax.rem(tm + 1, 32), lax.rem(tm + 31, 32)
    first = jnp.where(tm == 0, 1.0, 0.0).astype(F32)
    even = jnp.where(k == 0, step_size, 0.0).astype(F32)

    def at(t, sp):
        return {"tm": t, "space": sp}

    def near(step):
        p = lax.rem(32 * s + mine + step + 256, 256)
        return at(owner(p // 32, lax.rem(p, 32)), p // 32)

    partner = at(chip * 2 + 1 - k, s)
    nears = [near(1), near(-1), near(2), near(-2)]

    loads = [pltpu.make_async_copy(points_hbm.at[3 * m : 3 * m + 3], points.at[3 * m : 3 * m + 3], in_sem.at[m]) for m in range(3)]
    loads += [pltpu.make_async_copy(init_hbm, init, in_sem.at[3]), pltpu.make_async_copy(depth_hbm, depth, in_sem.at[4])]
    for n in (2, 0, 1, 4, 3):
        loads[n].start()
    vt[...] = jnp.zeros_like(vt)
    barrier = pltpu.get_barrier_semaphore()
    peers = [at(lax.rem(tm + d, 32), s) for d in range(1, 32)]
    peers += [at(tm, lax.rem(s + d, SPACE)) for d in range(1, SPACE)]
    peers += [at(t, sp) for t in (tm_next, tm_prev) for sp in (s_next, s_prev)]
    peers += nears
    for p in peers:
        pl.semaphore_signal(barrier, inc=1, device_id=p, device_id_type=MESH)
    pl.semaphore_wait(barrier, len(peers))

    def copy(src, dst, ss, rs, dev):
        return pltpu.make_async_remote_copy(src_ref=src, dst_ref=dst, send_sem=ss, recv_sem=rs, device_id=dev, device_id_type=MESH)

    def block(sp, kk):
        return pl.ds(pl.multiple_of(512 * sp + 256 * kk, PART), PART)

    def rows(start, n=ROWS):
        return pl.ds(pl.multiple_of(start, 8), n)

    loads[2].wait()

    z_place = lax.rem(tm, 8)
    far_end = (z_place == 7) & (tm < 31)
    PIECE = COLS // 8
    direct, by_a, by_b = range(0, 3), range(3, 6), range(6, 8)
    routes = ((by_a, relay_a, 6, 1), (by_b, relay_b, 2, 5))

    def piece(n):
        return pl.ds(PIECE * n, PIECE)

    def start_copy(n, to):
        return copy(points.at[6:9, :, piece(n)], s0.at[:, :, piece(n)], st_s.at[n], st_r.at[n], at(to, s))

    def via_copy(n, buffer, first_piece, to):
        return copy(points.at[6:9, :, piece(n)], buffer.at[n - first_piece], st_s.at[n], rl_r.at[n], at(to, s))

    def pass_copy(n, buffer, first_piece, ahead):
        return copy(buffer.at[n - first_piece], s0.at[:, :, piece(n)], rl_s.at[n], st_r.at[n], at(lax.rem(tm + ahead, 32), s))

    @pl.when((tm < 31) & (z_place != 7))
    def _():
        for n in range(8):
            start_copy(n, tm_next).start()

    @pl.when(far_end)
    def _():
        for ns, buffer, back, _ in routes:
            for n in ns:
                via_copy(n, buffer, ns[0], lax.rem(tm + 32 - back, 32)).start()

    for n in (0, 1, 4, 3):
        loads[n].wait()

    def pack_copy(n, j, send):
        up_down = lax.rem(s + (1 if (n % 2 == 0) == send else SPACE - 1), SPACE)
        slot = tm if n < 2 else (tm_next if send else tm_prev)
        cols = pl.ds(pl.multiple_of(j * CHUNK, CHUNK), CHUNK)
        src, dst = (ps, pr) if n < 2 else (fs, fr)
        return copy(src.at[n % 2, :, cols], dst.at[n % 2, :, cols], pk_s.at[n, j], pk_r.at[n, j], at(slot, up_down))

    def prepare(j, folded, bases):
        tiles = [[], []], [[], []]
        for base in bases:
            cols = pl.ds(base, CHUNK)
            top, bottom = [], []
            for f in range(3):
                p0, p1, p2 = (points[3 * m + f, :, cols] for m in range(3))
                x = (step_size * quad_near - half_step) * p0 + (step_size * quad_mid) * p1 + (step_size * quad_far) * p2
                y = (step_size * quad_far) * p0 + (step_size * quad_mid - half_step) * p1 + (step_size * quad_near) * p2
                a1[f, :, cols] = x
                a2[f, :, cols] = y
                top.append(x[:8])
                bottom.append(x[8:])
            for n, (parts, tile, row, inside) in enumerate(((bottom, 8, 7, 6), (top, 0, 0, 1))):
                d = depth[tile : tile + 8, cols]
                ends = [
                    jnp.where(tm == 31, init[f, tile : tile + 8, cols], points[6 + f, tile : tile + 8, cols]) for f in range(3)
                ]
                tiles[0][n].append(place(parts + [d], [row] * 4))
                tiles[1][n].append(place(ends + [d], [row] * 3 + [inside]))
        for n in range(2):
            ps[n, :, folded] = fold(*tiles[0][n])
            fs[n, :, folded] = fold(*tiles[1][n])
        for n in range(4):
            pack_copy(n, j, True).start()

    pairs(prepare)

    @pl.when(far_end)
    def _():
        for n in direct:
            start_copy(n, tm_next).start()

    def depth_pieces(base):
        return (
            (pl.ds(pl.multiple_of(base, 128), PART), pl.ds(128, PART)),
            (pl.ds(pl.multiple_of(lax.rem(base + COLS - 128, COLS), 128), 128), pl.ds(0, 128)),
            (pl.ds(pl.multiple_of(lax.rem(base + PART, COLS), 128), 128), pl.ds(384, 128)),
        )

    def depth_copy(d, n, send):
        sp = lax.rem(s + d, SPACE) if send else lax.rem(s + SPACE - d, SPACE)
        to = sp if send else s
        src, dst = depth_pieces(512 * to + 256 * (owned(to, tm) // 16))[n]
        return copy(depth.at[:, src], dr.at[rows(ROWS * (s if send else sp)), dst], dep_s.at[n, d], dep_r.at[n, d], at(tm, sp))

    for d in range(1, SPACE):
        for n in range(3):
            depth_copy(d, n, True).start()
    for src, dst in depth_pieces(512 * s + 256 * half):
        dr[rows(ROWS * s), dst] = depth[:, src]

    for ns, buffer, back, spot_of in routes:
        @pl.when((z_place == spot_of) & (tm < 24))
        def _(ns=ns, buffer=buffer, back=back):
            for n in ns:
                via_copy(n, buffer, ns[0], lax.rem(tm + back, 32)).wait_recv()
                pass_copy(n, buffer, ns[0], back + 1).start()

    for n in range(4):
        for j in range(PAIRS):
            pack_copy(n, j, False).wait_recv()

    @pl.when(tm > 0)
    def _():
        for n in range(8):
            start_copy(n, tm_prev).wait_recv()

    def ringed(j, folded, bases):
        row = lax.broadcasted_iota(jnp.int32, (8, CHUNK), 0)
        for h, base in enumerate(bases):
            cols = pl.ds(base, CHUNK)
            pa, pb, fa, fb = pr[1, :, folded], pr[0, :, folded], fr[1, :, folded], fr[0, :, folded]
            i = 4 * h + 3
            d = jnp.where(row < 4, sub_roll(fa, 1 - i), sub_roll(fb, 6 - i))
            d = jnp.where((row == 0) | (row == 7), unfold(pa, pb, i), d)
            drow[:, cols] = jnp.concatenate([depth[:, cols], d], axis=0)
            for f in range(3):
                main = jnp.where(tm == 0, init[f, :, cols], s0[f, :, cols])
                x = jnp.concatenate([main, unfold(fa, fb, 4 * h + f)], axis=0)
                y = jnp.concatenate([a1[f, :, cols], unfold(pa, pb, 4 * h + f)], axis=0)
                s0r[f, :, cols] = x
                q1[f, :, cols] = half_step * x + y

    pairs(ringed)

    def q2_copy(n, j, send):
        up_down = lax.rem(s + (1 if (n == 0) == send else SPACE - 1), SPACE)
        cols = pl.ds(pl.multiple_of(j * CHUNK, CHUNK), CHUNK)
        return copy(q2s.at[n, :, cols], q2r.at[n, :, cols], q2_ss.at[n, j], q2_rs.at[n, j], at(tm, up_down))

    def one(j, folded, bases):
        tiles = [[], []]
        for base in bases:
            cols = pl.ds(base, CHUNK)
            r = ring_rates(q1, drow, base)
            q = []
            for f in range(3):
                x = s0r[f, :ROWS, cols] + r[f][:ROWS]
                s1[f, :, cols] = x
                q.append(half_step * x + a2[f, :, cols])
                q2[f, :ROWS, cols] = q[f]
            tiles[0].append(place([x[8:] for x in q], [7] * 3))
            tiles[1].append(place([x[:8] for x in q], [0] * 3))
        for n in range(2):
            q2s[n, :, folded] = fold(*tiles[n])
            q2_copy(n, j, True).start()

    pairs(one)
    for n in range(2):
        for j in range(PAIRS):
            q2_copy(n, j, False).wait_recv()

    def q2_rows(j, folded, bases):
        for h, base in enumerate(bases):
            for f in range(3):
                q2[f, ROWS:, pl.ds(base, CHUNK)] = unfold(q2r[1, :, folded], q2r[0, :, folded], 4 * h + f)

    pairs(q2_rows)

    def q3_copy(n, i, send):
        up_down = lax.rem(s + (1 if (n == 0) == send else SPACE - 1), SPACE)
        cols = pl.ds(pl.multiple_of(i * CHUNK, CHUNK), CHUNK)
        return copy(q3s.at[n, :, cols], q3r.at[n, :, cols], q3_ss.at[n, i], q3_rs.at[n, i], at(tm, up_down))

    @pl.loop(0, COLS // CHUNK)
    def _(i):
        base = pl.multiple_of(i * CHUNK, CHUNK)
        cols = pl.ds(base, CHUNK)
        r = ring_rates(q2, drow, base)
        top, bottom = [], []
        for f in range(3):
            x, y = s0r[f, :ROWS, cols], s1[f, :, cols]
            z = y + r[f][:ROWS]
            partial[f, :, cols] = y - 0.5 * (x + z)
            q = (step_size * first + start_share) * x + one_share * y + two_share * z
            q3[f, :ROWS, cols] = q
            top.append(q[:8])
            bottom.append(q[8:])
        q3s[0, :, cols] = pack(bottom, 6)
        q3s[1, :, cols] = pack(top, 0)
        for n in range(2):
            q3_copy(n, i, True).start()

    for d in range(1, SPACE):
        for n in range(3):
            depth_copy(d, n, False).wait_recv()
    for t in range(4):
        dt[128 * t : 128 * t + 128, :] = dr[:, 128 * t : 128 * t + 128].T

    for i in range(COLS // CHUNK):
        for n in range(2):
            q3_copy(n, i, False).wait_recv()

    def edge_rows(base):
        cols = pl.ds(base, CHUNK)
        for f in range(3):
            q3[f, ROWS:, cols] = unpack(q3r[1, :, cols], q3r[0, :, cols], f)

    chunks(edge_rows)

    def three(base):
        cols = pl.ds(base, CHUNK)
        r = ring_rates(q3, drow, base)
        for f in range(3):
            x = r[f] + first * s0r[f, :, cols]
            br[f, :, cols] = x
            boosted[f, :, cols] = x[:ROWS]

    chunks(three)
    give = copy(boosted, other, oth_s.at[0], oth_r.at[0], partner)

    def item_copy(i):
        cols = pl.ds(pl.multiple_of(i * CHUNK, CHUNK), CHUNK)
        return copy(item.at[:, :, cols], ritem.at[:, :, cols], it_s.at[i], it_r.at[i], partner)

    @pl.loop(0, COLS // CHUNK)
    def _(i):
        base = pl.multiple_of(i * CHUNK, CHUNK)
        cols = pl.ds(base, CHUNK)
        r = ring_rates(br, drow, base)
        for f in range(3):
            item[f, :, cols] = br[f, :ROWS, cols] + even * r[f][:ROWS]
        item_copy(i).start()

    give.start()

    def one_copy(f, sp, send):
        to, by = (sp, s) if send else (s, sp)
        n = to if send else by
        return copy(esum.at[f, :, block(to, k)], rt.at[f, rows(ROWS * by), :], one_s.at[f, n], one_r.at[f, by], at(tm, sp))

    for i in range(COLS // CHUNK):
        item_copy(i).wait_recv()

    def summed(base):
        cols = pl.ds(base, CHUNK)
        for f in range(3):
            esum[f, :, cols] = item[f, :, cols] + ritem[f, :, cols]

    chunks(summed)
    for f in range(3):
        for d in range(1, SPACE):
            one_copy(f, lax.rem(s + d, SPACE), True).start()
    rt[:, rows(ROWS * s), :] = esum[:, :, block(s, k)]

    def two_copy(f, n):
        src, dst = et.at[f, rows(OWN * n, OWN), :], ex.at[chip, f, pl.ds(HALO, OWN), :]
        return copy(src, dst, two_s.at[f, n], two_r.at[f, chip], at(owner(s, 16 * k + n), s))

    for f in range(3):
        for d in range(1, SPACE):
            one_copy(f, lax.rem(s + SPACE - d, SPACE), False).wait_recv()
        for t in range(2):
            et[f, 128 * t : 128 * t + 128, :] = rt[f, :, 128 * t : 128 * t + 128].T

        @pl.loop(0, 16)
        def _(m, f=f):
            n = lax.rem(m + spot, 16)

            @pl.when((owner(s, 16 * k + n) != tm) & (chip < CHIPS - 1))
            def _():
                two_copy(f, n).start()

    @pl.when(half == k)
    def _():
        ex[chip, :, HALO : HALO + OWN, :] = et[:, rows(OWN * spot, OWN), :]

    def halo_copy(n, j, width):
        hop, sign = n // 2 + 1, 1 - 2 * (n % 2)
        far = OWN * (hop - 1)
        if sign > 0:
            src, dst = HALO + OWN - width, HALO - far - width
        else:
            src, dst = HALO, HALO + OWN + far
        return copy(ex.at[j, :, pl.ds(src, width), :], ex.at[j, :, pl.ds(dst, width), :], halo_s.at[n, j], halo_r.at[n, j], nears[n])

    def each_halo(j, act):
        for lo, hi, ns, width in ((0, 10, (0, 1), 16), (10, 14, (0, 1), 8), (0, 2, (2, 3), 16), (2, 6, (2, 3), 8)):
            @pl.when((j >= lo) & (j < hi))
            def _():
                for n in ns:
                    act(halo_copy(n, j, width))

    for c in (0, 1, 2, 5, 6, 9, 10, 13, 14, 3, 11, 7, 4, 8, 12):
        @pl.when((chip != c) | (half != k))
        def _(c=c):
            for f in range(3):
                src, dst = et.at[f, rows(OWN * spot, OWN), :], ex.at[c, f, pl.ds(HALO, OWN), :]
                copy(src, dst, two_s.at[f, 0], two_r.at[f, c], at(c * 2 + half, s)).wait_recv()

        for lo, hi, ns, width in ((0, 10, (0, 1), 16), (10, 14, (0, 1), 8), (0, 2, (2, 3), 16), (2, 6, (2, 3), 8)):
            if lo <= c < hi:
                for n in ns:
                    halo_copy(n, c, width).start()

    def scanned(lo, hi, halo, state):
        count = OWN + 2 * halo
        d_own = dt[rows(128 - halo + OWN * spot, count), :]

        def stepped(state):
            h, u, v = state
            r = rates(
                h, u, v, d_own * u, d_own * v,
                lambda x: pltpu.roll(x, 1, 0), lambda x: pltpu.roll(x, count - 1, 0),
                lambda x: pltpu.roll(x, 1, 1), lambda x: pltpu.roll(x, 127, 1), lambda x: x,
            )
            return tuple(x + step_size * y for x, y in zip(state, r))

        def body(j, state):
            state = stepped(stepped(state))
            each_halo(j, lambda x: x.wait_recv())
            state = tuple(x + ex[j, f, HALO - halo : HALO + OWN + halo] for f, x in enumerate(state))
            for f in range(3):
                vx[j + 1, f] = state[f][halo : halo + OWN]

            @pl.when((chip != j + 1) | (half != k))
            def _():
                ret_copy(j + 1).start()

            return state

        return lax.fori_loop(lo, hi, body, state)

    def ret_copy(j):
        return copy(vx.at[j], vt.at[:, rows(OWN * spot, OWN), :], ret_s.at[j], ret_r.at[spot], at(j * 2 + half, s))

    state = scanned(0, 7, 32, (jnp.zeros((WIDE, 128), F32),) * 3)
    state = scanned(7, 11, 16, tuple(x[16:64] for x in state))
    scanned(11, CHIPS - 1, 8, tuple(x[8:40] for x in state))

    @pl.when(chip > 0)
    def _():
        @pl.when(half == k)
        def _():
            vt[:, rows(OWN * spot, OWN), :] = vx[chip]

        @pl.loop(0, 16)
        def _(n):
            t = owner(s, 16 * k + n)

            @pl.when(t != tm)
            def _():
                copy(vx.at[0], vt.at[:, rows(OWN * n, OWN), :], ret_s.at[0], ret_r.at[n], at(t, s)).wait_recv()

    low = lax.broadcasted_iota(jnp.int32, (8, 128), 0) < 4
    for f in range(3):
        for t in range(2):
            cols = slice(128 * t, 128 * t + 128)
            x = vt[f, cols, :].T
            for sp in range(SPACE):
                vr[sp, f, :ROWS, cols] = x[16 * sp : 16 * sp + 16]
                a, b = (16 * sp + 16) % 128, (16 * sp + 120) % 128
                vr[sp, f, ROWS:, cols] = jnp.where(low, x[a : a + 8], x[b : b + 8])

    def row_copy(sp, send):
        to, by = (sp, s) if send else (s, sp)
        return copy(vr.at[to], vout.at[:, :, block(by, k)], row_s.at[sp], row_r.at[by], at(tm, sp))

    def fin_copy(sp, send):
        cols = block(sp, k if send else 1 - k)
        return copy(vout.at[:, :, cols], vout.at[:, :, cols], fin_s.at[sp], fin_r.at[sp], partner)

    for d in range(1, SPACE):
        row_copy(lax.rem(s + d, SPACE), True).start()
    vout[:, :, block(s, k)] = vr[s]
    fin_copy(s, True).start()
    for d in range(1, SPACE):
        sp = lax.rem(s + SPACE - d, SPACE)
        row_copy(sp, False).wait_recv()
        fin_copy(sp, True).start()
    give.wait_recv()
    for sp in range(SPACE):
        fin_copy(sp, False).wait_recv()

    @pl.when(tm < 31)
    def _():
        for n in range(8):
            start_copy(n, tm_next).wait_send()

    for ns, buffer, back, spot_of in routes:
        @pl.when((z_place == spot_of) & (tm < 24))
        def _(ns=ns, buffer=buffer, back=back):
            for n in ns:
                pass_copy(n, buffer, ns[0], back + 1).wait_send()

    for n in range(4):
        for j in range(PAIRS):
            pack_copy(n, j, True).wait_send()
    for n in range(2):
        for j in range(PAIRS):
            q2_copy(n, j, True).wait_send()
        for i in range(COLS // CHUNK):
            q3_copy(n, i, True).wait_send()
    give.wait_send()
    for i in range(COLS // CHUNK):
        item_copy(i).wait_send()
    for d in range(1, SPACE):
        for n in range(3):
            depth_copy(d, n, True).wait_send()
        for f in range(3):
            one_copy(f, lax.rem(s + d, SPACE), True).wait_send()
        row_copy(lax.rem(s + d, SPACE), True).wait_send()
    for sp in range(SPACE):
        fin_copy(sp, True).wait_send()

    @pl.loop(0, 16)
    def _(n):
        @pl.when((owner(s, 16 * k + n) != tm) & (chip < CHIPS - 1))
        def _():
            for f in range(3):
                two_copy(f, n).wait_send()

        each_halo(n, lambda x: x.wait_send())

        @pl.when((n > 0) & ((chip != n) | (half != k)))
        def _():
            ret_copy(n).wait_send()


def final_kernel(v, boosted, other, esum, partial, init, depth, out):
    slot = lax.axis_index("tm")
    even = lax.rem(slot, 2) == 0
    first = slot == 0

    def body(base):
        cols = pl.ds(base, CHUNK)
        d = wide(lambda c: depth[:, c], base)

        def stepped(state):
            h, u, w = state
            r = rates(h, u, w, d * u, d * w, left, right, up, down, lambda x: x)
            return [x + step_size * y for x, y in zip(state, r)]

        state = [wide(lambda c, f=f: v[f, :, c], base) for f in range(3)]
        a = stepped(state)
        b = stepped(a)
        for f in range(3):
            begin = inner(state[f])[:ROWS]
            ours = jnp.where(even, boosted[f, :, cols], other[f, :, cols])
            y1 = ours + inner(a[f])[:ROWS]
            y2 = esum[f, :, cols] + inner(b[f])[:ROWS]
            start = jnp.where(even, jnp.where(first, init[f, :, cols], begin), y1)
            end = jnp.where(even, y1, y2)
            out[0, f, :, cols] = start
            out[1, f, :, cols] = partial[f, :, cols] + 0.5 * (start + end)
            out[2, f, :, cols] = end

    chunks(body)


VM = pl.BlockSpec(memory_space=pltpu.VMEM)


def per_device(fine_nodes, init_state, mean_depth):
    points = fine_nodes[0].reshape(9, ROWS, COLS)
    state = jax.ShapeDtypeStruct((3, ROWS, COLS), F32)
    ring = jax.ShapeDtypeStruct((3, RING, COLS), F32)

    def vm(*shape):
        return pltpu.VMEM(shape, F32)

    def sems(*shape):
        return [pltpu.SemaphoreType.DMA(shape)] * 2

    flat, ringed = vm(3, ROWS, COLS), vm(3, RING, COLS)
    boosted, other, esum, partial, v, depth = pl.pallas_call(
        coarse_kernel,
        out_shape=[state, state, state, state, ring, jax.ShapeDtypeStruct((RING, COLS), F32)],
        in_specs=[pl.BlockSpec(memory_space=pltpu.HBM)] * 3,
        out_specs=[VM] * 6,
        scratch_shapes=[
            vm(9, ROWS, COLS), flat, vm(ROWS, COLS),
            flat, flat, flat, vm(2, 8, FOLD), vm(2, 8, FOLD), vm(2, 8, FOLD), vm(2, 8, FOLD),
            ringed, ringed, flat, ringed, vm(2, 8, FOLD), vm(2, 8, FOLD), ringed, vm(2, 8, COLS), vm(2, 8, COLS),
            ringed, flat, flat, vm(3, 3, ROWS, COLS // 8), vm(2, 3, ROWS, COLS // 8),
            vm(3, 128, PART), vm(3, PART, 128), vm(128, 512), vm(512, 128),
            vm(CHIPS, 3, WIDE, 128), vm(CHIPS, 3, OWN, 128), vm(3, PART, 128), vm(SPACE, 3, RING, PART),
            pltpu.SemaphoreType.DMA((5,)), *sems(8), *sems(8), *sems(4, 4), *sems(2, 4), *sems(2, 8), *sems(8), *sems(1), *sems(3, 8), *sems(3, 8), *sems(3, 16),
            *sems(4, 16), *sems(16), *sems(8), *sems(8),
        ],
        compiler_params=pltpu.CompilerParams(collective_id=0, has_side_effects=True, vmem_limit_bytes=36 << 20),
        name="sweep",
    )(*(pltpu.with_memory_space_constraint(x, pltpu.HBM) for x in (points, init_state, mean_depth)))

    out = pl.pallas_call(
        final_kernel,
        out_shape=jax.ShapeDtypeStruct((3, 3, ROWS, COLS), F32),
        in_specs=[VM] * 7,
        out_specs=VM,
        compiler_params=pltpu.CompilerParams(vmem_limit_bytes=24 << 20),
        name="final",
    )(v, boosted, other, esum, partial, init_state, depth)
    return out[None]


def solution(mesh):
    placed = (P("tm", None, None, "space", None), P(None, "space", None), P("space", None))
    return jax.shard_map(
        per_device,
        mesh=mesh,
        in_specs=placed,
        out_specs=P("tm", None, None, "space", None),
        check_vma=False,
    )
```

```python
import functools

import jax
import jax.numpy as jnp
from jax import lax
from jax.experimental import pallas as pl
from jax.experimental.pallas import tpu as pltpu
from jax.sharding import PartitionSpec as P

MESH = pl.DeviceIdType.MESH
F32 = jnp.float32

step_size = 0.3
viscosity = 1.0 / 3.0
coriolis = 0.5
quad_near = 5.0 / 24.0
quad_mid = 1.0 / 3.0
quad_far = -1.0 / 24.0
half_step = 0.5 * step_size
start_share = -(half_step + step_size / 3.0)
one_share = 2.0 * step_size / 3.0
two_share = half_step - step_size / 3.0

ROWS = 16
COLS = 4096
SPACE = 8
CHIPS = 16
PART = 256
OWN = 16
HALO = 32
WIDE = OWN + 2 * HALO


def rates(h, u, v, de, dn, left, right, up, down, centre):
    nh, nu, nv = viscosity * h, viscosity * u, viscosity * v
    he, hn, hh = 0.5 * de, 0.5 * dn, 0.5 * h
    nhc, nuc, nvc = centre(nh), centre(nu), centre(nv)
    hr = right(nh - he) + left(nh + he) + down(centre(nh - hn)) + up(centre(nh + hn)) - 4.0 * nhc
    ur = right(nu - hh) + left(nu + hh) + down(nuc) + up(nuc) - 4.0 * nuc + coriolis * centre(v)
    vr = right(nv) + left(nv) + down(centre(nv - hh)) + up(centre(nv + hh)) - 4.0 * nvc - coriolis * centre(u)
    return hr, ur, vr


CHUNK = 512
RING = 24


def edges(base):
    lo = pl.multiple_of(lax.rem(base + COLS - 128, COLS), 128)
    hi = pl.multiple_of(lax.rem(base + CHUNK, COLS), 128)
    return pl.ds(lo, 128), pl.ds(base, CHUNK), pl.ds(hi, 128)


def wide(get, base):
    return jnp.concatenate([get(c) for c in edges(base)], axis=1)


def right(x):
    return pltpu.roll(x, x.shape[1] - 1, 1)


def left(x):
    return pltpu.roll(x, 1, 1)


def down(x):
    return pltpu.roll(x, RING - 1, 0)


def up(x):
    return pltpu.roll(x, 1, 0)


def inner(x):
    return x[:, 128 : 128 + CHUNK]


def ring_rates(q, depth, base):
    h, u, v = (wide(lambda c, f=f: q[f, :, c], base) for f in range(3))
    d = wide(lambda c: depth[:, c], base)
    return rates(h, u, v, d * u, d * v, lambda x: inner(left(x)), lambda x: inner(right(x)), up, down, inner)


def chunks(body):
    @pl.loop(0, COLS // CHUNK)
    def _(i):
        body(pl.multiple_of(i * CHUNK, CHUNK))


PAIRS = COLS // CHUNK // 2
FOLD = COLS // 2


def pairs(body):
    @pl.loop(0, PAIRS)
    def _(j):
        base = pl.multiple_of(j * CHUNK, CHUNK)
        body(j, pl.ds(base, CHUNK), [base, pl.multiple_of(base + FOLD, CHUNK)])


def sub_roll(x, by):
    by %= 8
    return x if by == 0 else pltpu.roll(x, by, 0)


def pack(parts, at):
    row = lax.broadcasted_iota(jnp.int32, parts[0].shape, 0)
    tile = sub_roll(parts[0], -at)
    for i in range(1, len(parts)):
        tile = jnp.where(row >= 2 * i, sub_roll(parts[i], 2 * i - at), tile)
    return tile


def place(parts, at):
    row = lax.broadcasted_iota(jnp.int32, parts[0].shape, 0)
    tile = sub_roll(parts[0], -at[0])
    for i in range(1, len(parts)):
        tile = jnp.where(row >= i, sub_roll(parts[i], i - at[i]), tile)
    return tile


def fold(first, second):
    row = lax.broadcasted_iota(jnp.int32, first.shape, 0)
    return jnp.where(row < 4, first, sub_roll(second, 4))


def unfold(after, before, i):
    row = lax.broadcasted_iota(jnp.int32, after.shape, 0)
    return jnp.where(row < 4, sub_roll(after, -i), sub_roll(before, 7 - i))


def unpack(after, before, i):
    row = lax.broadcasted_iota(jnp.int32, after.shape, 0)
    return jnp.where(row < 4, sub_roll(after, -2 * i), sub_roll(before, 6 - 2 * i))


def snake(n):
    z, x = n // 4, lax.rem(n, 4)
    return z * 4 + jnp.where(lax.rem(z, 2) == 0, x, 3 - x)


def turned(s, chip):
    return chip // 4 * 4 + lax.rem(chip + 2 * lax.rem(s, 2), 4)


def owner(s, i):
    o = jnp.where(lax.rem(s, 2) == 0, i, 31 - i)
    return turned(s, snake(o // 2)) * 2 + lax.rem(o, 2)


def owned(s, tm):
    o = snake(turned(s, tm // 2)) * 2 + lax.rem(tm, 2)
    return jnp.where(lax.rem(s, 2) == 0, o, 31 - o)


def coarse_kernel(
    points_hbm, init_hbm, depth_hbm,
    out,
    boosted, other, esum, partial, vout, drow, points, init, depth, s0, a1, a2, ps, pr, fs, fr, s0r, q1, s1, q2, q2s, q2r, q3, q3s, q3r, br, item, ritem, relay_a, relay_b,
    rt, et, dr, dt, ex, vx, vt, vr,
    in_sem, st_s, st_r, rl_s, rl_r, pk_s, pk_r, q2_ss, q2_rs, q3_ss, q3_rs, it_s, it_r, oth_s, oth_r, one_s, one_r, dep_s, dep_r, two_s, two_r,
    halo_s, halo_r, ret_s, ret_r, row_s, row_r, fin_s, fin_r,
):
    tm = lax.axis_index("tm")
    s = lax.axis_index("space")
    chip, k = tm // 2, lax.rem(tm, 2)
    mine = owned(s, tm)
    half, spot = mine // 16, lax.rem(mine, 16)
    s_next, s_prev = lax.rem(s + 1, SPACE), lax.rem(s + SPACE - 1, SPACE)
    tm_next, tm_prev = lax.rem(tm + 1, 32), lax.rem(tm + 31, 32)
    first = jnp.where(tm == 0, 1.0, 0.0).astype(F32)

    def at(t, sp):
        return {"tm": t, "space": sp}

    def near(step):
        p = lax.rem(32 * s + mine + step + 256, 256)
        return at(owner(p // 32, lax.rem(p, 32)), p // 32)

    partner = at(chip * 2 + 1 - k, s)
    nears = [near(1), near(-1), near(2), near(-2)]

    loads = [pltpu.make_async_copy(points_hbm.at[3 * m : 3 * m + 3], points.at[3 * m : 3 * m + 3], in_sem.at[m]) for m in range(3)]
    loads += [pltpu.make_async_copy(init_hbm, init, in_sem.at[3]), pltpu.make_async_copy(depth_hbm, depth, in_sem.at[4])]
    for n in (2, 0, 1, 4, 3):
        loads[n].start()
    vt[...] = jnp.zeros_like(vt)
    barrier = pltpu.get_barrier_semaphore()
    peers = [at(lax.rem(tm + d, 32), s) for d in range(1, 32)]
    peers += [at(tm, lax.rem(s + d, SPACE)) for d in range(1, SPACE)]
    peers += [at(t, sp) for t in (tm_next, tm_prev) for sp in (s_next, s_prev)]
    peers += nears
    for p in peers:
        pl.semaphore_signal(barrier, inc=1, device_id=p, device_id_type=MESH)
    pl.semaphore_wait(barrier, len(peers))

    def copy(src, dst, ss, rs, dev):
        return pltpu.make_async_remote_copy(src_ref=src, dst_ref=dst, send_sem=ss, recv_sem=rs, device_id=dev, device_id_type=MESH)

    def block(sp, kk):
        return pl.ds(pl.multiple_of(512 * sp + 256 * kk, PART), PART)

    def rows(start, n=ROWS):
        return pl.ds(pl.multiple_of(start, 8), n)

    loads[2].wait()

    z_place = lax.rem(tm, 8)
    far_end = (z_place == 7) & (tm < 31)
    PIECE = COLS // 8
    direct, by_a, by_b = range(0, 2), range(2, 5), range(5, 8)
    routes = ((by_a, relay_a, 6, 1), (by_b, relay_b, 2, 5))

    def piece(n):
        return pl.ds(PIECE * n, PIECE)

    def start_copy(n, to):
        return copy(points.at[6:9, :, piece(n)], s0.at[:, :, piece(n)], st_s.at[n], st_r.at[n], at(to, s))

    def via_copy(n, buffer, first_piece, to):
        return copy(points.at[6:9, :, piece(n)], buffer.at[n - first_piece], st_s.at[n], rl_r.at[n], at(to, s))

    def pass_copy(n, buffer, first_piece, ahead):
        return copy(buffer.at[n - first_piece], s0.at[:, :, piece(n)], rl_s.at[n], st_r.at[n], at(lax.rem(tm + ahead, 32), s))

    @pl.when((tm < 31) & (z_place != 7))
    def _():
        for n in range(8):
            start_copy(n, tm_next).start()

    @pl.when(far_end)
    def _():
        for ns, buffer, back, _ in routes:
            for n in ns:
                via_copy(n, buffer, ns[0], lax.rem(tm + 32 - back, 32)).start()

    for n in (0, 1, 4, 3):
        loads[n].wait()

    def pack_copy(n, j, send):
        up_down = lax.rem(s + (1 if (n % 2 == 0) == send else SPACE - 1), SPACE)
        slot = tm if n < 2 else (tm_next if send else tm_prev)
        cols = pl.ds(pl.multiple_of(j * CHUNK, CHUNK), CHUNK)
        src, dst = (ps, pr) if n < 2 else (fs, fr)
        return copy(src.at[n % 2, :, cols], dst.at[n % 2, :, cols], pk_s.at[n, j], pk_r.at[n, j], at(slot, up_down))

    def prepare(j, folded, bases):
        tiles = [[], []], [[], []]
        for base in bases:
            cols = pl.ds(base, CHUNK)
            top, bottom = [], []
            for f in range(3):
                p0, p1, p2 = (points[3 * m + f, :, cols] for m in range(3))
                x = (step_size * quad_near - half_step) * p0 + (step_size * quad_mid) * p1 + (step_size * quad_far) * p2
                y = (step_size * quad_far) * p0 + (step_size * quad_mid - half_step) * p1 + (step_size * quad_near) * p2
                a1[f, :, cols] = x
                a2[f, :, cols] = y
                top.append(x[:8])
                bottom.append(x[8:])
            for n, (parts, tile, row, inside) in enumerate(((bottom, 8, 7, 6), (top, 0, 0, 1))):
                d = depth[tile : tile + 8, cols]
                ends = [
                    jnp.where(tm == 31, init[f, tile : tile + 8, cols], points[6 + f, tile : tile + 8, cols]) for f in range(3)
                ]
                tiles[0][n].append(place(parts + [d], [row] * 4))
                tiles[1][n].append(place(ends + [d], [row] * 3 + [inside]))
        for n in range(2):
            ps[n, :, folded] = fold(*tiles[0][n])
            fs[n, :, folded] = fold(*tiles[1][n])
        for n in range(4):
            pack_copy(n, j, True).start()

    pairs(prepare)

    @pl.when(far_end)
    def _():
        for n in direct:
            start_copy(n, tm_next).start()

    for ns, buffer, back, spot_of in routes:
        @pl.when((z_place == spot_of) & (tm < 24))
        def _(ns=ns, buffer=buffer, back=back):
            for n in ns:
                via_copy(n, buffer, ns[0], lax.rem(tm + back, 32)).wait_recv()
                pass_copy(n, buffer, ns[0], back + 1).start()

    for n in range(4):
        for j in range(PAIRS):
            pack_copy(n, j, False).wait_recv()

    @pl.when(tm > 0)
    def _():
        for n in range(8):
            start_copy(n, tm_prev).wait_recv()

    def ringed(j, folded, bases):
        row = lax.broadcasted_iota(jnp.int32, (8, CHUNK), 0)
        for h, base in enumerate(bases):
            cols = pl.ds(base, CHUNK)
            pa, pb, fa, fb = pr[1, :, folded], pr[0, :, folded], fr[1, :, folded], fr[0, :, folded]
            i = 4 * h + 3
            d = jnp.where(row < 4, sub_roll(fa, 1 - i), sub_roll(fb, 6 - i))
            d = jnp.where((row == 0) | (row == 7), unfold(pa, pb, i), d)
            drow[:, cols] = jnp.concatenate([depth[:, cols], d], axis=0)
            for f in range(3):
                main = jnp.where(tm == 0, init[f, :, cols], s0[f, :, cols])
                x = jnp.concatenate([main, unfold(fa, fb, 4 * h + f)], axis=0)
                y = jnp.concatenate([a1[f, :, cols], unfold(pa, pb, 4 * h + f)], axis=0)
                s0r[f, :, cols] = x
                q1[f, :, cols] = half_step * x + y

    pairs(ringed)

    def q2_copy(n, j, send):
        up_down = lax.rem(s + (1 if (n == 0) == send else SPACE - 1), SPACE)
        cols = pl.ds(pl.multiple_of(j * CHUNK, CHUNK), CHUNK)
        return copy(q2s.at[n, :, cols], q2r.at[n, :, cols], q2_ss.at[n, j], q2_rs.at[n, j], at(tm, up_down))

    def one(j, folded, bases):
        tiles = [[], []]
        for base in bases:
            cols = pl.ds(base, CHUNK)
            r = ring_rates(q1, drow, base)
            q = []
            for f in range(3):
                x = s0r[f, :ROWS, cols] + r[f][:ROWS]
                s1[f, :, cols] = x
                q.append(half_step * x + a2[f, :, cols])
                q2[f, :ROWS, cols] = q[f]
            tiles[0].append(place([x[8:] for x in q], [7] * 3))
            tiles[1].append(place([x[:8] for x in q], [0] * 3))
        for n in range(2):
            q2s[n, :, folded] = fold(*tiles[n])
            q2_copy(n, j, True).start()

    pairs(one)
    for n in range(2):
        for j in range(PAIRS):
            q2_copy(n, j, False).wait_recv()

    def q2_rows(j, folded, bases):
        for h, base in enumerate(bases):
            for f in range(3):
                q2[f, ROWS:, pl.ds(base, CHUNK)] = unfold(q2r[1, :, folded], q2r[0, :, folded], 4 * h + f)

    pairs(q2_rows)

    def q3_copy(n, j, send):
        up_down = lax.rem(s + (1 if (n % 2 == 0) == send else SPACE - 1), SPACE)
        cols = pl.ds(pl.multiple_of(j * CHUNK, CHUNK), CHUNK)
        return copy(q3s.at[n, :, cols], q3r.at[n, :, cols], q3_ss.at[n, j], q3_rs.at[n, j], at(tm, up_down))

    def two(j, folded, bases):
        tiles = [[], [], [], []]
        for base in bases:
            cols = pl.ds(base, CHUNK)
            r = ring_rates(q2, drow, base)
            top, bottom = [], []
            for f in range(3):
                x, y = s0r[f, :ROWS, cols], s1[f, :, cols]
                z = y + r[f][:ROWS]
                partial[f, :, cols] = y - 0.5 * (x + z)
                q = (step_size * first + start_share) * x + one_share * y + two_share * z
                q3[f, :ROWS, cols] = q
                top.append(q[:8])
                bottom.append(q[8:])
            for n, (parts, row) in enumerate(((bottom, 7), (top, 0), (bottom, 6), (top, 1))):
                tiles[n].append(place(parts, [row] * 3))
        for n in range(4):
            q3s[n, :, folded] = fold(*tiles[n])
        for n in range(2):
            q3_copy(n, j, True).start()

        @pl.when(k == 0)
        def _():
            for n in range(2, 4):
                q3_copy(n, j, True).start()

    pairs(two)
    for n in range(2):
        for j in range(PAIRS):
            q3_copy(n, j, False).wait_recv()

    @pl.when(k == 0)
    def _():
        for n in range(2, 4):
            for j in range(PAIRS):
                q3_copy(n, j, False).wait_recv()

    def q3_rows(j, folded, bases):
        row = lax.broadcasted_iota(jnp.int32, (8, CHUNK), 0)
        for h, base in enumerate(bases):
            for f in range(3):
                i = 4 * h + f
                near_rows = unfold(q3r[1, :, folded], q3r[0, :, folded], i)
                far_rows = jnp.where(row < 4, sub_roll(q3r[3, :, folded], 1 - i), sub_roll(q3r[2, :, folded], 6 - i))
                q3[f, ROWS:, pl.ds(base, CHUNK)] = jnp.where((row == 0) | (row == 7), near_rows, far_rows)

    pairs(q3_rows)

    def three(base):
        cols = pl.ds(base, CHUNK)
        r = ring_rates(q3, drow, base)
        for f in range(3):
            x = r[f] + first * s0r[f, :, cols]
            br[f, :, cols] = x
            boosted[f, :, cols] = x[:ROWS]

    chunks(three)
    give = copy(boosted, other, oth_s.at[0], oth_r.at[0], partner)

    def item_copy(i):
        cols = pl.ds(pl.multiple_of(i * CHUNK, CHUNK), CHUNK)
        return copy(item.at[:, :, cols], ritem.at[:, :, cols], it_s.at[i], it_r.at[i], partner)

    @pl.loop(0, COLS // CHUNK)
    def _(i):
        base = pl.multiple_of(i * CHUNK, CHUNK)
        cols = pl.ds(base, CHUNK)
        r = ring_rates(br, drow, base)
        for f in range(3):
            item[f, :, cols] = jnp.where(k == 0, boosted[f, :, cols] + step_size * r[f][:ROWS], boosted[f, :, cols])
        item_copy(i).start()

    give.start()

    def one_copy(f, sp, send):
        to, by = (sp, s) if send else (s, sp)
        n = to if send else by
        return copy(esum.at[f, :, block(to, k)], rt.at[f, rows(ROWS * by), :], one_s.at[f, n], one_r.at[f, by], at(tm, sp))

    for i in range(COLS // CHUNK):
        item_copy(i).wait_recv()

    def summed(base):
        cols = pl.ds(base, CHUNK)
        for f in range(3):
            esum[f, :, cols] = item[f, :, cols] + ritem[f, :, cols]

    chunks(summed)
    for f in range(3):
        for d in range(1, SPACE):
            one_copy(f, lax.rem(s + d, SPACE), True).start()
    rt[:, rows(ROWS * s), :] = esum[:, :, block(s, k)]

    def depth_pieces(base):
        return (
            (pl.ds(pl.multiple_of(base, 128), PART), pl.ds(128, PART)),
            (pl.ds(pl.multiple_of(lax.rem(base + COLS - 128, COLS), 128), 128), pl.ds(0, 128)),
            (pl.ds(pl.multiple_of(lax.rem(base + PART, COLS), 128), 128), pl.ds(384, 128)),
        )

    def depth_copy(d, n, send):
        sp = lax.rem(s + d, SPACE) if send else lax.rem(s + SPACE - d, SPACE)
        to = sp if send else s
        src, dst = depth_pieces(512 * to + 256 * (owned(to, tm) // 16))[n]
        return copy(depth.at[:, src], dr.at[rows(ROWS * (s if send else sp)), dst], dep_s.at[n, d], dep_r.at[n, d], at(tm, sp))

    for d in range(1, SPACE):
        for n in range(3):
            depth_copy(d, n, True).start()
    for src, dst in depth_pieces(512 * s + 256 * half):
        dr[rows(ROWS * s), dst] = depth[:, src]


    def two_copy(f, n):
        src, dst = et.at[f, rows(OWN * n, OWN), :], ex.at[chip, f, pl.ds(HALO, OWN), :]
        return copy(src, dst, two_s.at[f, n], two_r.at[f, chip], at(owner(s, 16 * k + n), s))

    for f in range(3):
        for d in range(1, SPACE):
            one_copy(f, lax.rem(s + SPACE - d, SPACE), False).wait_recv()
        for t in range(2):
            et[f, 128 * t : 128 * t + 128, :] = rt[f, :, 128 * t : 128 * t + 128].T

        @pl.loop(0, 16)
        def _(m, f=f):
            n = lax.rem(m + spot, 16)

            @pl.when((owner(s, 16 * k + n) != tm) & (chip < CHIPS - 1))
            def _():
                two_copy(f, n).start()

    @pl.when(half == k)
    def _():
        ex[chip, :, HALO : HALO + OWN, :] = et[:, rows(OWN * spot, OWN), :]

    def halo_copy(n, j, width):
        hop, sign = n // 2 + 1, 1 - 2 * (n % 2)
        far = OWN * (hop - 1)
        if sign > 0:
            src, dst = HALO + OWN - width, HALO - far - width
        else:
            src, dst = HALO, HALO + OWN + far
        return copy(ex.at[j, :, pl.ds(src, width), :], ex.at[j, :, pl.ds(dst, width), :], halo_s.at[n, j], halo_r.at[n, j], nears[n])

    def each_halo(j, act):
        for lo, hi, ns, width in ((0, 10, (0, 1), 16), (10, 14, (0, 1), 8), (0, 2, (2, 3), 16), (2, 6, (2, 3), 8)):
            @pl.when((j >= lo) & (j < hi))
            def _():
                for n in ns:
                    act(halo_copy(n, j, width))

    for c in (0, 1, 2, 5, 6, 9, 10, 13, 14, 3, 11, 7, 4, 8, 12):
        @pl.when((chip != c) | (half != k))
        def _(c=c):
            for f in range(3):
                src, dst = et.at[f, rows(OWN * spot, OWN), :], ex.at[c, f, pl.ds(HALO, OWN), :]
                copy(src, dst, two_s.at[f, 0], two_r.at[f, c], at(c * 2 + half, s)).wait_recv()

        for lo, hi, ns, width in ((0, 10, (0, 1), 16), (10, 14, (0, 1), 8), (0, 2, (2, 3), 16), (2, 6, (2, 3), 8)):
            if lo <= c < hi:
                for n in ns:
                    halo_copy(n, c, width).start()

    for d in range(1, SPACE):
        for n in range(3):
            depth_copy(d, n, False).wait_recv()
    for t in range(4):
        dt[128 * t : 128 * t + 128, :] = dr[:, 128 * t : 128 * t + 128].T


    def scanned(lo, hi, halo, state):
        count = OWN + 2 * halo
        d_own = dt[rows(128 - halo + OWN * spot, count), :]

        def stepped(state):
            h, u, v = state
            r = rates(
                h, u, v, d_own * u, d_own * v,
                lambda x: pltpu.roll(x, 1, 0), lambda x: pltpu.roll(x, count - 1, 0),
                lambda x: pltpu.roll(x, 1, 1), lambda x: pltpu.roll(x, 127, 1), lambda x: x,
            )
            return tuple(x + step_size * y for x, y in zip(state, r))

        def body(j, state):
            state = stepped(stepped(state))
            each_halo(j, lambda x: x.wait_recv())
            state = tuple(x + ex[j, f, HALO - halo : HALO + OWN + halo] for f, x in enumerate(state))
            for f in range(3):
                vx[j + 1, f] = state[f][halo : halo + OWN]

            @pl.when((chip != j + 1) | (half != k))
            def _():
                ret_copy(j + 1).start()

            return state

        return lax.fori_loop(lo, hi, body, state)

    def ret_copy(j):
        return copy(vx.at[j], vt.at[:, rows(OWN * spot, OWN), :], ret_s.at[j], ret_r.at[spot], at(j * 2 + half, s))

    state = scanned(0, 7, 32, (jnp.zeros((WIDE, 128), F32),) * 3)
    state = scanned(7, 11, 16, tuple(x[16:64] for x in state))
    scanned(11, CHIPS - 1, 8, tuple(x[8:40] for x in state))

    @pl.when(tm < 31)
    def _():
        for n in range(8):
            start_copy(n, tm_next).wait_send()

    for ns, buffer, back, spot_of in routes:
        @pl.when((z_place == spot_of) & (tm < 24))
        def _(ns=ns, buffer=buffer, back=back):
            for n in ns:
                pass_copy(n, buffer, ns[0], back + 1).wait_send()

    for n in range(4):
        for j in range(PAIRS):
            pack_copy(n, j, True).wait_send()
    for n in range(2):
        for j in range(PAIRS):
            q2_copy(n, j, True).wait_send()
            q3_copy(n, j, True).wait_send()

    @pl.when(k == 0)
    def _():
        for n in range(2, 4):
            for j in range(PAIRS):
                q3_copy(n, j, True).wait_send()

    give.wait_send()
    for i in range(COLS // CHUNK):
        item_copy(i).wait_send()
    for d in range(1, SPACE):
        for n in range(3):
            depth_copy(d, n, True).wait_send()
        for f in range(3):
            one_copy(f, lax.rem(s + d, SPACE), True).wait_send()

    @pl.loop(0, 16)
    def _(n):
        @pl.when((owner(s, 16 * k + n) != tm) & (chip < CHIPS - 1))
        def _():
            for f in range(3):
                two_copy(f, n).wait_send()

        each_halo(n, lambda x: x.wait_send())

    @pl.when(chip > 0)
    def _():
        @pl.when(half == k)
        def _():
            vt[:, rows(OWN * spot, OWN), :] = vx[chip]

        @pl.loop(0, 16)
        def _(n):
            t = owner(s, 16 * k + n)

            @pl.when(t != tm)
            def _():
                copy(vx.at[0], vt.at[:, rows(OWN * n, OWN), :], ret_s.at[0], ret_r.at[n], at(t, s)).wait_recv()

    low = lax.broadcasted_iota(jnp.int32, (8, 128), 0) < 4
    for f in range(3):
        for t in range(2):
            cols = slice(128 * t, 128 * t + 128)
            x = vt[f, cols, :].T
            for sp in range(SPACE):
                vr[sp, f, :ROWS, cols] = x[16 * sp : 16 * sp + 16]
                a, b = (16 * sp + 16) % 128, (16 * sp + 120) % 128
                vr[sp, f, ROWS:, cols] = jnp.where(low, x[a : a + 8], x[b : b + 8])

    def row_copy(sp, send):
        to, by = (sp, s) if send else (s, sp)
        return copy(vr.at[to], vout.at[:, :, block(by, k)], row_s.at[sp], row_r.at[by], at(tm, sp))

    def fin_copy(sp, send):
        cols = block(sp, k if send else 1 - k)
        return copy(vout.at[:, :, cols], vout.at[:, :, cols], fin_s.at[sp], fin_r.at[sp], partner)

    for d in range(1, SPACE):
        row_copy(lax.rem(s + d, SPACE), True).start()
    vout[:, :, block(s, k)] = vr[s]
    fin_copy(s, True).start()
    give.wait_recv()

    def finish(sp):
        base = pl.multiple_of(sp * CHUNK, CHUNK)
        cols = pl.ds(base, CHUNK)
        d = wide(lambda c: drow[:, c], base)

        def stepped(state):
            h, u, w = state
            r = rates(h, u, w, d * u, d * w, left, right, up, down, lambda x: x)
            return [x + step_size * y for x, y in zip(state, r)]

        state = [wide(lambda c, f=f: vout[f, :, c], base) for f in range(3)]
        a = stepped(state)
        b = stepped(a)
        for f in range(3):
            begin = inner(state[f])[:ROWS]
            ours = jnp.where(k == 0, boosted[f, :, cols], other[f, :, cols])
            y1 = ours + inner(a[f])[:ROWS]
            y2 = esum[f, :, cols] + inner(b[f])[:ROWS]
            start = jnp.where(k == 0, jnp.where(tm == 0, init[f, :, cols], begin), y1)
            end = jnp.where(k == 0, y1, y2)
            out[0, f, :, cols] = start
            out[1, f, :, cols] = partial[f, :, cols] + 0.5 * (start + end)
            out[2, f, :, cols] = end

    @pl.loop(1, SPACE)
    def _(d):
        sp = lax.rem(s + SPACE - d, SPACE)
        row_copy(sp, False).wait_recv()
        fin_copy(sp, True).start()
        fin_copy(lax.rem(sp + 1, SPACE), False).wait_recv()

        @pl.when(d >= 3)
        def _():
            finish(lax.rem(sp + 2, SPACE))

    fin_copy(lax.rem(s + 1, SPACE), False).wait_recv()

    @pl.loop(0, 3)
    def _(i):
        finish(lax.rem(s + 2 * SPACE - 6 - i, SPACE))

    for d in range(1, SPACE):
        row_copy(lax.rem(s + d, SPACE), True).wait_send()
    for sp in range(SPACE):
        fin_copy(sp, True).wait_send()

    @pl.loop(1, 16)
    def _(n):
        @pl.when((chip != n) | (half != k))
        def _():
            ret_copy(n).wait_send()


VM = pl.BlockSpec(memory_space=pltpu.VMEM)


def per_device(fine_nodes, init_state, mean_depth):
    points = fine_nodes[0].reshape(9, ROWS, COLS)

    def vm(*shape):
        return pltpu.VMEM(shape, F32)

    def sems(*shape):
        return [pltpu.SemaphoreType.DMA(shape)] * 2

    flat, ringed = vm(3, ROWS, COLS), vm(3, RING, COLS)
    out = pl.pallas_call(
        coarse_kernel,
        out_shape=jax.ShapeDtypeStruct((3, 3, ROWS, COLS), F32),
        in_specs=[pl.BlockSpec(memory_space=pltpu.HBM)] * 3,
        out_specs=VM,
        scratch_shapes=[
            flat, flat, flat, flat, ringed, vm(RING, COLS), vm(9, ROWS, COLS), flat, vm(ROWS, COLS),
            flat, flat, flat, vm(2, 8, FOLD), vm(2, 8, FOLD), vm(2, 8, FOLD), vm(2, 8, FOLD),
            ringed, ringed, flat, ringed, vm(2, 8, FOLD), vm(2, 8, FOLD), ringed, vm(4, 8, FOLD), vm(4, 8, FOLD),
            ringed, flat, flat, vm(3, 3, ROWS, COLS // 8), vm(3, 3, ROWS, COLS // 8),
            vm(3, 128, PART), vm(3, PART, 128), vm(128, 512), vm(512, 128),
            vm(CHIPS, 3, WIDE, 128), vm(CHIPS, 3, OWN, 128), vm(3, PART, 128), vm(SPACE, 3, RING, PART),
            pltpu.SemaphoreType.DMA((5,)), *sems(8), *sems(8), *sems(4, 4), *sems(2, 4), *sems(4, 4), *sems(8), *sems(1), *sems(3, 8), *sems(3, 8), *sems(3, 16),
            *sems(4, 16), *sems(16), *sems(8), *sems(8),
        ],
        compiler_params=pltpu.CompilerParams(collective_id=0, has_side_effects=True, vmem_limit_bytes=40 << 20),
        name="sweep",
    )(*(pltpu.with_memory_space_constraint(x, pltpu.HBM) for x in (points, init_state, mean_depth)))
    return out[None]


def solution(mesh):
    placed = (P("tm", None, None, "space", None), P(None, "space", None), P("space", None))
    return jax.shard_map(
        per_device,
        mesh=mesh,
        in_specs=placed,
        out_specs=P("tm", None, None, "space", None),
        check_vma=False,
    )
```

```python
import functools

import jax
import jax.numpy as jnp
from jax import lax
from jax.experimental import pallas as pl
from jax.experimental.pallas import tpu as pltpu
from jax.sharding import PartitionSpec as P

MESH = pl.DeviceIdType.MESH
F32 = jnp.float32

step_size = 0.3
viscosity = 1.0 / 3.0
coriolis = 0.5
quad_near = 5.0 / 24.0
quad_mid = 1.0 / 3.0
quad_far = -1.0 / 24.0
half_step = 0.5 * step_size
start_share = -(half_step + step_size / 3.0)
one_share = 2.0 * step_size / 3.0
two_share = half_step - step_size / 3.0

ROWS = 16
COLS = 4096
SPACE = 8
CHIPS = 16
PART = 256
OWN = 16
HALO = 32
WIDE = OWN + 2 * HALO


def rates(h, u, v, de, dn, left, right, up, down, centre):
    nh, nu, nv = viscosity * h, viscosity * u, viscosity * v
    he, hn, hh = 0.5 * de, 0.5 * dn, 0.5 * h
    nhc, nuc, nvc = centre(nh), centre(nu), centre(nv)
    hr = right(nh - he) + left(nh + he) + down(centre(nh - hn)) + up(centre(nh + hn)) - 4.0 * nhc
    ur = right(nu - hh) + left(nu + hh) + down(nuc) + up(nuc) - 4.0 * nuc + coriolis * centre(v)
    vr = right(nv) + left(nv) + down(centre(nv - hh)) + up(centre(nv + hh)) - 4.0 * nvc - coriolis * centre(u)
    return hr, ur, vr


CHUNK = 512
RING = 24


def edges(base):
    lo = pl.multiple_of(lax.rem(base + COLS - 128, COLS), 128)
    hi = pl.multiple_of(lax.rem(base + CHUNK, COLS), 128)
    return pl.ds(lo, 128), pl.ds(base, CHUNK), pl.ds(hi, 128)


def wide(get, base):
    return jnp.concatenate([get(c) for c in edges(base)], axis=1)


def right(x):
    return pltpu.roll(x, x.shape[1] - 1, 1)


def left(x):
    return pltpu.roll(x, 1, 1)


def down(x):
    return pltpu.roll(x, RING - 1, 0)


def up(x):
    return pltpu.roll(x, 1, 0)


def inner(x):
    return x[:, 128 : 128 + CHUNK]


def ring_rates(q, depth, base):
    h, u, v = (wide(lambda c, f=f: q[f, :, c], base) for f in range(3))
    d = wide(lambda c: depth[:, c], base)
    return rates(h, u, v, d * u, d * v, lambda x: inner(left(x)), lambda x: inner(right(x)), up, down, inner)


def chunks(body):
    @pl.loop(0, COLS // CHUNK)
    def _(i):
        body(pl.multiple_of(i * CHUNK, CHUNK))


PAIRS = COLS // CHUNK // 2
FOLD = COLS // 2


def pairs(body):
    @pl.loop(0, PAIRS)
    def _(j):
        base = pl.multiple_of(j * CHUNK, CHUNK)
        body(j, pl.ds(base, CHUNK), [base, pl.multiple_of(base + FOLD, CHUNK)])


def sub_roll(x, by):
    by %= 8
    return x if by == 0 else pltpu.roll(x, by, 0)


def pack(parts, at):
    row = lax.broadcasted_iota(jnp.int32, parts[0].shape, 0)
    tile = sub_roll(parts[0], -at)
    for i in range(1, len(parts)):
        tile = jnp.where(row >= 2 * i, sub_roll(parts[i], 2 * i - at), tile)
    return tile


def place(parts, at):
    row = lax.broadcasted_iota(jnp.int32, parts[0].shape, 0)
    tile = sub_roll(parts[0], -at[0])
    for i in range(1, len(parts)):
        tile = jnp.where(row >= i, sub_roll(parts[i], i - at[i]), tile)
    return tile


def fold(first, second):
    row = lax.broadcasted_iota(jnp.int32, first.shape, 0)
    return jnp.where(row < 4, first, sub_roll(second, 4))


def unfold(after, before, i):
    row = lax.broadcasted_iota(jnp.int32, after.shape, 0)
    return jnp.where(row < 4, sub_roll(after, -i), sub_roll(before, 7 - i))


def unpack(after, before, i):
    row = lax.broadcasted_iota(jnp.int32, after.shape, 0)
    return jnp.where(row < 4, sub_roll(after, -2 * i), sub_roll(before, 6 - 2 * i))


def snake(n):
    z, x = n // 4, lax.rem(n, 4)
    return z * 4 + jnp.where(lax.rem(z, 2) == 0, x, 3 - x)


def turned(s, chip):
    return chip // 4 * 4 + lax.rem(chip + 2 * lax.rem(s, 2), 4)


def owner(s, i):
    o = jnp.where(lax.rem(s, 2) == 0, i, 31 - i)
    return turned(s, snake(o // 2)) * 2 + lax.rem(o, 2)


def owned(s, tm):
    o = snake(turned(s, tm // 2)) * 2 + lax.rem(tm, 2)
    return jnp.where(lax.rem(s, 2) == 0, o, 31 - o)


def coarse_kernel(
    points_hbm, init_hbm, depth_hbm,
    out,
    boosted, other, esum, partial, vout, drow, points, init, depth, s0, a1, a2, ps, pr, fs, fr, s0r, q1, s1, q2, q2s, q2r, q3, q3s, q3r, br, item, ritem, relay_a, relay_b, relay_c,
    rt, et, dr, dt, ex, vx, vt, vr,
    in_sem, st_s, st_r, rl_s, rl_r, pk_s, pk_r, q2_ss, q2_rs, q3_ss, q3_rs, it_s, it_r, oth_s, oth_r, one_s, one_r, dep_s, dep_r, two_s, two_r,
    halo_s, halo_r, ret_s, ret_r, row_s, row_r, fin_s, fin_r,
):
    tm = lax.axis_index("tm")
    s = lax.axis_index("space")
    chip, k = tm // 2, lax.rem(tm, 2)
    mine = owned(s, tm)
    half, spot = mine // 16, lax.rem(mine, 16)
    s_next, s_prev = lax.rem(s + 1, SPACE), lax.rem(s + SPACE - 1, SPACE)
    tm_next, tm_prev = lax.rem(tm + 1, 32), lax.rem(tm + 31, 32)
    first = jnp.where(tm == 0, 1.0, 0.0).astype(F32)

    def at(t, sp):
        return {"tm": t, "space": sp}

    def near(step):
        p = lax.rem(32 * s + mine + step + 256, 256)
        return at(owner(p // 32, lax.rem(p, 32)), p // 32)

    partner = at(chip * 2 + 1 - k, s)
    nears = [near(1), near(-1), near(2), near(-2)]

    loads = [pltpu.make_async_copy(points_hbm.at[3 * m : 3 * m + 3], points.at[3 * m : 3 * m + 3], in_sem.at[m]) for m in range(3)]
    loads += [pltpu.make_async_copy(init_hbm, init, in_sem.at[3]), pltpu.make_async_copy(depth_hbm, depth, in_sem.at[4])]
    for n in (2, 0, 1, 4, 3):
        loads[n].start()
    vt[...] = jnp.zeros_like(vt)
    barrier = pltpu.get_barrier_semaphore()
    peers = [at(lax.rem(tm + d, 32), s) for d in range(1, 32)]
    peers += [at(tm, lax.rem(s + d, SPACE)) for d in range(1, SPACE)]
    peers += [at(t, sp) for t in (tm_next, tm_prev) for sp in (s_next, s_prev)]
    peers += nears
    for p in peers:
        pl.semaphore_signal(barrier, inc=1, device_id=p, device_id_type=MESH)
    pl.semaphore_wait(barrier, len(peers))

    def copy(src, dst, ss, rs, dev):
        return pltpu.make_async_remote_copy(src_ref=src, dst_ref=dst, send_sem=ss, recv_sem=rs, device_id=dev, device_id_type=MESH)

    def block(sp, kk):
        return pl.ds(pl.multiple_of(512 * sp + 256 * kk, PART), PART)

    def rows(start, n=ROWS):
        return pl.ds(pl.multiple_of(start, 8), n)

    loads[2].wait()

    z_place = lax.rem(tm, 8)
    far_end = (z_place == 7) & (tm < 31)
    PIECE = COLS // 8
    direct = range(0, 2)
    routes = ((range(2, 4), relay_a, 6, 1), (range(4, 6), relay_b, 2, 5), (range(6, 8), relay_c, 4, 3))

    def piece(n):
        return pl.ds(PIECE * n, PIECE)

    def start_copy(n, to):
        return copy(points.at[6:9, :, piece(n)], s0.at[:, :, piece(n)], st_s.at[n], st_r.at[n], at(to, s))

    def via_copy(n, buffer, first_piece, to):
        return copy(points.at[6:9, :, piece(n)], buffer.at[n - first_piece], st_s.at[n], rl_r.at[n], at(to, s))

    def pass_copy(n, buffer, first_piece, ahead):
        return copy(buffer.at[n - first_piece], s0.at[:, :, piece(n)], rl_s.at[n], st_r.at[n], at(lax.rem(tm + ahead, 32), s))

    @pl.when((tm < 31) & (z_place != 7))
    def _():
        for n in range(8):
            start_copy(n, tm_next).start()

    @pl.when(far_end)
    def _():
        for ns, buffer, back, _ in routes:
            for n in ns:
                via_copy(n, buffer, ns[0], lax.rem(tm + 32 - back, 32)).start()

    for n in (0, 1, 4, 3):
        loads[n].wait()

    def pack_copy(n, j, send):
        up_down = lax.rem(s + (1 if (n % 2 == 0) == send else SPACE - 1), SPACE)
        slot = tm if n < 2 else (tm_next if send else tm_prev)
        cols = pl.ds(pl.multiple_of(j * CHUNK, CHUNK), CHUNK)
        src, dst = (ps, pr) if n < 2 else (fs, fr)
        return copy(src.at[n % 2, :, cols], dst.at[n % 2, :, cols], pk_s.at[n, j], pk_r.at[n, j], at(slot, up_down))

    def prepare(j, folded, bases):
        tiles = [[], []], [[], []]
        for base in bases:
            cols = pl.ds(base, CHUNK)
            top, bottom = [], []
            for f in range(3):
                p0, p1, p2 = (points[3 * m + f, :, cols] for m in range(3))
                x = (step_size * quad_near - half_step) * p0 + (step_size * quad_mid) * p1 + (step_size * quad_far) * p2
                y = (step_size * quad_far) * p0 + (step_size * quad_mid - half_step) * p1 + (step_size * quad_near) * p2
                a1[f, :, cols] = x
                a2[f, :, cols] = y
                top.append(x[:8])
                bottom.append(x[8:])
            for n, (parts, tile, row, inside) in enumerate(((bottom, 8, 7, 6), (top, 0, 0, 1))):
                d = depth[tile : tile + 8, cols]
                ends = [
                    jnp.where(tm == 31, init[f, tile : tile + 8, cols], points[6 + f, tile : tile + 8, cols]) for f in range(3)
                ]
                tiles[0][n].append(place(parts + [d], [row] * 4))
                tiles[1][n].append(place(ends + [d], [row] * 3 + [inside]))
        for n in range(2):
            ps[n, :, folded] = fold(*tiles[0][n])
            fs[n, :, folded] = fold(*tiles[1][n])
        for n in range(2, 4):
            pack_copy(n, j, True).start()

    pairs(prepare)

    @pl.when(far_end)
    def _():
        for n in direct:
            start_copy(n, tm_next).start()

    for n in range(2):
        for j in range(PAIRS):
            pack_copy(n, j, True).start()

    for ns, buffer, back, spot_of in routes:
        @pl.when((z_place == spot_of) & (tm < 24))
        def _(ns=ns, buffer=buffer, back=back):
            for n in ns:
                via_copy(n, buffer, ns[0], lax.rem(tm + back, 32)).wait_recv()
                pass_copy(n, buffer, ns[0], back + 1).start()

    for n in range(4):
        for j in range(PAIRS):
            pack_copy(n, j, False).wait_recv()

    @pl.when(tm > 0)
    def _():
        for n in range(8):
            start_copy(n, tm_prev).wait_recv()

    def ringed(j, folded, bases):
        row = lax.broadcasted_iota(jnp.int32, (8, CHUNK), 0)
        for h, base in enumerate(bases):
            cols = pl.ds(base, CHUNK)
            pa, pb, fa, fb = pr[1, :, folded], pr[0, :, folded], fr[1, :, folded], fr[0, :, folded]
            i = 4 * h + 3
            d = jnp.where(row < 4, sub_roll(fa, 1 - i), sub_roll(fb, 6 - i))
            d = jnp.where((row == 0) | (row == 7), unfold(pa, pb, i), d)
            drow[:, cols] = jnp.concatenate([depth[:, cols], d], axis=0)
            for f in range(3):
                main = jnp.where(tm == 0, init[f, :, cols], s0[f, :, cols])
                x = jnp.concatenate([main, unfold(fa, fb, 4 * h + f)], axis=0)
                y = jnp.concatenate([a1[f, :, cols], unfold(pa, pb, 4 * h + f)], axis=0)
                s0r[f, :, cols] = x
                q1[f, :, cols] = half_step * x + y

    pairs(ringed)

    def q2_copy(n, j, send):
        up_down = lax.rem(s + (1 if (n == 0) == send else SPACE - 1), SPACE)
        cols = pl.ds(pl.multiple_of(j * CHUNK, CHUNK), CHUNK)
        return copy(q2s.at[n, :, cols], q2r.at[n, :, cols], q2_ss.at[n, j], q2_rs.at[n, j], at(tm, up_down))

    def one(j, folded, bases):
        tiles = [[], []]
        for base in bases:
            cols = pl.ds(base, CHUNK)
            r = ring_rates(q1, drow, base)
            q = []
            for f in range(3):
                x = s0r[f, :ROWS, cols] + r[f][:ROWS]
                s1[f, :, cols] = x
                q.append(half_step * x + a2[f, :, cols])
                q2[f, :ROWS, cols] = q[f]
            tiles[0].append(place([x[8:] for x in q], [7] * 3))
            tiles[1].append(place([x[:8] for x in q], [0] * 3))
        for n in range(2):
            q2s[n, :, folded] = fold(*tiles[n])
            q2_copy(n, j, True).start()

    pairs(one)
    for n in range(2):
        for j in range(PAIRS):
            q2_copy(n, j, False).wait_recv()

    def q2_rows(j, folded, bases):
        for h, base in enumerate(bases):
            for f in range(3):
                q2[f, ROWS:, pl.ds(base, CHUNK)] = unfold(q2r[1, :, folded], q2r[0, :, folded], 4 * h + f)

    pairs(q2_rows)

    def q3_copy(n, j, send):
        up_down = lax.rem(s + (1 if (n % 2 == 0) == send else SPACE - 1), SPACE)
        cols = pl.ds(pl.multiple_of(j * CHUNK, CHUNK), CHUNK)
        return copy(q3s.at[n, :, cols], q3r.at[n, :, cols], q3_ss.at[n, j], q3_rs.at[n, j], at(tm, up_down))

    def two(j, folded, bases):
        tiles = [[], [], [], []]
        for base in bases:
            cols = pl.ds(base, CHUNK)
            r = ring_rates(q2, drow, base)
            top, bottom = [], []
            for f in range(3):
                x, y = s0r[f, :ROWS, cols], s1[f, :, cols]
                z = y + r[f][:ROWS]
                partial[f, :, cols] = y - 0.5 * (x + z)
                q = (step_size * first + start_share) * x + one_share * y + two_share * z
                q3[f, :ROWS, cols] = q
                top.append(q[:8])
                bottom.append(q[8:])
            for n, (parts, row) in enumerate(((bottom, 7), (top, 0), (bottom, 6), (top, 1))):
                tiles[n].append(place(parts, [row] * 3))
        for n in range(4):
            q3s[n, :, folded] = fold(*tiles[n])
        for n in range(2):
            q3_copy(n, j, True).start()

        @pl.when(k == 0)
        def _():
            for n in range(2, 4):
                q3_copy(n, j, True).start()

    pairs(two)
    for n in range(2):
        for j in range(PAIRS):
            q3_copy(n, j, False).wait_recv()

    @pl.when(k == 0)
    def _():
        for n in range(2, 4):
            for j in range(PAIRS):
                q3_copy(n, j, False).wait_recv()

    def q3_rows(j, folded, bases):
        row = lax.broadcasted_iota(jnp.int32, (8, CHUNK), 0)
        for h, base in enumerate(bases):
            for f in range(3):
                i = 4 * h + f
                near_rows = unfold(q3r[1, :, folded], q3r[0, :, folded], i)
                far_rows = jnp.where(row < 4, sub_roll(q3r[3, :, folded], 1 - i), sub_roll(q3r[2, :, folded], 6 - i))
                q3[f, ROWS:, pl.ds(base, CHUNK)] = jnp.where((row == 0) | (row == 7), near_rows, far_rows)

    pairs(q3_rows)

    def three(base):
        cols = pl.ds(base, CHUNK)
        r = ring_rates(q3, drow, base)
        for f in range(3):
            x = r[f] + first * s0r[f, :, cols]
            br[f, :, cols] = x
            boosted[f, :, cols] = x[:ROWS]

    chunks(three)
    give = copy(boosted, other, oth_s.at[0], oth_r.at[0], partner)

    def item_copy(i):
        cols = pl.ds(pl.multiple_of(i * CHUNK, CHUNK), CHUNK)
        return copy(item.at[:, :, cols], ritem.at[:, :, cols], it_s.at[i], it_r.at[i], partner)

    @pl.loop(0, COLS // CHUNK)
    def _(i):
        base = pl.multiple_of(i * CHUNK, CHUNK)
        cols = pl.ds(base, CHUNK)
        r = ring_rates(br, drow, base)
        for f in range(3):
            item[f, :, cols] = jnp.where(k == 0, boosted[f, :, cols] + step_size * r[f][:ROWS], boosted[f, :, cols])
        item_copy(i).start()

    give.start()

    def one_copy(f, sp, send):
        to, by = (sp, s) if send else (s, sp)
        n = to if send else by
        return copy(esum.at[f, :, block(to, k)], rt.at[f, rows(ROWS * by), :], one_s.at[f, n], one_r.at[f, by], at(tm, sp))

    for i in range(COLS // CHUNK):
        item_copy(i).wait_recv()

    def summed(base):
        cols = pl.ds(base, CHUNK)
        for f in range(3):
            esum[f, :, cols] = item[f, :, cols] + ritem[f, :, cols]

    chunks(summed)
    for f in range(3):
        for d in range(1, SPACE):
            one_copy(f, lax.rem(s + d, SPACE), True).start()
    rt[:, rows(ROWS * s), :] = esum[:, :, block(s, k)]

    def depth_pieces(base):
        return (
            (pl.ds(pl.multiple_of(base, 128), PART), pl.ds(128, PART)),
            (pl.ds(pl.multiple_of(lax.rem(base + COLS - 128, COLS), 128), 128), pl.ds(0, 128)),
            (pl.ds(pl.multiple_of(lax.rem(base + PART, COLS), 128), 128), pl.ds(384, 128)),
        )

    def depth_copy(d, n, send):
        sp = lax.rem(s + d, SPACE) if send else lax.rem(s + SPACE - d, SPACE)
        to = sp if send else s
        src, dst = depth_pieces(512 * to + 256 * (owned(to, tm) // 16))[n]
        return copy(depth.at[:, src], dr.at[rows(ROWS * (s if send else sp)), dst], dep_s.at[n, d], dep_r.at[n, d], at(tm, sp))

    for d in range(1, SPACE):
        for n in range(3):
            depth_copy(d, n, True).start()
    for src, dst in depth_pieces(512 * s + 256 * half):
        dr[rows(ROWS * s), dst] = depth[:, src]


    def two_copy(f, n):
        src, dst = et.at[f, rows(OWN * n, OWN), :], ex.at[chip, f, pl.ds(HALO, OWN), :]
        return copy(src, dst, two_s.at[f, n], two_r.at[f, chip], at(owner(s, 16 * k + n), s))

    for f in range(3):
        for d in range(1, SPACE):
            one_copy(f, lax.rem(s + SPACE - d, SPACE), False).wait_recv()
        for t in range(2):
            et[f, 128 * t : 128 * t + 128, :] = rt[f, :, 128 * t : 128 * t + 128].T

        @pl.loop(0, 16)
        def _(m, f=f):
            n = lax.rem(m + spot, 16)

            @pl.when((owner(s, 16 * k + n) != tm) & (chip < CHIPS - 1))
            def _():
                two_copy(f, n).start()

    @pl.when(half == k)
    def _():
        ex[chip, :, HALO : HALO + OWN, :] = et[:, rows(OWN * spot, OWN), :]

    def halo_copy(n, j, width):
        hop, sign = n // 2 + 1, 1 - 2 * (n % 2)
        far = OWN * (hop - 1)
        if sign > 0:
            src, dst = HALO + OWN - width, HALO - far - width
        else:
            src, dst = HALO, HALO + OWN + far
        return copy(ex.at[j, :, pl.ds(src, width), :], ex.at[j, :, pl.ds(dst, width), :], halo_s.at[n, j], halo_r.at[n, j], nears[n])

    def each_halo(j, act):
        for lo, hi, ns, width in ((0, 10, (0, 1), 16), (10, 14, (0, 1), 8), (0, 2, (2, 3), 16), (2, 6, (2, 3), 8)):
            @pl.when((j >= lo) & (j < hi))
            def _():
                for n in ns:
                    act(halo_copy(n, j, width))

    for c in (0, 1, 2, 3, 5, 6, 4, 7, 9, 10, 11, 8, 13, 14, 12):
        @pl.when((chip != c) | (half != k))
        def _(c=c):
            for f in range(3):
                src, dst = et.at[f, rows(OWN * spot, OWN), :], ex.at[c, f, pl.ds(HALO, OWN), :]
                copy(src, dst, two_s.at[f, 0], two_r.at[f, c], at(c * 2 + half, s)).wait_recv()

        for lo, hi, ns, width in ((0, 10, (0, 1), 16), (10, 14, (0, 1), 8), (0, 2, (2, 3), 16), (2, 6, (2, 3), 8)):
            if lo <= c < hi:
                for n in ns:
                    halo_copy(n, c, width).start()

    for d in range(1, SPACE):
        for n in range(3):
            depth_copy(d, n, False).wait_recv()
    for t in range(4):
        dt[128 * t : 128 * t + 128, :] = dr[:, 128 * t : 128 * t + 128].T


    def scanned(lo, hi, halo, state):
        count = OWN + 2 * halo
        d_own = dt[rows(128 - halo + OWN * spot, count), :]

        def stepped(state):
            h, u, v = state
            r = rates(
                h, u, v, d_own * u, d_own * v,
                lambda x: pltpu.roll(x, 1, 0), lambda x: pltpu.roll(x, count - 1, 0),
                lambda x: pltpu.roll(x, 1, 1), lambda x: pltpu.roll(x, 127, 1), lambda x: x,
            )
            return tuple(x + step_size * y for x, y in zip(state, r))

        def body(j, state):
            state = stepped(stepped(state))
            each_halo(j, lambda x: x.wait_recv())
            state = tuple(x + ex[j, f, HALO - halo : HALO + OWN + halo] for f, x in enumerate(state))
            for f in range(3):
                vx[j + 1, f] = state[f][halo : halo + OWN]

            @pl.when((chip != j + 1) | (half != k))
            def _():
                ret_copy(j + 1).start()

            return state

        return lax.fori_loop(lo, hi, body, state)

    def ret_copy(j):
        return copy(vx.at[j], vt.at[:, rows(OWN * spot, OWN), :], ret_s.at[j], ret_r.at[spot], at(j * 2 + half, s))

    state = scanned(0, 7, 32, (jnp.zeros((WIDE, 128), F32),) * 3)
    state = scanned(7, 11, 16, tuple(x[16:64] for x in state))
    scanned(11, CHIPS - 1, 8, tuple(x[8:40] for x in state))

    @pl.when(chip > 0)
    def _():
        @pl.when(half == k)
        def _():
            vt[:, rows(OWN * spot, OWN), :] = vx[chip]

        @pl.loop(0, 16)
        def _(n):
            t = owner(s, 16 * k + n)

            @pl.when(t != tm)
            def _():
                copy(vx.at[0], vt.at[:, rows(OWN * n, OWN), :], ret_s.at[0], ret_r.at[n], at(t, s)).wait_recv()

    low = lax.broadcasted_iota(jnp.int32, (8, 128), 0) < 4
    for f in range(3):
        for t in range(2):
            cols = slice(128 * t, 128 * t + 128)
            x = vt[f, cols, :].T
            for sp in range(SPACE):
                vr[sp, f, :ROWS, cols] = x[16 * sp : 16 * sp + 16]
                a, b = (16 * sp + 16) % 128, (16 * sp + 120) % 128
                vr[sp, f, ROWS:, cols] = jnp.where(low, x[a : a + 8], x[b : b + 8])

    def row_copy(sp, send):
        to, by = (sp, s) if send else (s, sp)
        return copy(vr.at[to], vout.at[:, :, block(by, k)], row_s.at[sp], row_r.at[by], at(tm, sp))

    def fin_copy(sp, send):
        cols = block(sp, k if send else 1 - k)
        return copy(vout.at[:, :, cols], vout.at[:, :, cols], fin_s.at[sp], fin_r.at[sp], partner)

    for d in range(1, SPACE):
        row_copy(lax.rem(s + d, SPACE), True).start()
    vout[:, :, block(s, k)] = vr[s]
    fin_copy(s, True).start()
    give.wait_recv()

    @pl.when(tm < 31)
    def _():
        for n in range(8):
            start_copy(n, tm_next).wait_send()

    for ns, buffer, back, spot_of in routes:
        @pl.when((z_place == spot_of) & (tm < 24))
        def _(ns=ns, buffer=buffer, back=back):
            for n in ns:
                pass_copy(n, buffer, ns[0], back + 1).wait_send()

    for n in range(4):
        for j in range(PAIRS):
            pack_copy(n, j, True).wait_send()
    for n in range(2):
        for j in range(PAIRS):
            q2_copy(n, j, True).wait_send()
            q3_copy(n, j, True).wait_send()

    @pl.when(k == 0)
    def _():
        for n in range(2, 4):
            for j in range(PAIRS):
                q3_copy(n, j, True).wait_send()

    give.wait_send()
    for i in range(COLS // CHUNK):
        item_copy(i).wait_send()
    for d in range(1, SPACE):
        for n in range(3):
            depth_copy(d, n, True).wait_send()
        for f in range(3):
            one_copy(f, lax.rem(s + d, SPACE), True).wait_send()

    @pl.loop(0, 16)
    def _(n):
        @pl.when((owner(s, 16 * k + n) != tm) & (chip < CHIPS - 1))
        def _():
            for f in range(3):
                two_copy(f, n).wait_send()

        each_halo(n, lambda x: x.wait_send())


    def finish(sp):
        base = pl.multiple_of(sp * CHUNK, CHUNK)
        cols = pl.ds(base, CHUNK)
        d = wide(lambda c: drow[:, c], base)

        def stepped(state):
            h, u, w = state
            r = rates(h, u, w, d * u, d * w, left, right, up, down, lambda x: x)
            return [x + step_size * y for x, y in zip(state, r)]

        state = [wide(lambda c, f=f: vout[f, :, c], base) for f in range(3)]
        a = stepped(state)
        b = stepped(a)
        for f in range(3):
            begin = inner(state[f])[:ROWS]
            ours = jnp.where(k == 0, boosted[f, :, cols], other[f, :, cols])
            y1 = ours + inner(a[f])[:ROWS]
            y2 = esum[f, :, cols] + inner(b[f])[:ROWS]
            start = jnp.where(k == 0, jnp.where(tm == 0, init[f, :, cols], begin), y1)
            end = jnp.where(k == 0, y1, y2)
            out[0, f, :, cols] = start
            out[1, f, :, cols] = partial[f, :, cols] + 0.5 * (start + end)
            out[2, f, :, cols] = end

    @pl.loop(1, SPACE)
    def _(d):
        sp = lax.rem(s + SPACE - d, SPACE)
        row_copy(sp, False).wait_recv()
        fin_copy(sp, True).start()
        fin_copy(lax.rem(sp + 1, SPACE), False).wait_recv()

        @pl.when(d >= 3)
        def _():
            finish(lax.rem(sp + 2, SPACE))

    fin_copy(lax.rem(s + 1, SPACE), False).wait_recv()

    @pl.loop(0, 3)
    def _(i):
        finish(lax.rem(s + 2 * SPACE - 6 - i, SPACE))

    for d in range(1, SPACE):
        row_copy(lax.rem(s + d, SPACE), True).wait_send()
    for sp in range(SPACE):
        fin_copy(sp, True).wait_send()

    @pl.loop(1, 16)
    def _(n):
        @pl.when((chip != n) | (half != k))
        def _():
            ret_copy(n).wait_send()


VM = pl.BlockSpec(memory_space=pltpu.VMEM)


def per_device(fine_nodes, init_state, mean_depth):
    points = fine_nodes[0].reshape(9, ROWS, COLS)

    def vm(*shape):
        return pltpu.VMEM(shape, F32)

    def sems(*shape):
        return [pltpu.SemaphoreType.DMA(shape)] * 2

    flat, ringed = vm(3, ROWS, COLS), vm(3, RING, COLS)
    out = pl.pallas_call(
        coarse_kernel,
        out_shape=jax.ShapeDtypeStruct((3, 3, ROWS, COLS), F32),
        in_specs=[pl.BlockSpec(memory_space=pltpu.HBM)] * 3,
        out_specs=VM,
        scratch_shapes=[
            flat, flat, flat, flat, ringed, vm(RING, COLS), vm(9, ROWS, COLS), flat, vm(ROWS, COLS),
            flat, flat, flat, vm(2, 8, FOLD), vm(2, 8, FOLD), vm(2, 8, FOLD), vm(2, 8, FOLD),
            ringed, ringed, flat, ringed, vm(2, 8, FOLD), vm(2, 8, FOLD), ringed, vm(4, 8, FOLD), vm(4, 8, FOLD),
            ringed, flat, flat, vm(2, 3, ROWS, COLS // 8), vm(2, 3, ROWS, COLS // 8), vm(2, 3, ROWS, COLS // 8),
            vm(3, 128, PART), vm(3, PART, 128), vm(128, 512), vm(512, 128),
            vm(CHIPS, 3, WIDE, 128), vm(CHIPS, 3, OWN, 128), vm(3, PART, 128), vm(SPACE, 3, RING, PART),
            pltpu.SemaphoreType.DMA((5,)), *sems(8), *sems(8), *sems(4, 4), *sems(2, 4), *sems(4, 4), *sems(8), *sems(1), *sems(3, 8), *sems(3, 8), *sems(3, 16),
            *sems(4, 16), *sems(16), *sems(8), *sems(8),
        ],
        compiler_params=pltpu.CompilerParams(collective_id=0, has_side_effects=True, vmem_limit_bytes=40 << 20),
        name="sweep",
    )(*(pltpu.with_memory_space_constraint(x, pltpu.HBM) for x in (points, init_state, mean_depth)))
    return out[None]


def solution(mesh):
    placed = (P("tm", None, None, "space", None), P(None, "space", None), P("space", None))
    return jax.shard_map(
        per_device,
        mesh=mesh,
        in_specs=placed,
        out_specs=P("tm", None, None, "space", None),
        check_vma=False,
    )
```

```python
import functools

import jax
import jax.numpy as jnp
from jax import lax
from jax.experimental import pallas as pl
from jax.experimental.pallas import tpu as pltpu
from jax.sharding import PartitionSpec as P

MESH = pl.DeviceIdType.MESH
F32 = jnp.float32

step_size = 0.3
viscosity = 1.0 / 3.0
coriolis = 0.5
quad_near = 5.0 / 24.0
quad_mid = 1.0 / 3.0
quad_far = -1.0 / 24.0
half_step = 0.5 * step_size
start_share = -(half_step + step_size / 3.0)
one_share = 2.0 * step_size / 3.0
two_share = half_step - step_size / 3.0

ROWS = 16
COLS = 4096
SPACE = 8
CHIPS = 16
PART = 256
OWN = 16
HALO = 16
MIDDLE = 7
WIDE = OWN + 2 * HALO


def rates(h, u, v, de, dn, left, right, up, down, centre):
    nh, nu, nv = viscosity * h, viscosity * u, viscosity * v
    he, hn, hh = 0.5 * de, 0.5 * dn, 0.5 * h
    nhc, nuc, nvc = centre(nh), centre(nu), centre(nv)
    hr = right(nh - he) + left(nh + he) + down(centre(nh - hn)) + up(centre(nh + hn)) - 4.0 * nhc
    ur = right(nu - hh) + left(nu + hh) + down(nuc) + up(nuc) - 4.0 * nuc + coriolis * centre(v)
    vr = right(nv) + left(nv) + down(centre(nv - hh)) + up(centre(nv + hh)) - 4.0 * nvc - coriolis * centre(u)
    return hr, ur, vr


CHUNK = 512
RING = 24


def edges(base):
    lo = pl.multiple_of(lax.rem(base + COLS - 128, COLS), 128)
    hi = pl.multiple_of(lax.rem(base + CHUNK, COLS), 128)
    return pl.ds(lo, 128), pl.ds(base, CHUNK), pl.ds(hi, 128)


def wide(get, base):
    return jnp.concatenate([get(c) for c in edges(base)], axis=1)


def right(x):
    return pltpu.roll(x, x.shape[1] - 1, 1)


def left(x):
    return pltpu.roll(x, 1, 1)


def down(x):
    return pltpu.roll(x, RING - 1, 0)


def up(x):
    return pltpu.roll(x, 1, 0)


def inner(x):
    return x[:, 128 : 128 + CHUNK]


def ring_rates(q, depth, base):
    h, u, v = (wide(lambda c, f=f: q[f, :, c], base) for f in range(3))
    d = wide(lambda c: depth[:, c], base)
    return rates(h, u, v, d * u, d * v, lambda x: inner(left(x)), lambda x: inner(right(x)), up, down, inner)


def chunks(body):
    @pl.loop(0, COLS // CHUNK)
    def _(i):
        body(pl.multiple_of(i * CHUNK, CHUNK))


PAIRS = COLS // CHUNK // 2
FOLD = COLS // 2


def pairs(body):
    @pl.loop(0, PAIRS)
    def _(j):
        base = pl.multiple_of(j * CHUNK, CHUNK)
        body(j, pl.ds(base, CHUNK), [base, pl.multiple_of(base + FOLD, CHUNK)])


def sub_roll(x, by):
    by %= 8
    return x if by == 0 else pltpu.roll(x, by, 0)


def pack(parts, at):
    row = lax.broadcasted_iota(jnp.int32, parts[0].shape, 0)
    tile = sub_roll(parts[0], -at)
    for i in range(1, len(parts)):
        tile = jnp.where(row >= 2 * i, sub_roll(parts[i], 2 * i - at), tile)
    return tile


def place(parts, at):
    row = lax.broadcasted_iota(jnp.int32, parts[0].shape, 0)
    tile = sub_roll(parts[0], -at[0])
    for i in range(1, len(parts)):
        tile = jnp.where(row >= i, sub_roll(parts[i], i - at[i]), tile)
    return tile


def fold(first, second):
    row = lax.broadcasted_iota(jnp.int32, first.shape, 0)
    return jnp.where(row < 4, first, sub_roll(second, 4))


def unfold(after, before, i):
    row = lax.broadcasted_iota(jnp.int32, after.shape, 0)
    return jnp.where(row < 4, sub_roll(after, -i), sub_roll(before, 7 - i))


def unpack(after, before, i):
    row = lax.broadcasted_iota(jnp.int32, after.shape, 0)
    return jnp.where(row < 4, sub_roll(after, -2 * i), sub_roll(before, 6 - 2 * i))


def snake(n):
    z, x = n // 4, lax.rem(n, 4)
    return z * 4 + jnp.where(lax.rem(z, 2) == 0, x, 3 - x)


def turned(s, chip):
    return chip // 4 * 4 + lax.rem(chip + 2 * lax.rem(s, 2), 4)


def owner(s, i):
    o = jnp.where(lax.rem(s, 2) == 0, i, 31 - i)
    return turned(s, snake(o // 2)) * 2 + lax.rem(o, 2)


def owned(s, tm):
    o = snake(turned(s, tm // 2)) * 2 + lax.rem(tm, 2)
    return jnp.where(lax.rem(s, 2) == 0, o, 31 - o)


def coarse_kernel(
    points_hbm, init_hbm, depth_hbm,
    out,
    boosted, other, esum, partial, vout, drow, points, init, depth, s0, a1, a2, ps, pr, fs, fr, s0r, q1, s1, q2, q2s, q2r, q3, q3s, q3r, br, item, ritem, relay_a, relay_b, relay_c,
    rt, et, dr, dt, ex, vx, middle, vt, vr,
    in_sem, st_s, st_r, rl_s, rl_r, pk_s, pk_r, q2_ss, q2_rs, q3_ss, q3_rs, it_s, it_r, oth_s, oth_r, one_s, one_r, dep_s, dep_r, two_s, two_r,
    halo_s, halo_r, ret_s, ret_r, row_s, row_r, fin_s, fin_r,
):
    tm = lax.axis_index("tm")
    s = lax.axis_index("space")
    chip, k = tm // 2, lax.rem(tm, 2)
    mine = owned(s, tm)
    half, spot = mine // 16, lax.rem(mine, 16)
    s_next, s_prev = lax.rem(s + 1, SPACE), lax.rem(s + SPACE - 1, SPACE)
    tm_next, tm_prev = lax.rem(tm + 1, 32), lax.rem(tm + 31, 32)
    first = jnp.where(tm == 0, 1.0, 0.0).astype(F32)

    def at(t, sp):
        return {"tm": t, "space": sp}

    def near(step):
        p = lax.rem(32 * s + mine + step + 256, 256)
        return at(owner(p // 32, lax.rem(p, 32)), p // 32)

    partner = at(chip * 2 + 1 - k, s)
    nears = [near(1), near(-1)]

    loads = [pltpu.make_async_copy(points_hbm.at[3 * m : 3 * m + 3], points.at[3 * m : 3 * m + 3], in_sem.at[m]) for m in range(3)]
    loads += [pltpu.make_async_copy(init_hbm, init, in_sem.at[3]), pltpu.make_async_copy(depth_hbm, depth, in_sem.at[4])]
    for n in (2, 0, 1, 4, 3):
        loads[n].start()
    vt[...] = jnp.zeros_like(vt)
    barrier = pltpu.get_barrier_semaphore()
    z, x = tm // 8, lax.rem(tm // 2, 4)
    peers = [
        at(lax.rem(z + dz, 4) * 8 + lax.rem(x + dx, 4) * 2 + c, s)
        for dz in (2, 1, 3, 0) for dx in (2, 1, 3, 0) for c in range(2) if dz or dx
    ] + [partner]
    peers += [at(tm, lax.rem(s + d, SPACE)) for d in range(1, SPACE)]
    peers += [at(t, sp) for t in (tm_next, tm_prev) for sp in (s_next, s_prev)]
    peers += nears
    for p in peers:
        pl.semaphore_signal(barrier, inc=1, device_id=p, device_id_type=MESH)
    pl.semaphore_wait(barrier, len(peers))

    def copy(src, dst, ss, rs, dev):
        return pltpu.make_async_remote_copy(src_ref=src, dst_ref=dst, send_sem=ss, recv_sem=rs, device_id=dev, device_id_type=MESH)

    def block(sp, kk):
        return pl.ds(pl.multiple_of(512 * sp + 256 * kk, PART), PART)

    def rows(start, n=ROWS):
        return pl.ds(pl.multiple_of(start, 8), n)

    loads[2].wait()

    z_place = lax.rem(tm, 8)
    far_end = (z_place == 7) & (tm < 31)
    PIECE = COLS // 8
    direct = range(0, 2)
    routes = ((range(2, 4), relay_a, 6, 1), (range(4, 6), relay_b, 2, 5), (range(6, 8), relay_c, 4, 3))

    def piece(n):
        return pl.ds(PIECE * n, PIECE)

    def start_copy(n, to):
        return copy(points.at[6:9, :, piece(n)], s0.at[:, :, piece(n)], st_s.at[n], st_r.at[n], at(to, s))

    def via_copy(n, buffer, first_piece, to):
        return copy(points.at[6:9, :, piece(n)], buffer.at[n - first_piece], st_s.at[n], rl_r.at[n], at(to, s))

    def pass_copy(n, buffer, first_piece, ahead):
        return copy(buffer.at[n - first_piece], s0.at[:, :, piece(n)], rl_s.at[n], st_r.at[n], at(lax.rem(tm + ahead, 32), s))

    @pl.when((tm < 31) & (z_place != 7))
    def _():
        for n in range(8):
            start_copy(n, tm_next).start()

    @pl.when(far_end)
    def _():
        for ns, buffer, back, _ in routes:
            for n in ns:
                via_copy(n, buffer, ns[0], lax.rem(tm + 32 - back, 32)).start()

    for n in (0, 1, 4, 3):
        loads[n].wait()

    def pack_copy(n, j, send):
        up_down = lax.rem(s + (1 if (n % 2 == 0) == send else SPACE - 1), SPACE)
        slot = tm if n < 2 else (tm_next if send else tm_prev)
        cols = pl.ds(pl.multiple_of(j * CHUNK, CHUNK), CHUNK)
        src, dst = (ps, pr) if n < 2 else (fs, fr)
        return copy(src.at[n % 2, :, cols], dst.at[n % 2, :, cols], pk_s.at[n, j], pk_r.at[n, j], at(slot, up_down))

    def prepare(j, folded, bases):
        tiles = [[], []], [[], []]
        for base in bases:
            cols = pl.ds(base, CHUNK)
            top, bottom = [], []
            for f in range(3):
                p0, p1, p2 = (points[3 * m + f, :, cols] for m in range(3))
                x = (step_size * quad_near - half_step) * p0 + (step_size * quad_mid) * p1 + (step_size * quad_far) * p2
                y = (step_size * quad_far) * p0 + (step_size * quad_mid - half_step) * p1 + (step_size * quad_near) * p2
                a1[f, :, cols] = x
                a2[f, :, cols] = y
                top.append(x[:8])
                bottom.append(x[8:])
            for n, (parts, tile, row, inside) in enumerate(((bottom, 8, 7, 6), (top, 0, 0, 1))):
                d = depth[tile : tile + 8, cols]
                ends = [
                    jnp.where(tm == 31, init[f, tile : tile + 8, cols], points[6 + f, tile : tile + 8, cols]) for f in range(3)
                ]
                tiles[0][n].append(place(parts + [d], [row] * 4))
                tiles[1][n].append(place(ends + [d], [row] * 3 + [inside]))
        for n in range(2):
            ps[n, :, folded] = fold(*tiles[0][n])
            fs[n, :, folded] = fold(*tiles[1][n])
        for n in range(2, 4):
            pack_copy(n, j, True).start()

    pairs(prepare)

    @pl.when(far_end)
    def _():
        for n in direct:
            start_copy(n, tm_next).start()

    for n in range(2):
        for j in range(PAIRS):
            pack_copy(n, j, True).start()

    for ns, buffer, back, spot_of in routes:
        @pl.when((z_place == spot_of) & (tm < 24))
        def _(ns=ns, buffer=buffer, back=back):
            for n in ns:
                via_copy(n, buffer, ns[0], lax.rem(tm + back, 32)).wait_recv()
                pass_copy(n, buffer, ns[0], back + 1).start()

    for n in range(4):
        for j in range(PAIRS):
            pack_copy(n, j, False).wait_recv()

    @pl.when(tm > 0)
    def _():
        for n in range(8):
            start_copy(n, tm_prev).wait_recv()

    def ringed(j, folded, bases):
        row = lax.broadcasted_iota(jnp.int32, (8, CHUNK), 0)
        for h, base in enumerate(bases):
            cols = pl.ds(base, CHUNK)
            pa, pb, fa, fb = pr[1, :, folded], pr[0, :, folded], fr[1, :, folded], fr[0, :, folded]
            i = 4 * h + 3
            d = jnp.where(row < 4, sub_roll(fa, 1 - i), sub_roll(fb, 6 - i))
            d = jnp.where((row == 0) | (row == 7), unfold(pa, pb, i), d)
            drow[:, cols] = jnp.concatenate([depth[:, cols], d], axis=0)
            for f in range(3):
                main = jnp.where(tm == 0, init[f, :, cols], s0[f, :, cols])
                x = jnp.concatenate([main, unfold(fa, fb, 4 * h + f)], axis=0)
                y = jnp.concatenate([a1[f, :, cols], unfold(pa, pb, 4 * h + f)], axis=0)
                s0r[f, :, cols] = x
                q1[f, :, cols] = half_step * x + y

    pairs(ringed)

    def q2_copy(n, j, send):
        up_down = lax.rem(s + (1 if (n == 0) == send else SPACE - 1), SPACE)
        cols = pl.ds(pl.multiple_of(j * CHUNK, CHUNK), CHUNK)
        return copy(q2s.at[n, :, cols], q2r.at[n, :, cols], q2_ss.at[n, j], q2_rs.at[n, j], at(tm, up_down))

    def one(j, folded, bases):
        tiles = [[], []]
        for base in bases:
            cols = pl.ds(base, CHUNK)
            r = ring_rates(q1, drow, base)
            q = []
            for f in range(3):
                x = s0r[f, :ROWS, cols] + r[f][:ROWS]
                s1[f, :, cols] = x
                q.append(half_step * x + a2[f, :, cols])
                q2[f, :ROWS, cols] = q[f]
            tiles[0].append(place([x[8:] for x in q], [7] * 3))
            tiles[1].append(place([x[:8] for x in q], [0] * 3))
        for n in range(2):
            q2s[n, :, folded] = fold(*tiles[n])
            q2_copy(n, j, True).start()

    pairs(one)
    for n in range(2):
        for j in range(PAIRS):
            q2_copy(n, j, False).wait_recv()

    def q2_rows(j, folded, bases):
        for h, base in enumerate(bases):
            for f in range(3):
                q2[f, ROWS:, pl.ds(base, CHUNK)] = unfold(q2r[1, :, folded], q2r[0, :, folded], 4 * h + f)

    pairs(q2_rows)

    def q3_copy(n, j, send):
        up_down = lax.rem(s + (1 if (n % 2 == 0) == send else SPACE - 1), SPACE)
        cols = pl.ds(pl.multiple_of(j * CHUNK, CHUNK), CHUNK)
        return copy(q3s.at[n, :, cols], q3r.at[n, :, cols], q3_ss.at[n, j], q3_rs.at[n, j], at(tm, up_down))

    def two(j, folded, bases):
        tiles = [[], [], [], []]
        for base in bases:
            cols = pl.ds(base, CHUNK)
            r = ring_rates(q2, drow, base)
            top, bottom = [], []
            for f in range(3):
                x, y = s0r[f, :ROWS, cols], s1[f, :, cols]
                z = y + r[f][:ROWS]
                partial[f, :, cols] = y - 0.5 * (x + z)
                q = (step_size * first + start_share) * x + one_share * y + two_share * z
                q3[f, :ROWS, cols] = q
                top.append(q[:8])
                bottom.append(q[8:])
            for n, (parts, row) in enumerate(((bottom, 7), (top, 0), (bottom, 6), (top, 1))):
                tiles[n].append(place(parts, [row] * 3))
        for n in range(4):
            q3s[n, :, folded] = fold(*tiles[n])
        for n in range(2):
            q3_copy(n, j, True).start()

        @pl.when(k == 0)
        def _():
            for n in range(2, 4):
                q3_copy(n, j, True).start()

    pairs(two)
    for n in range(2):
        for j in range(PAIRS):
            q3_copy(n, j, False).wait_recv()

    @pl.when(k == 0)
    def _():
        for n in range(2, 4):
            for j in range(PAIRS):
                q3_copy(n, j, False).wait_recv()

    def q3_rows(j, folded, bases):
        row = lax.broadcasted_iota(jnp.int32, (8, CHUNK), 0)
        for h, base in enumerate(bases):
            for f in range(3):
                i = 4 * h + f
                near_rows = unfold(q3r[1, :, folded], q3r[0, :, folded], i)
                far_rows = jnp.where(row < 4, sub_roll(q3r[3, :, folded], 1 - i), sub_roll(q3r[2, :, folded], 6 - i))
                q3[f, ROWS:, pl.ds(base, CHUNK)] = jnp.where((row == 0) | (row == 7), near_rows, far_rows)

    pairs(q3_rows)

    def three(base):
        cols = pl.ds(base, CHUNK)
        r = ring_rates(q3, drow, base)
        for f in range(3):
            x = r[f] + first * s0r[f, :, cols]
            br[f, :, cols] = x
            boosted[f, :, cols] = x[:ROWS]

    chunks(three)
    give = copy(boosted, other, oth_s.at[0], oth_r.at[0], partner)

    def item_copy(i):
        cols = pl.ds(pl.multiple_of(i * CHUNK, CHUNK), CHUNK)
        return copy(item.at[:, :, cols], ritem.at[:, :, cols], it_s.at[i], it_r.at[i], partner)

    @pl.loop(0, COLS // CHUNK)
    def _(i):
        base = pl.multiple_of(i * CHUNK, CHUNK)
        cols = pl.ds(base, CHUNK)
        r = ring_rates(br, drow, base)
        for f in range(3):
            item[f, :, cols] = jnp.where(k == 0, boosted[f, :, cols] + step_size * r[f][:ROWS], boosted[f, :, cols])
        item_copy(i).start()

    give.start()

    def one_copy(f, sp, send):
        to, by = (sp, s) if send else (s, sp)
        n = to if send else by
        return copy(esum.at[f, :, block(to, k)], rt.at[f, rows(ROWS * by), :], one_s.at[f, n], one_r.at[f, by], at(tm, sp))

    for i in range(COLS // CHUNK):
        item_copy(i).wait_recv()

    def summed(base):
        cols = pl.ds(base, CHUNK)
        for f in range(3):
            esum[f, :, cols] = item[f, :, cols] + ritem[f, :, cols]

    chunks(summed)
    for f in range(3):
        for d in range(1, SPACE):
            one_copy(f, lax.rem(s + d, SPACE), True).start()
    rt[:, rows(ROWS * s), :] = esum[:, :, block(s, k)]

    def depth_pieces(base):
        return (
            (pl.ds(pl.multiple_of(base, 128), PART), pl.ds(128, PART)),
            (pl.ds(pl.multiple_of(lax.rem(base + COLS - 128, COLS), 128), 128), pl.ds(0, 128)),
            (pl.ds(pl.multiple_of(lax.rem(base + PART, COLS), 128), 128), pl.ds(384, 128)),
        )

    def depth_copy(d, n, send):
        sp = lax.rem(s + d, SPACE) if send else lax.rem(s + SPACE - d, SPACE)
        to = sp if send else s
        src, dst = depth_pieces(512 * to + 256 * (owned(to, tm) // 16))[n]
        return copy(depth.at[:, src], dr.at[rows(ROWS * (s if send else sp)), dst], dep_s.at[n, d], dep_r.at[n, d], at(tm, sp))

    for d in range(1, SPACE):
        for n in range(3):
            depth_copy(d, n, True).start()
    for src, dst in depth_pieces(512 * s + 256 * half):
        dr[rows(ROWS * s), dst] = depth[:, src]


    def two_copy(f, n):
        src, dst = et.at[f, rows(OWN * n, OWN), :], ex.at[chip, f, pl.ds(HALO, OWN), :]
        return copy(src, dst, two_s.at[f, n], two_r.at[f, chip], at(owner(s, 16 * k + n), s))

    for f in range(3):
        for d in range(1, SPACE):
            one_copy(f, lax.rem(s + SPACE - d, SPACE), False).wait_recv()
        for t in range(2):
            et[f, 128 * t : 128 * t + 128, :] = rt[f, :, 128 * t : 128 * t + 128].T

        @pl.loop(0, 16)
        def _(m, f=f):
            n = lax.rem(m + spot, 16)

            @pl.when((owner(s, 16 * k + n) != tm) & (chip < CHIPS - 1))
            def _():
                two_copy(f, n).start()

    @pl.when(half == k)
    def _():
        ex[chip, :, HALO : HALO + OWN, :] = et[:, rows(OWN * spot, OWN), :]

    spans = ((0, 2, 16), (2, 6, 8), (7, 10, 16), (10, 14, 8))

    def halo_copy(n, j, width):
        src, dst = (HALO + OWN - width, HALO - width) if n == 0 else (HALO, HALO + OWN)
        return copy(ex.at[j, :, pl.ds(src, width), :], ex.at[j, :, pl.ds(dst, width), :], halo_s.at[n, j], halo_r.at[n, j], nears[n])

    def middle_copy(n):
        return copy(vx.at[MIDDLE], middle.at[n], halo_s.at[n, 15], halo_r.at[n, 15], nears[n])

    def each_halo(j, act):
        for lo, hi, width in spans:
            @pl.when((j >= lo) & (j < hi))
            def _():
                for n in range(2):
                    act(halo_copy(n, j, width))

    for c in (0, 1, 2, 3, 5, 6, 4, 7, 9, 10, 11, 8, 13, 14, 12):
        @pl.when((chip != c) | (half != k))
        def _(c=c):
            for f in range(3):
                src, dst = et.at[f, rows(OWN * spot, OWN), :], ex.at[c, f, pl.ds(HALO, OWN), :]
                copy(src, dst, two_s.at[f, 0], two_r.at[f, c], at(c * 2 + half, s)).wait_recv()

        for lo, hi, width in spans:
            if lo <= c < hi:
                for n in range(2):
                    halo_copy(n, c, width).start()

    for d in range(1, SPACE):
        for n in range(3):
            depth_copy(d, n, False).wait_recv()
    for t in range(4):
        dt[128 * t : 128 * t + 128, :] = dr[:, 128 * t : 128 * t + 128].T


    def scanned(lo, hi, halo, state):
        count = OWN + 2 * halo
        d_own = dt[rows(128 - halo + OWN * spot, count), :]

        def stepped(state):
            h, u, v = state
            r = rates(
                h, u, v, d_own * u, d_own * v,
                lambda x: pltpu.roll(x, 1, 0), lambda x: pltpu.roll(x, count - 1, 0),
                lambda x: pltpu.roll(x, 1, 1), lambda x: pltpu.roll(x, 127, 1), lambda x: x,
            )
            return tuple(x + step_size * y for x, y in zip(state, r))

        def body(j, state):
            state = stepped(stepped(state))
            each_halo(j, lambda x: x.wait_recv())
            state = tuple(x + ex[j, f, HALO - halo : HALO + OWN + halo] for f, x in enumerate(state))
            for f in range(3):
                vx[j + 1, f] = state[f][halo : halo + OWN]

            @pl.when((chip != j + 1) | (half != k))
            def _():
                ret_copy(j + 1).start()

            return state

        return lax.fori_loop(lo, hi, body, state)

    def ret_copy(j):
        return copy(vx.at[j], vt.at[:, rows(OWN * spot, OWN), :], ret_s.at[j], ret_r.at[spot], at(j * 2 + half, s))

    state = scanned(0, MIDDLE, HALO, (jnp.zeros((WIDE, 128), F32),) * 3)
    for n in range(2):
        middle_copy(n).start()
    for n in range(2):
        middle_copy(n).wait_recv()
    state = tuple(jnp.concatenate([middle[0, f], x[HALO : HALO + OWN], middle[1, f]], axis=0) for f, x in enumerate(state))
    state = scanned(MIDDLE, 11, HALO, state)
    scanned(11, CHIPS - 1, 8, tuple(x[8:40] for x in state))

    @pl.when(chip > 0)
    def _():
        @pl.when(half == k)
        def _():
            vt[:, rows(OWN * spot, OWN), :] = vx[chip]

        @pl.loop(0, 16)
        def _(n):
            t = owner(s, 16 * k + n)

            @pl.when(t != tm)
            def _():
                copy(vx.at[0], vt.at[:, rows(OWN * n, OWN), :], ret_s.at[0], ret_r.at[n], at(t, s)).wait_recv()

    low = lax.broadcasted_iota(jnp.int32, (8, 128), 0) < 4
    for f in range(3):
        for t in range(2):
            cols = slice(128 * t, 128 * t + 128)
            x = vt[f, cols, :].T
            for sp in range(SPACE):
                vr[sp, f, :ROWS, cols] = x[16 * sp : 16 * sp + 16]
                a, b = (16 * sp + 16) % 128, (16 * sp + 120) % 128
                vr[sp, f, ROWS:, cols] = jnp.where(low, x[a : a + 8], x[b : b + 8])

    def row_copy(sp, send):
        to, by = (sp, s) if send else (s, sp)
        return copy(vr.at[to], vout.at[:, :, block(by, k)], row_s.at[sp], row_r.at[by], at(tm, sp))

    def fin_copy(sp, send):
        cols = block(sp, k if send else 1 - k)
        return copy(vout.at[:, :, cols], vout.at[:, :, cols], fin_s.at[sp], fin_r.at[sp], partner)

    for d in range(1, SPACE):
        row_copy(lax.rem(s + d, SPACE), True).start()
    vout[:, :, block(s, k)] = vr[s]
    fin_copy(s, True).start()
    give.wait_recv()

    @pl.when(tm < 31)
    def _():
        for n in range(8):
            start_copy(n, tm_next).wait_send()

    for ns, buffer, back, spot_of in routes:
        @pl.when((z_place == spot_of) & (tm < 24))
        def _(ns=ns, buffer=buffer, back=back):
            for n in ns:
                pass_copy(n, buffer, ns[0], back + 1).wait_send()

    for n in range(4):
        for j in range(PAIRS):
            pack_copy(n, j, True).wait_send()
    for n in range(2):
        for j in range(PAIRS):
            q2_copy(n, j, True).wait_send()
            q3_copy(n, j, True).wait_send()

    @pl.when(k == 0)
    def _():
        for n in range(2, 4):
            for j in range(PAIRS):
                q3_copy(n, j, True).wait_send()

    give.wait_send()
    for i in range(COLS // CHUNK):
        item_copy(i).wait_send()
    for d in range(1, SPACE):
        for n in range(3):
            depth_copy(d, n, True).wait_send()
        for f in range(3):
            one_copy(f, lax.rem(s + d, SPACE), True).wait_send()

    @pl.loop(0, 16)
    def _(n):
        @pl.when((owner(s, 16 * k + n) != tm) & (chip < CHIPS - 1))
        def _():
            for f in range(3):
                two_copy(f, n).wait_send()

        each_halo(n, lambda x: x.wait_send())

    for n in range(2):
        middle_copy(n).wait_send()


    def finish(sp):
        base = pl.multiple_of(sp * CHUNK, CHUNK)
        cols = pl.ds(base, CHUNK)
        d = wide(lambda c: drow[:, c], base)

        def stepped(state):
            h, u, w = state
            r = rates(h, u, w, d * u, d * w, left, right, up, down, lambda x: x)
            return [x + step_size * y for x, y in zip(state, r)]

        state = [wide(lambda c, f=f: vout[f, :, c], base) for f in range(3)]
        a = stepped(state)
        b = stepped(a)
        for f in range(3):
            begin = inner(state[f])[:ROWS]
            ours = jnp.where(k == 0, boosted[f, :, cols], other[f, :, cols])
            y1 = ours + inner(a[f])[:ROWS]
            y2 = esum[f, :, cols] + inner(b[f])[:ROWS]
            start = jnp.where(k == 0, jnp.where(tm == 0, init[f, :, cols], begin), y1)
            end = jnp.where(k == 0, y1, y2)
            out[0, f, :, cols] = start
            out[1, f, :, cols] = partial[f, :, cols] + 0.5 * (start + end)
            out[2, f, :, cols] = end

    @pl.loop(1, SPACE)
    def _(d):
        sp = lax.rem(s + SPACE - d, SPACE)
        row_copy(sp, False).wait_recv()
        fin_copy(sp, True).start()
        fin_copy(lax.rem(sp + 1, SPACE), False).wait_recv()

        @pl.when(d >= 3)
        def _():
            finish(lax.rem(sp + 2, SPACE))

    fin_copy(lax.rem(s + 1, SPACE), False).wait_recv()

    @pl.loop(0, 3)
    def _(i):
        finish(lax.rem(s + 2 * SPACE - 6 - i, SPACE))

    for d in range(1, SPACE):
        row_copy(lax.rem(s + d, SPACE), True).wait_send()
    for sp in range(SPACE):
        fin_copy(sp, True).wait_send()

    @pl.loop(1, 16)
    def _(n):
        @pl.when((chip != n) | (half != k))
        def _():
            ret_copy(n).wait_send()


VM = pl.BlockSpec(memory_space=pltpu.VMEM)


def per_device(fine_nodes, init_state, mean_depth):
    points = fine_nodes[0].reshape(9, ROWS, COLS)

    def vm(*shape):
        return pltpu.VMEM(shape, F32)

    def sems(*shape):
        return [pltpu.SemaphoreType.DMA(shape)] * 2

    flat, ringed = vm(3, ROWS, COLS), vm(3, RING, COLS)
    out = pl.pallas_call(
        coarse_kernel,
        out_shape=jax.ShapeDtypeStruct((3, 3, ROWS, COLS), F32),
        in_specs=[pl.BlockSpec(memory_space=pltpu.HBM)] * 3,
        out_specs=VM,
        scratch_shapes=[
            flat, flat, flat, flat, ringed, vm(RING, COLS), vm(9, ROWS, COLS), flat, vm(ROWS, COLS),
            flat, flat, flat, vm(2, 8, FOLD), vm(2, 8, FOLD), vm(2, 8, FOLD), vm(2, 8, FOLD),
            ringed, ringed, flat, ringed, vm(2, 8, FOLD), vm(2, 8, FOLD), ringed, vm(4, 8, FOLD), vm(4, 8, FOLD),
            ringed, flat, flat, vm(2, 3, ROWS, COLS // 8), vm(2, 3, ROWS, COLS // 8), vm(2, 3, ROWS, COLS // 8),
            vm(3, 128, PART), vm(3, PART, 128), vm(128, 512), vm(512, 128),
            vm(CHIPS, 3, WIDE, 128), vm(CHIPS, 3, OWN, 128), vm(2, 3, OWN, 128), vm(3, PART, 128), vm(SPACE, 3, RING, PART),
            pltpu.SemaphoreType.DMA((5,)), *sems(8), *sems(8), *sems(4, 4), *sems(2, 4), *sems(4, 4), *sems(8), *sems(1), *sems(3, 8), *sems(3, 8), *sems(3, 16),
            *sems(2, 16), *sems(16), *sems(8), *sems(8),
        ],
        compiler_params=pltpu.CompilerParams(collective_id=0, has_side_effects=True, vmem_limit_bytes=40 << 20),
        name="sweep",
    )(*(pltpu.with_memory_space_constraint(x, pltpu.HBM) for x in (points, init_state, mean_depth)))
    return out[None]


def solution(mesh):
    placed = (P("tm", None, None, "space", None), P(None, "space", None), P("space", None))
    return jax.shard_map(
        per_device,
        mesh=mesh,
        in_specs=placed,
        out_specs=P("tm", None, None, "space", None),
        check_vma=False,
    )
```

```python
import functools

import jax
import jax.numpy as jnp
from jax import lax
from jax.experimental import pallas as pl
from jax.experimental.pallas import tpu as pltpu
from jax.sharding import PartitionSpec as P

MESH = pl.DeviceIdType.MESH
F32 = jnp.float32

step_size = 0.3
viscosity = 1.0 / 3.0
coriolis = 0.5
quad_near = 5.0 / 24.0
quad_mid = 1.0 / 3.0
quad_far = -1.0 / 24.0
half_step = 0.5 * step_size
start_share = -(half_step + step_size / 3.0)
one_share = 2.0 * step_size / 3.0
two_share = half_step - step_size / 3.0

ROWS = 16
COLS = 4096
SPACE = 8
CHIPS = 16
PART = 256
OWN = 16
HALO = 16
MIDDLE = 7
WIDE = OWN + 2 * HALO


def rates(h, u, v, de, dn, left, right, up, down, centre):
    nh, nu, nv = viscosity * h, viscosity * u, viscosity * v
    he, hn, hh = 0.5 * de, 0.5 * dn, 0.5 * h
    nhc, nuc, nvc = centre(nh), centre(nu), centre(nv)
    hr = right(nh - he) + left(nh + he) + down(centre(nh - hn)) + up(centre(nh + hn)) - 4.0 * nhc
    ur = right(nu - hh) + left(nu + hh) + down(nuc) + up(nuc) - 4.0 * nuc + coriolis * centre(v)
    vr = right(nv) + left(nv) + down(centre(nv - hh)) + up(centre(nv + hh)) - 4.0 * nvc - coriolis * centre(u)
    return hr, ur, vr


CHUNK = 512
RING = 24


def edges(base):
    lo = pl.multiple_of(lax.rem(base + COLS - 128, COLS), 128)
    hi = pl.multiple_of(lax.rem(base + CHUNK, COLS), 128)
    return pl.ds(lo, 128), pl.ds(base, CHUNK), pl.ds(hi, 128)


def wide(get, base):
    return jnp.concatenate([get(c) for c in edges(base)], axis=1)


def right(x):
    return pltpu.roll(x, x.shape[1] - 1, 1)


def left(x):
    return pltpu.roll(x, 1, 1)


def down(x):
    return pltpu.roll(x, RING - 1, 0)


def up(x):
    return pltpu.roll(x, 1, 0)


def inner(x):
    return x[:, 128 : 128 + CHUNK]


def ring_rates(q, depth, base):
    h, u, v = (wide(lambda c, f=f: q[f, :, c], base) for f in range(3))
    d = wide(lambda c: depth[:, c], base)
    return rates(h, u, v, d * u, d * v, lambda x: inner(left(x)), lambda x: inner(right(x)), up, down, inner)


def chunks(body):
    @pl.loop(0, COLS // CHUNK)
    def _(i):
        body(pl.multiple_of(i * CHUNK, CHUNK))


PAIRS = COLS // CHUNK // 2
FOLD = COLS // 2


def pairs(body):
    @pl.loop(0, PAIRS)
    def _(j):
        base = pl.multiple_of(j * CHUNK, CHUNK)
        body(j, pl.ds(base, CHUNK), [base, pl.multiple_of(base + FOLD, CHUNK)])


def sub_roll(x, by):
    by %= 8
    return x if by == 0 else pltpu.roll(x, by, 0)


def pack(parts, at):
    row = lax.broadcasted_iota(jnp.int32, parts[0].shape, 0)
    tile = sub_roll(parts[0], -at)
    for i in range(1, len(parts)):
        tile = jnp.where(row >= 2 * i, sub_roll(parts[i], 2 * i - at), tile)
    return tile


def place(parts, at):
    row = lax.broadcasted_iota(jnp.int32, parts[0].shape, 0)
    tile = sub_roll(parts[0], -at[0])
    for i in range(1, len(parts)):
        tile = jnp.where(row >= i, sub_roll(parts[i], i - at[i]), tile)
    return tile


def fold(first, second):
    row = lax.broadcasted_iota(jnp.int32, first.shape, 0)
    return jnp.where(row < 4, first, sub_roll(second, 4))


def unfold(after, before, i):
    row = lax.broadcasted_iota(jnp.int32, after.shape, 0)
    return jnp.where(row < 4, sub_roll(after, -i), sub_roll(before, 7 - i))


def unpack(after, before, i):
    row = lax.broadcasted_iota(jnp.int32, after.shape, 0)
    return jnp.where(row < 4, sub_roll(after, -2 * i), sub_roll(before, 6 - 2 * i))


def snake(n):
    z, x = n // 4, lax.rem(n, 4)
    return z * 4 + jnp.where(lax.rem(z, 2) == 0, x, 3 - x)


def turned(s, chip):
    return chip // 4 * 4 + lax.rem(chip + 2 * lax.rem(s, 2), 4)


def owner(s, i):
    o = jnp.where(lax.rem(s, 2) == 0, i, 31 - i)
    return turned(s, snake(o // 2)) * 2 + lax.rem(o, 2)


def owned(s, tm):
    o = snake(turned(s, tm // 2)) * 2 + lax.rem(tm, 2)
    return jnp.where(lax.rem(s, 2) == 0, o, 31 - o)


def coarse_kernel(
    points_hbm, init_hbm, depth_hbm,
    out,
    boosted, other, esum, partial, vout, drow, points, init, depth, s0, a1, a2, ps, pr, fs, fr, s0r, q1, s1, q2, q2s, q2r, q3, q3s, q3r, br, item, ritem, relay_a, relay_b, relay_c,
    rt, et, dr, dt, ex, vx, middle, vt, vr,
    in_sem, st_s, st_r, rl_s, rl_r, pk_s, pk_r, q2_ss, q2_rs, q3_ss, q3_rs, it_s, it_r, oth_s, oth_r, one_s, one_r, dep_s, dep_r, two_s, two_r,
    halo_s, halo_r, ret_s, ret_r, row_s, row_r, fin_s, fin_r,
):
    tm = lax.axis_index("tm")
    s = lax.axis_index("space")
    chip, k = tm // 2, lax.rem(tm, 2)
    mine = owned(s, tm)
    half, spot = mine // 16, lax.rem(mine, 16)
    s_next, s_prev = lax.rem(s + 1, SPACE), lax.rem(s + SPACE - 1, SPACE)
    tm_next, tm_prev = lax.rem(tm + 1, 32), lax.rem(tm + 31, 32)
    first = jnp.where(tm == 0, 1.0, 0.0).astype(F32)

    def at(t, sp):
        return {"tm": t, "space": sp}

    def near(step):
        p = lax.rem(32 * s + mine + step + 256, 256)
        return at(owner(p // 32, lax.rem(p, 32)), p // 32)

    partner = at(chip * 2 + 1 - k, s)
    nears = [near(1), near(-1)]

    loads = [pltpu.make_async_copy(points_hbm.at[3 * m : 3 * m + 3], points.at[3 * m : 3 * m + 3], in_sem.at[m]) for m in range(3)]
    loads += [pltpu.make_async_copy(init_hbm, init, in_sem.at[3]), pltpu.make_async_copy(depth_hbm, depth, in_sem.at[4])]
    for n in (2, 0, 1, 4, 3):
        loads[n].start()
    vt[...] = jnp.zeros_like(vt)
    barrier = pltpu.get_barrier_semaphore()
    z, x = tm // 8, lax.rem(tm // 2, 4)
    peers = [
        at(lax.rem(z + dz, 4) * 8 + lax.rem(x + dx, 4) * 2 + c, s)
        for dz in (2, 1, 3, 0) for dx in (2, 1, 3, 0) for c in range(2) if dz or dx
    ] + [partner]
    peers += [at(tm, lax.rem(s + d, SPACE)) for d in range(1, SPACE)]
    peers += [at(t, sp) for t in (tm_next, tm_prev) for sp in (s_next, s_prev)]
    peers += nears
    for p in peers:
        pl.semaphore_signal(barrier, inc=1, device_id=p, device_id_type=MESH)
    pl.semaphore_wait(barrier, len(peers))

    def copy(src, dst, ss, rs, dev):
        return pltpu.make_async_remote_copy(src_ref=src, dst_ref=dst, send_sem=ss, recv_sem=rs, device_id=dev, device_id_type=MESH)

    def block(sp, kk):
        return pl.ds(pl.multiple_of(512 * sp + 256 * kk, PART), PART)

    def rows(start, n=ROWS):
        return pl.ds(pl.multiple_of(start, 8), n)

    loads[2].wait()

    z_place = lax.rem(tm, 8)
    far_end = (z_place == 7) & (tm < 31)
    PIECE = COLS // 8
    direct = range(0, 2)
    routes = ((range(2, 4), relay_a, 6, 1), (range(4, 6), relay_b, 2, 5), (range(6, 8), relay_c, 4, 3))

    def piece(n):
        return pl.ds(PIECE * n, PIECE)

    def start_copy(n, to):
        return copy(points.at[6:9, :, piece(n)], s0.at[:, :, piece(n)], st_s.at[n], st_r.at[n], at(to, s))

    def via_copy(n, buffer, first_piece, to):
        return copy(points.at[6:9, :, piece(n)], buffer.at[n - first_piece], st_s.at[n], rl_r.at[n], at(to, s))

    def pass_copy(n, buffer, first_piece, ahead):
        return copy(buffer.at[n - first_piece], s0.at[:, :, piece(n)], rl_s.at[n], st_r.at[n], at(lax.rem(tm + ahead, 32), s))

    @pl.when((tm < 31) & (z_place != 7))
    def _():
        for n in range(8):
            start_copy(n, tm_next).start()

    @pl.when(far_end)
    def _():
        for ns, buffer, back, _ in routes:
            for n in ns:
                via_copy(n, buffer, ns[0], lax.rem(tm + 32 - back, 32)).start()

    for n in (0, 1, 4, 3):
        loads[n].wait()

    def pack_copy(n, j, send):
        up_down = lax.rem(s + (1 if (n % 2 == 0) == send else SPACE - 1), SPACE)
        slot = tm if n < 2 else (tm_next if send else tm_prev)
        cols = pl.ds(pl.multiple_of(j * CHUNK, CHUNK), CHUNK)
        src, dst = (ps, pr) if n < 2 else (fs, fr)
        return copy(src.at[n % 2, :, cols], dst.at[n % 2, :, cols], pk_s.at[n, j], pk_r.at[n, j], at(slot, up_down))

    def prepare(j, folded, bases):
        tiles = [[], []], [[], []]
        for base in bases:
            cols = pl.ds(base, CHUNK)
            top, bottom = [], []
            for f in range(3):
                p0, p1, p2 = (points[3 * m + f, :, cols] for m in range(3))
                x = (step_size * quad_near - half_step) * p0 + (step_size * quad_mid) * p1 + (step_size * quad_far) * p2
                y = (step_size * quad_far) * p0 + (step_size * quad_mid - half_step) * p1 + (step_size * quad_near) * p2
                a1[f, :, cols] = x
                a2[f, :, cols] = y
                top.append(x[:8])
                bottom.append(x[8:])
            for n, (parts, tile, row, inside) in enumerate(((bottom, 8, 7, 6), (top, 0, 0, 1))):
                d = depth[tile : tile + 8, cols]
                ends = [
                    jnp.where(tm == 31, init[f, tile : tile + 8, cols], points[6 + f, tile : tile + 8, cols]) for f in range(3)
                ]
                tiles[0][n].append(place(parts + [d], [row] * 4))
                tiles[1][n].append(place(ends + [d], [row] * 3 + [inside]))
        for n in range(2):
            ps[n, :, folded] = fold(*tiles[0][n])
            fs[n, :, folded] = fold(*tiles[1][n])
        for n in range(2, 4):
            pack_copy(n, j, True).start()

    pairs(prepare)

    @pl.when(far_end)
    def _():
        for n in direct:
            start_copy(n, tm_next).start()

    for n in range(2):
        for j in range(PAIRS):
            pack_copy(n, j, True).start()

    for ns, buffer, back, spot_of in routes:
        @pl.when((z_place == spot_of) & (tm < 24))
        def _(ns=ns, buffer=buffer, back=back):
            for n in ns:
                via_copy(n, buffer, ns[0], lax.rem(tm + back, 32)).wait_recv()
                pass_copy(n, buffer, ns[0], back + 1).start()

    for n in range(4):
        for j in range(PAIRS):
            pack_copy(n, j, False).wait_recv()

    @pl.when(tm > 0)
    def _():
        for n in range(8):
            start_copy(n, tm_prev).wait_recv()

    def ringed(j, folded, bases):
        row = lax.broadcasted_iota(jnp.int32, (8, CHUNK), 0)
        for h, base in enumerate(bases):
            cols = pl.ds(base, CHUNK)
            pa, pb, fa, fb = pr[1, :, folded], pr[0, :, folded], fr[1, :, folded], fr[0, :, folded]
            i = 4 * h + 3
            d = jnp.where(row < 4, sub_roll(fa, 1 - i), sub_roll(fb, 6 - i))
            d = jnp.where((row == 0) | (row == 7), unfold(pa, pb, i), d)
            drow[:, cols] = jnp.concatenate([depth[:, cols], d], axis=0)
            for f in range(3):
                main = jnp.where(tm == 0, init[f, :, cols], s0[f, :, cols])
                x = jnp.concatenate([main, unfold(fa, fb, 4 * h + f)], axis=0)
                y = jnp.concatenate([a1[f, :, cols], unfold(pa, pb, 4 * h + f)], axis=0)
                s0r[f, :, cols] = x
                q1[f, :, cols] = half_step * x + y

    pairs(ringed)

    def q2_copy(n, j, send):
        up_down = lax.rem(s + (1 if (n == 0) == send else SPACE - 1), SPACE)
        cols = pl.ds(pl.multiple_of(j * CHUNK, CHUNK), CHUNK)
        return copy(q2s.at[n, :, cols], q2r.at[n, :, cols], q2_ss.at[n, j], q2_rs.at[n, j], at(tm, up_down))

    def one(j, folded, bases):
        tiles = [[], []]
        for base in bases:
            cols = pl.ds(base, CHUNK)
            r = ring_rates(q1, drow, base)
            q = []
            for f in range(3):
                x = s0r[f, :ROWS, cols] + r[f][:ROWS]
                s1[f, :, cols] = x
                q.append(half_step * x + a2[f, :, cols])
                q2[f, :ROWS, cols] = q[f]
            tiles[0].append(place([x[8:] for x in q], [7] * 3))
            tiles[1].append(place([x[:8] for x in q], [0] * 3))
        for n in range(2):
            q2s[n, :, folded] = fold(*tiles[n])
            q2_copy(n, j, True).start()

    pairs(one)
    for n in range(2):
        for j in range(PAIRS):
            q2_copy(n, j, False).wait_recv()

    def q2_rows(j, folded, bases):
        for h, base in enumerate(bases):
            for f in range(3):
                q2[f, ROWS:, pl.ds(base, CHUNK)] = unfold(q2r[1, :, folded], q2r[0, :, folded], 4 * h + f)

    pairs(q2_rows)

    def q3_copy(n, j, send):
        up_down = lax.rem(s + (1 if (n % 2 == 0) == send else SPACE - 1), SPACE)
        cols = pl.ds(pl.multiple_of(j * CHUNK, CHUNK), CHUNK)
        return copy(q3s.at[n, :, cols], q3r.at[n, :, cols], q3_ss.at[n, j], q3_rs.at[n, j], at(tm, up_down))

    def two(j, folded, bases):
        tiles = [[], [], [], []]
        for base in bases:
            cols = pl.ds(base, CHUNK)
            r = ring_rates(q2, drow, base)
            top, bottom = [], []
            for f in range(3):
                x, y = s0r[f, :ROWS, cols], s1[f, :, cols]
                z = y + r[f][:ROWS]
                partial[f, :, cols] = y - 0.5 * (x + z)
                q = (step_size * first + start_share) * x + one_share * y + two_share * z
                q3[f, :ROWS, cols] = q
                top.append(q[:8])
                bottom.append(q[8:])
            for n, (parts, row) in enumerate(((bottom, 7), (top, 0), (bottom, 6), (top, 1))):
                tiles[n].append(place(parts, [row] * 3))
        for n in range(4):
            q3s[n, :, folded] = fold(*tiles[n])
        for n in range(2):
            q3_copy(n, j, True).start()

        @pl.when(k == 0)
        def _():
            for n in range(2, 4):
                q3_copy(n, j, True).start()

    pairs(two)
    for n in range(2):
        for j in range(PAIRS):
            q3_copy(n, j, False).wait_recv()

    @pl.when(k == 0)
    def _():
        for n in range(2, 4):
            for j in range(PAIRS):
                q3_copy(n, j, False).wait_recv()

    def q3_rows(j, folded, bases):
        row = lax.broadcasted_iota(jnp.int32, (8, CHUNK), 0)
        for h, base in enumerate(bases):
            for f in range(3):
                i = 4 * h + f
                near_rows = unfold(q3r[1, :, folded], q3r[0, :, folded], i)
                far_rows = jnp.where(row < 4, sub_roll(q3r[3, :, folded], 1 - i), sub_roll(q3r[2, :, folded], 6 - i))
                q3[f, ROWS:, pl.ds(base, CHUNK)] = jnp.where((row == 0) | (row == 7), near_rows, far_rows)

    pairs(q3_rows)

    def three(base):
        cols = pl.ds(base, CHUNK)
        r = ring_rates(q3, drow, base)
        for f in range(3):
            x = r[f] + first * s0r[f, :, cols]
            br[f, :, cols] = x
            boosted[f, :, cols] = x[:ROWS]

    chunks(three)
    give = copy(boosted, other, oth_s.at[0], oth_r.at[0], partner)

    def item_copy(i):
        cols = pl.ds(pl.multiple_of(i * CHUNK, CHUNK), CHUNK)
        return copy(item.at[:, :, cols], ritem.at[:, :, cols], it_s.at[i], it_r.at[i], partner)

    @pl.loop(0, COLS // CHUNK)
    def _(i):
        base = pl.multiple_of(i * CHUNK, CHUNK)
        cols = pl.ds(base, CHUNK)
        r = ring_rates(br, drow, base)
        for f in range(3):
            item[f, :, cols] = jnp.where(k == 0, boosted[f, :, cols] + step_size * r[f][:ROWS], boosted[f, :, cols])
        item_copy(i).start()

    give.start()

    def one_copy(f, sp, send):
        to, by = (sp, s) if send else (s, sp)
        n = to if send else by
        return copy(esum.at[f, :, block(to, k)], rt.at[f, rows(ROWS * by), :], one_s.at[f, n], one_r.at[f, by], at(tm, sp))

    for i in range(COLS // CHUNK):
        item_copy(i).wait_recv()

    def summed(base):
        cols = pl.ds(base, CHUNK)
        for f in range(3):
            esum[f, :, cols] = item[f, :, cols] + ritem[f, :, cols]

    chunks(summed)
    for f in range(3):
        for d in range(1, SPACE):
            one_copy(f, lax.rem(s + d, SPACE), True).start()
    rt[:, rows(ROWS * s), :] = esum[:, :, block(s, k)]

    def depth_pieces(base):
        return (
            (pl.ds(pl.multiple_of(base, 128), PART), pl.ds(128, PART)),
            (pl.ds(pl.multiple_of(lax.rem(base + COLS - 128, COLS), 128), 128), pl.ds(0, 128)),
            (pl.ds(pl.multiple_of(lax.rem(base + PART, COLS), 128), 128), pl.ds(384, 128)),
        )

    def depth_copy(d, n, send):
        sp = lax.rem(s + d, SPACE) if send else lax.rem(s + SPACE - d, SPACE)
        to = sp if send else s
        src, dst = depth_pieces(512 * to + 256 * (owned(to, tm) // 16))[n]
        return copy(depth.at[:, src], dr.at[rows(ROWS * (s if send else sp)), dst], dep_s.at[n, d], dep_r.at[n, d], at(tm, sp))

    for d in range(1, SPACE):
        for n in range(3):
            depth_copy(d, n, True).start()
    for src, dst in depth_pieces(512 * s + 256 * half):
        dr[rows(ROWS * s), dst] = depth[:, src]


    def two_copy(f, n):
        src, dst = et.at[f, rows(OWN * n, OWN), :], ex.at[chip, f, pl.ds(HALO, OWN), :]
        return copy(src, dst, two_s.at[f, n], two_r.at[f, chip], at(owner(s, 16 * k + n), s))

    for f in range(3):
        for d in range(1, SPACE):
            one_copy(f, lax.rem(s + SPACE - d, SPACE), False).wait_recv()
        for t in range(2):
            et[f, 128 * t : 128 * t + 128, :] = rt[f, :, 128 * t : 128 * t + 128].T

        @pl.loop(0, 16)
        def _(m, f=f):
            n = lax.rem(m + spot, 16)

            @pl.when((owner(s, 16 * k + n) != tm) & (chip < CHIPS - 1))
            def _():
                two_copy(f, n).start()

    @pl.when(half == k)
    def _():
        ex[chip, :, HALO : HALO + OWN, :] = et[:, rows(OWN * spot, OWN), :]

    spans = ((0, 2, 16), (2, 6, 8), (7, 10, 16), (10, 14, 8))

    def halo_copy(n, j, width):
        src, dst = (HALO + OWN - width, HALO - width) if n == 0 else (HALO, HALO + OWN)
        return copy(ex.at[j, :, pl.ds(src, width), :], ex.at[j, :, pl.ds(dst, width), :], halo_s.at[n, j], halo_r.at[n, j], nears[n])

    def middle_copy(n):
        return copy(vx.at[MIDDLE], middle.at[n], halo_s.at[n, 15], halo_r.at[n, 15], nears[n])

    def each_halo(j, act):
        for lo, hi, width in spans:
            @pl.when((j >= lo) & (j < hi))
            def _():
                for n in range(2):
                    act(halo_copy(n, j, width))

    for c in (0, 1, 2, 3, 5, 6, 4, 7, 9, 10, 11, 8, 13, 14, 12):
        @pl.when((chip != c) | (half != k))
        def _(c=c):
            for f in range(3):
                src, dst = et.at[f, rows(OWN * spot, OWN), :], ex.at[c, f, pl.ds(HALO, OWN), :]
                copy(src, dst, two_s.at[f, 0], two_r.at[f, c], at(c * 2 + half, s)).wait_recv()

        for lo, hi, width in spans:
            if lo <= c < hi:
                for n in range(2):
                    halo_copy(n, c, width).start()

    for d in range(1, SPACE):
        for n in range(3):
            depth_copy(d, n, False).wait_recv()
    for t in range(4):
        dt[128 * t : 128 * t + 128, :] = dr[:, 128 * t : 128 * t + 128].T


    def scanned(lo, hi, halo, state, send):
        count = OWN + 2 * halo
        d_own = dt[rows(128 - halo + OWN * spot, count), :]

        def stepped(state):
            h, u, v = state
            r = rates(
                h, u, v, d_own * u, d_own * v,
                lambda x: pltpu.roll(x, 1, 0), lambda x: pltpu.roll(x, count - 1, 0),
                lambda x: pltpu.roll(x, 1, 1), lambda x: pltpu.roll(x, 127, 1), lambda x: x,
            )
            return tuple(x + step_size * y for x, y in zip(state, r))

        def body(j, state):
            state = stepped(stepped(state))
            each_halo(j, lambda x: x.wait_recv())
            state = tuple(x + ex[j, f, HALO - halo : HALO + OWN + halo] for f, x in enumerate(state))
            for f in range(3):
                vx[j + 1, f] = state[f][halo : halo + OWN]

            if send:
                give_back(j + 1)
            return state

        return lax.fori_loop(lo, hi, body, state)

    def give_back(j):
        @pl.when((chip != j) | (half != k))
        def _():
            ret_copy(j).start()

    def ret_copy(j):
        return copy(vx.at[j], vt.at[:, rows(OWN * spot, OWN), :], ret_s.at[j], ret_r.at[spot], at(j * 2 + half, s))

    state = scanned(0, MIDDLE, HALO, (jnp.zeros((WIDE, 128), F32),) * 3, False)
    for n in range(2):
        middle_copy(n).start()

    @pl.loop(0, MIDDLE)
    def _(i):
        give_back(1 + lax.rem(chip + i, MIDDLE))

    for n in range(2):
        middle_copy(n).wait_recv()
    state = tuple(jnp.concatenate([middle[0, f], x[HALO : HALO + OWN], middle[1, f]], axis=0) for f, x in enumerate(state))
    state = scanned(MIDDLE, 11, HALO, state, True)
    scanned(11, CHIPS - 1, 8, tuple(x[8:40] for x in state), True)

    @pl.when(chip > 0)
    def _():
        @pl.when(half == k)
        def _():
            vt[:, rows(OWN * spot, OWN), :] = vx[chip]

        @pl.loop(0, 16)
        def _(n):
            t = owner(s, 16 * k + n)

            @pl.when(t != tm)
            def _():
                copy(vx.at[0], vt.at[:, rows(OWN * n, OWN), :], ret_s.at[0], ret_r.at[n], at(t, s)).wait_recv()

    low = lax.broadcasted_iota(jnp.int32, (8, 128), 0) < 4
    for f in range(3):
        for t in range(2):
            cols = slice(128 * t, 128 * t + 128)
            x = vt[f, cols, :].T
            for sp in range(SPACE):
                vr[sp, f, :ROWS, cols] = x[16 * sp : 16 * sp + 16]
                a, b = (16 * sp + 16) % 128, (16 * sp + 120) % 128
                vr[sp, f, ROWS:, cols] = jnp.where(low, x[a : a + 8], x[b : b + 8])

    def row_copy(sp, send):
        to, by = (sp, s) if send else (s, sp)
        return copy(vr.at[to], vout.at[:, :, block(by, k)], row_s.at[sp], row_r.at[by], at(tm, sp))

    def fin_copy(sp, send):
        cols = block(sp, k if send else 1 - k)
        return copy(vout.at[:, :, cols], vout.at[:, :, cols], fin_s.at[sp], fin_r.at[sp], partner)

    for d in range(1, SPACE):
        row_copy(lax.rem(s + d, SPACE), True).start()
    vout[:, :, block(s, k)] = vr[s]
    fin_copy(s, True).start()
    give.wait_recv()

    @pl.when(tm < 31)
    def _():
        for n in range(8):
            start_copy(n, tm_next).wait_send()

    for ns, buffer, back, spot_of in routes:
        @pl.when((z_place == spot_of) & (tm < 24))
        def _(ns=ns, buffer=buffer, back=back):
            for n in ns:
                pass_copy(n, buffer, ns[0], back + 1).wait_send()

    for n in range(4):
        for j in range(PAIRS):
            pack_copy(n, j, True).wait_send()
    for n in range(2):
        for j in range(PAIRS):
            q2_copy(n, j, True).wait_send()
            q3_copy(n, j, True).wait_send()

    @pl.when(k == 0)
    def _():
        for n in range(2, 4):
            for j in range(PAIRS):
                q3_copy(n, j, True).wait_send()

    give.wait_send()
    for i in range(COLS // CHUNK):
        item_copy(i).wait_send()
    for d in range(1, SPACE):
        for n in range(3):
            depth_copy(d, n, True).wait_send()
        for f in range(3):
            one_copy(f, lax.rem(s + d, SPACE), True).wait_send()

    @pl.loop(0, 16)
    def _(n):
        @pl.when((owner(s, 16 * k + n) != tm) & (chip < CHIPS - 1))
        def _():
            for f in range(3):
                two_copy(f, n).wait_send()

        each_halo(n, lambda x: x.wait_send())

    for n in range(2):
        middle_copy(n).wait_send()


    def finish(sp):
        base = pl.multiple_of(sp * CHUNK, CHUNK)
        cols = pl.ds(base, CHUNK)
        d = wide(lambda c: drow[:, c], base)

        def stepped(state):
            h, u, w = state
            r = rates(h, u, w, d * u, d * w, left, right, up, down, lambda x: x)
            return [x + step_size * y for x, y in zip(state, r)]

        state = [wide(lambda c, f=f: vout[f, :, c], base) for f in range(3)]
        a = stepped(state)
        b = stepped(a)
        for f in range(3):
            begin = inner(state[f])[:ROWS]
            ours = jnp.where(k == 0, boosted[f, :, cols], other[f, :, cols])
            y1 = ours + inner(a[f])[:ROWS]
            y2 = esum[f, :, cols] + inner(b[f])[:ROWS]
            start = jnp.where(k == 0, jnp.where(tm == 0, init[f, :, cols], begin), y1)
            end = jnp.where(k == 0, y1, y2)
            out[0, f, :, cols] = start
            out[1, f, :, cols] = partial[f, :, cols] + 0.5 * (start + end)
            out[2, f, :, cols] = end

    @pl.loop(1, SPACE)
    def _(d):
        sp = lax.rem(s + SPACE - d, SPACE)
        row_copy(sp, False).wait_recv()
        fin_copy(sp, True).start()
        fin_copy(lax.rem(sp + 1, SPACE), False).wait_recv()

        @pl.when(d >= 3)
        def _():
            finish(lax.rem(sp + 2, SPACE))

    fin_copy(lax.rem(s + 1, SPACE), False).wait_recv()

    @pl.loop(0, 3)
    def _(i):
        finish(lax.rem(s + 2 * SPACE - 6 - i, SPACE))

    for d in range(1, SPACE):
        row_copy(lax.rem(s + d, SPACE), True).wait_send()
    for sp in range(SPACE):
        fin_copy(sp, True).wait_send()

    @pl.loop(1, 16)
    def _(n):
        @pl.when((chip != n) | (half != k))
        def _():
            ret_copy(n).wait_send()


VM = pl.BlockSpec(memory_space=pltpu.VMEM)


def per_device(fine_nodes, init_state, mean_depth):
    points = fine_nodes[0].reshape(9, ROWS, COLS)

    def vm(*shape):
        return pltpu.VMEM(shape, F32)

    def sems(*shape):
        return [pltpu.SemaphoreType.DMA(shape)] * 2

    flat, ringed = vm(3, ROWS, COLS), vm(3, RING, COLS)
    out = pl.pallas_call(
        coarse_kernel,
        out_shape=jax.ShapeDtypeStruct((3, 3, ROWS, COLS), F32),
        in_specs=[pl.BlockSpec(memory_space=pltpu.HBM)] * 3,
        out_specs=VM,
        scratch_shapes=[
            flat, flat, flat, flat, ringed, vm(RING, COLS), vm(9, ROWS, COLS), flat, vm(ROWS, COLS),
            flat, flat, flat, vm(2, 8, FOLD), vm(2, 8, FOLD), vm(2, 8, FOLD), vm(2, 8, FOLD),
            ringed, ringed, flat, ringed, vm(2, 8, FOLD), vm(2, 8, FOLD), ringed, vm(4, 8, FOLD), vm(4, 8, FOLD),
            ringed, flat, flat, vm(2, 3, ROWS, COLS // 8), vm(2, 3, ROWS, COLS // 8), vm(2, 3, ROWS, COLS // 8),
            vm(3, 128, PART), vm(3, PART, 128), vm(128, 512), vm(512, 128),
            vm(CHIPS, 3, WIDE, 128), vm(CHIPS, 3, OWN, 128), vm(2, 3, OWN, 128), vm(3, PART, 128), vm(SPACE, 3, RING, PART),
            pltpu.SemaphoreType.DMA((5,)), *sems(8), *sems(8), *sems(4, 4), *sems(2, 4), *sems(4, 4), *sems(8), *sems(1), *sems(3, 8), *sems(3, 8), *sems(3, 16),
            *sems(2, 16), *sems(16), *sems(8), *sems(8),
        ],
        compiler_params=pltpu.CompilerParams(collective_id=0, has_side_effects=True, vmem_limit_bytes=40 << 20),
        name="sweep",
    )(*(pltpu.with_memory_space_constraint(x, pltpu.HBM) for x in (points, init_state, mean_depth)))
    return out[None]


def solution(mesh):
    placed = (P("tm", None, None, "space", None), P(None, "space", None), P("space", None))
    return jax.shard_map(
        per_device,
        mesh=mesh,
        in_specs=placed,
        out_specs=P("tm", None, None, "space", None),
        check_vma=False,
    )
```

```python
import functools

import jax
import jax.numpy as jnp
from jax import lax
from jax.experimental import pallas as pl
from jax.experimental.pallas import tpu as pltpu
from jax.sharding import PartitionSpec as P

MESH = pl.DeviceIdType.MESH
F32 = jnp.float32

step_size = 0.3
viscosity = 1.0 / 3.0
coriolis = 0.5
quad_near = 5.0 / 24.0
quad_mid = 1.0 / 3.0
quad_far = -1.0 / 24.0
half_step = 0.5 * step_size
start_share = -(half_step + step_size / 3.0)
one_share = 2.0 * step_size / 3.0
two_share = half_step - step_size / 3.0

ROWS = 16
COLS = 4096
SPACE = 8
CHIPS = 16
PART = 256
OWN = 16
HALO = 16
MIDDLE = 7
WIDE = OWN + 2 * HALO


def rates(h, u, v, de, dn, left, right, up, down, centre):
    nh, nu, nv = viscosity * h, viscosity * u, viscosity * v
    he, hn, hh = 0.5 * de, 0.5 * dn, 0.5 * h
    nhc, nuc, nvc = centre(nh), centre(nu), centre(nv)
    hr = right(nh - he) + left(nh + he) + down(centre(nh - hn)) + up(centre(nh + hn)) - 4.0 * nhc
    ur = right(nu - hh) + left(nu + hh) + down(nuc) + up(nuc) - 4.0 * nuc + coriolis * centre(v)
    vr = right(nv) + left(nv) + down(centre(nv - hh)) + up(centre(nv + hh)) - 4.0 * nvc - coriolis * centre(u)
    return hr, ur, vr


CHUNK = 512
RING = 24


def edges(base):
    if isinstance(base, int):
        lo, hi = (base - 128) % COLS, (base + CHUNK) % COLS
    else:
        lo = pl.multiple_of(lax.rem(base + COLS - 128, COLS), 128)
        hi = pl.multiple_of(lax.rem(base + CHUNK, COLS), 128)
    return pl.ds(lo, 128), pl.ds(base, CHUNK), pl.ds(hi, 128)


def wide(get, base):
    return jnp.concatenate([get(c) for c in edges(base)], axis=1)


def right(x):
    return pltpu.roll(x, x.shape[1] - 1, 1)


def left(x):
    return pltpu.roll(x, 1, 1)


def down(x):
    return pltpu.roll(x, RING - 1, 0)


def up(x):
    return pltpu.roll(x, 1, 0)


def inner(x):
    return x[:, 128 : 128 + CHUNK]


def ring_rates(q, depth, base):
    h, u, v = (wide(lambda c, f=f: q[f, :, c], base) for f in range(3))
    d = wide(lambda c: depth[:, c], base)
    return rates(h, u, v, d * u, d * v, lambda x: inner(left(x)), lambda x: inner(right(x)), up, down, inner)


def chunks(body):
    @pl.loop(0, COLS // CHUNK)
    def _(i):
        body(pl.multiple_of(i * CHUNK, CHUNK))


PAIRS = COLS // CHUNK // 2
FOLD = COLS // 2


def pairs(body):
    @pl.loop(0, PAIRS)
    def _(j):
        base = pl.multiple_of(j * CHUNK, CHUNK)
        body(j, pl.ds(base, CHUNK), [base, pl.multiple_of(base + FOLD, CHUNK)])


def pair(body, j):
    base = j * CHUNK
    body(j, pl.ds(base, CHUNK), [base, base + FOLD])


def sub_roll(x, by):
    by %= 8
    return x if by == 0 else pltpu.roll(x, by, 0)


def pack(parts, at):
    row = lax.broadcasted_iota(jnp.int32, parts[0].shape, 0)
    tile = sub_roll(parts[0], -at)
    for i in range(1, len(parts)):
        tile = jnp.where(row >= 2 * i, sub_roll(parts[i], 2 * i - at), tile)
    return tile


def place(parts, at):
    row = lax.broadcasted_iota(jnp.int32, parts[0].shape, 0)
    tile = sub_roll(parts[0], -at[0])
    for i in range(1, len(parts)):
        tile = jnp.where(row >= i, sub_roll(parts[i], i - at[i]), tile)
    return tile


def fold(first, second):
    row = lax.broadcasted_iota(jnp.int32, first.shape, 0)
    return jnp.where(row < 4, first, sub_roll(second, 4))


def unfold(after, before, i):
    row = lax.broadcasted_iota(jnp.int32, after.shape, 0)
    return jnp.where(row < 4, sub_roll(after, -i), sub_roll(before, 7 - i))


def unpack(after, before, i):
    row = lax.broadcasted_iota(jnp.int32, after.shape, 0)
    return jnp.where(row < 4, sub_roll(after, -2 * i), sub_roll(before, 6 - 2 * i))


def snake(n):
    z, x = n // 4, lax.rem(n, 4)
    return z * 4 + jnp.where(lax.rem(z, 2) == 0, x, 3 - x)


def turned(s, chip):
    return chip // 4 * 4 + lax.rem(chip + 2 * lax.rem(s, 2), 4)


def owner(s, i):
    o = jnp.where(lax.rem(s, 2) == 0, i, 31 - i)
    return turned(s, snake(o // 2)) * 2 + lax.rem(o, 2)


def owned(s, tm):
    o = snake(turned(s, tm // 2)) * 2 + lax.rem(tm, 2)
    return jnp.where(lax.rem(s, 2) == 0, o, 31 - o)


def coarse_kernel(
    points_hbm, init_hbm, depth_hbm,
    out,
    boosted, other, esum, partial, vout, drow, points, init, depth, s0, a1, a2, ps, pr, fs, fr, s0r, q1, s1, q2, q2s, q2r, q3, q3s, q3r, br, item, ritem, relay_a, relay_b, relay_c,
    rt, et, dr, dt, ex, vx, middle, vt, vr,
    in_sem, st_s, st_r, rl_s, rl_r, pk_s, pk_r, q2_ss, q2_rs, q3_ss, q3_rs, it_s, it_r, oth_s, oth_r, one_s, one_r, dep_s, dep_r, two_s, two_r,
    halo_s, halo_r, ret_s, ret_r, row_s, row_r, fin_s, fin_r,
):
    tm = lax.axis_index("tm")
    s = lax.axis_index("space")
    chip, k = tm // 2, lax.rem(tm, 2)
    mine = owned(s, tm)
    half, spot = mine // 16, lax.rem(mine, 16)
    s_next, s_prev = lax.rem(s + 1, SPACE), lax.rem(s + SPACE - 1, SPACE)
    tm_next, tm_prev = lax.rem(tm + 1, 32), lax.rem(tm + 31, 32)
    first = jnp.where(tm == 0, 1.0, 0.0).astype(F32)

    def at(t, sp):
        return {"tm": t, "space": sp}

    def near(step):
        p = lax.rem(32 * s + mine + step + 256, 256)
        return at(owner(p // 32, lax.rem(p, 32)), p // 32)

    partner = at(chip * 2 + 1 - k, s)
    nears = [near(1), near(-1)]

    loads = [pltpu.make_async_copy(points_hbm.at[3 * m : 3 * m + 3], points.at[3 * m : 3 * m + 3], in_sem.at[m]) for m in range(3)]
    loads += [pltpu.make_async_copy(init_hbm, init, in_sem.at[3]), pltpu.make_async_copy(depth_hbm, depth, in_sem.at[4])]
    for n in (2, 0, 1, 4, 3):
        loads[n].start()
    vt[...] = jnp.zeros_like(vt)
    barrier = pltpu.get_barrier_semaphore()
    z, x = tm // 8, lax.rem(tm // 2, 4)
    peers = [
        at(lax.rem(z + dz, 4) * 8 + lax.rem(x + dx, 4) * 2 + c, s)
        for dz in (2, 1, 3, 0) for dx in (2, 1, 3, 0) for c in range(2) if dz or dx
    ] + [partner]
    peers += [at(tm, lax.rem(s + d, SPACE)) for d in range(1, SPACE)]
    peers += [at(t, sp) for t in (tm_next, tm_prev) for sp in (s_next, s_prev)]
    peers += nears
    for p in peers:
        pl.semaphore_signal(barrier, inc=1, device_id=p, device_id_type=MESH)
    pl.semaphore_wait(barrier, len(peers))

    def copy(src, dst, ss, rs, dev):
        return pltpu.make_async_remote_copy(src_ref=src, dst_ref=dst, send_sem=ss, recv_sem=rs, device_id=dev, device_id_type=MESH)

    def block(sp, kk):
        return pl.ds(pl.multiple_of(512 * sp + 256 * kk, PART), PART)

    def rows(start, n=ROWS):
        return pl.ds(pl.multiple_of(start, 8), n)

    loads[2].wait()

    z_place = lax.rem(tm, 8)
    far_end = (z_place == 7) & (tm < 31)
    PIECE = COLS // 8
    direct = range(0, 2)
    routes = ((range(2, 4), relay_a, 6, 1), (range(4, 6), relay_b, 2, 5), (range(6, 8), relay_c, 4, 3))

    def piece(n):
        return pl.ds(PIECE * n, PIECE)

    def start_copy(n, to):
        return copy(points.at[6:9, :, piece(n)], s0.at[:, :, piece(n)], st_s.at[n], st_r.at[n], at(to, s))

    def via_copy(n, buffer, first_piece, to):
        return copy(points.at[6:9, :, piece(n)], buffer.at[n - first_piece], st_s.at[n], rl_r.at[n], at(to, s))

    def pass_copy(n, buffer, first_piece, ahead):
        return copy(buffer.at[n - first_piece], s0.at[:, :, piece(n)], rl_s.at[n], st_r.at[n], at(lax.rem(tm + ahead, 32), s))

    @pl.when((tm < 31) & (z_place != 7))
    def _():
        for n in (0, 4, 1, 5, 2, 6, 3, 7):
            start_copy(n, tm_next).start()

    @pl.when(far_end)
    def _():
        for ns, buffer, back, _ in routes:
            for n in ns:
                via_copy(n, buffer, ns[0], lax.rem(tm + 32 - back, 32)).start()

    for n in (0, 1, 4, 3):
        loads[n].wait()

    def pack_copy(n, j, send):
        up_down = lax.rem(s + (1 if (n % 2 == 0) == send else SPACE - 1), SPACE)
        slot = tm if n < 2 else (tm_next if send else tm_prev)
        cols = pl.ds(j * CHUNK, CHUNK) if isinstance(j, int) else pl.ds(pl.multiple_of(j * CHUNK, CHUNK), CHUNK)
        src, dst = (ps, pr) if n < 2 else (fs, fr)
        return copy(src.at[n % 2, :, cols], dst.at[n % 2, :, cols], pk_s.at[n, j], pk_r.at[n, j], at(slot, up_down))

    def prepare(j, folded, bases):
        tiles = [[], []], [[], []]
        for base in bases:
            cols = pl.ds(base, CHUNK)
            top, bottom = [], []
            for f in range(3):
                p0, p1, p2 = (points[3 * m + f, :, cols] for m in range(3))
                x = (step_size * quad_near - half_step) * p0 + (step_size * quad_mid) * p1 + (step_size * quad_far) * p2
                y = (step_size * quad_far) * p0 + (step_size * quad_mid - half_step) * p1 + (step_size * quad_near) * p2
                a1[f, :, cols] = x
                a2[f, :, cols] = y
                top.append(x[:8])
                bottom.append(x[8:])
            for n, (parts, tile, row, inside) in enumerate(((bottom, 8, 7, 6), (top, 0, 0, 1))):
                d = depth[tile : tile + 8, cols]
                ends = [
                    jnp.where(tm == 31, init[f, tile : tile + 8, cols], points[6 + f, tile : tile + 8, cols]) for f in range(3)
                ]
                tiles[0][n].append(place(parts + [d], [row] * 4))
                tiles[1][n].append(place(ends + [d], [row] * 3 + [inside]))
        for n in range(2):
            ps[n, :, folded] = fold(*tiles[0][n])
            fs[n, :, folded] = fold(*tiles[1][n])
        for n in range(2, 4):
            pack_copy(n, j, True).start()

    pairs(prepare)

    @pl.when(far_end)
    def _():
        for n in direct:
            start_copy(n, tm_next).start()

    for n in range(2):
        for j in range(PAIRS):
            pack_copy(n, j, True).start()

    for ns, buffer, back, spot_of in routes:
        @pl.when((z_place == spot_of) & (tm < 24))
        def _(ns=ns, buffer=buffer, back=back):
            for n in ns:
                via_copy(n, buffer, ns[0], lax.rem(tm + back, 32)).wait_recv()
                pass_copy(n, buffer, ns[0], back + 1).start()

    for n in range(4):
        for j in range(PAIRS):
            pack_copy(n, j, False).wait_recv()

    def ringed(j, folded, bases):
        row = lax.broadcasted_iota(jnp.int32, (8, CHUNK), 0)
        for h, base in enumerate(bases):
            cols = pl.ds(base, CHUNK)
            pa, pb, fa, fb = pr[1, :, folded], pr[0, :, folded], fr[1, :, folded], fr[0, :, folded]
            i = 4 * h + 3
            d = jnp.where(row < 4, sub_roll(fa, 1 - i), sub_roll(fb, 6 - i))
            d = jnp.where((row == 0) | (row == 7), unfold(pa, pb, i), d)
            drow[:, cols] = jnp.concatenate([depth[:, cols], d], axis=0)
            for f in range(3):
                main = jnp.where(tm == 0, init[f, :, cols], s0[f, :, cols])
                x = jnp.concatenate([main, unfold(fa, fb, 4 * h + f)], axis=0)
                y = jnp.concatenate([a1[f, :, cols], unfold(pa, pb, 4 * h + f)], axis=0)
                s0r[f, :, cols] = x
                q1[f, :, cols] = half_step * x + y

    def q2_copy(n, j, send):
        up_down = lax.rem(s + (1 if (n == 0) == send else SPACE - 1), SPACE)
        cols = pl.ds(j * CHUNK, CHUNK) if isinstance(j, int) else pl.ds(pl.multiple_of(j * CHUNK, CHUNK), CHUNK)
        return copy(q2s.at[n, :, cols], q2r.at[n, :, cols], q2_ss.at[n, j], q2_rs.at[n, j], at(tm, up_down))

    def one(j, folded, bases):
        tiles = [[], []]
        for base in bases:
            cols = pl.ds(base, CHUNK)
            r = ring_rates(q1, drow, base)
            q = []
            for f in range(3):
                x = s0r[f, :ROWS, cols] + r[f][:ROWS]
                s1[f, :, cols] = x
                q.append(half_step * x + a2[f, :, cols])
                q2[f, :ROWS, cols] = q[f]
            tiles[0].append(place([x[8:] for x in q], [7] * 3))
            tiles[1].append(place([x[:8] for x in q], [0] * 3))
        for n in range(2):
            q2s[n, :, folded] = fold(*tiles[n])
            q2_copy(n, j, True).start()

    for j in range(PAIRS):
        @pl.when(tm > 0)
        def _(j=j):
            start_copy(j, tm_prev).wait_recv()
            start_copy(j + PAIRS, tm_prev).wait_recv()

        pair(ringed, j)
        if j >= 2:
            pair(one, j - 1)
    pair(one, 3)
    pair(one, 0)

    def q3_copy(n, j, send):
        up_down = lax.rem(s + (1 if (n % 2 == 0) == send else SPACE - 1), SPACE)
        cols = pl.ds(j * CHUNK, CHUNK) if isinstance(j, int) else pl.ds(pl.multiple_of(j * CHUNK, CHUNK), CHUNK)
        return copy(q3s.at[n, :, cols], q3r.at[n, :, cols], q3_ss.at[n, j], q3_rs.at[n, j], at(tm, up_down))

    def two(j, folded, bases):
        for n in range(2):
            q2_copy(n, j, False).wait_recv()
        tiles = [[], [], [], []]
        for h, base in enumerate(bases):
            cols = pl.ds(base, CHUNK)
            for f in range(3):
                q2[f, ROWS:, cols] = unfold(q2r[1, :, folded], q2r[0, :, folded], 4 * h + f)
            r = ring_rates(q2, drow, base)
            top, bottom = [], []
            for f in range(3):
                x, y = s0r[f, :ROWS, cols], s1[f, :, cols]
                z = y + r[f][:ROWS]
                partial[f, :, cols] = y - 0.5 * (x + z)
                q = (step_size * first + start_share) * x + one_share * y + two_share * z
                q3[f, :ROWS, cols] = q
                top.append(q[:8])
                bottom.append(q[8:])
            for n, (parts, row) in enumerate(((bottom, 7), (top, 0), (bottom, 6), (top, 1))):
                tiles[n].append(place(parts, [row] * 3))
        for n in range(4):
            q3s[n, :, folded] = fold(*tiles[n])
        for n in range(2):
            q3_copy(n, j, True).start()

        @pl.when(k == 0)
        def _():
            for n in range(2, 4):
                q3_copy(n, j, True).start()

    for j in (1, 2, 3, 0):
        pair(two, j)

    def q3_rows(j, folded, bases):
        for n in range(2):
            q3_copy(n, j, False).wait_recv()

        @pl.when(k == 0)
        def _():
            for n in range(2, 4):
                q3_copy(n, j, False).wait_recv()

        row = lax.broadcasted_iota(jnp.int32, (8, CHUNK), 0)
        for h, base in enumerate(bases):
            for f in range(3):
                i = 4 * h + f
                near_rows = unfold(q3r[1, :, folded], q3r[0, :, folded], i)
                far_rows = jnp.where(row < 4, sub_roll(q3r[3, :, folded], 1 - i), sub_roll(q3r[2, :, folded], 6 - i))
                q3[f, ROWS:, pl.ds(base, CHUNK)] = jnp.where((row == 0) | (row == 7), near_rows, far_rows)

    def three(j, folded, bases):
        for base in bases:
            cols = pl.ds(base, CHUNK)
            r = ring_rates(q3, drow, base)
            for f in range(3):
                x = r[f] + first * s0r[f, :, cols]
                br[f, :, cols] = x
                boosted[f, :, cols] = x[:ROWS]

    pair(q3_rows, 1)
    pair(q3_rows, 2)
    pair(q3_rows, 3)
    pair(three, 2)
    pair(q3_rows, 0)
    for j in (3, 0, 1):
        pair(three, j)
    give = copy(boosted, other, oth_s.at[0], oth_r.at[0], partner)

    def item_copy(i):
        cols = pl.ds(pl.multiple_of(i * CHUNK, CHUNK), CHUNK)
        return copy(item.at[:, :, cols], ritem.at[:, :, cols], it_s.at[i], it_r.at[i], partner)

    @pl.loop(0, COLS // CHUNK)
    def _(i):
        base = pl.multiple_of(i * CHUNK, CHUNK)
        cols = pl.ds(base, CHUNK)
        r = ring_rates(br, drow, base)
        for f in range(3):
            item[f, :, cols] = jnp.where(k == 0, boosted[f, :, cols] + step_size * r[f][:ROWS], boosted[f, :, cols])
        item_copy(i).start()

    give.start()

    def one_copy(f, sp, send):
        to, by = (sp, s) if send else (s, sp)
        n = to if send else by
        return copy(esum.at[f, :, block(to, k)], rt.at[f, rows(ROWS * by), :], one_s.at[f, n], one_r.at[f, by], at(tm, sp))

    for i in range(COLS // CHUNK):
        item_copy(i).wait_recv()

    def summed(base):
        cols = pl.ds(base, CHUNK)
        for f in range(3):
            esum[f, :, cols] = item[f, :, cols] + ritem[f, :, cols]

    chunks(summed)
    for f in range(3):
        for d in range(1, SPACE):
            one_copy(f, lax.rem(s + d, SPACE), True).start()
    rt[:, rows(ROWS * s), :] = esum[:, :, block(s, k)]

    def depth_pieces(base):
        return (
            (pl.ds(pl.multiple_of(base, 128), PART), pl.ds(128, PART)),
            (pl.ds(pl.multiple_of(lax.rem(base + COLS - 128, COLS), 128), 128), pl.ds(0, 128)),
            (pl.ds(pl.multiple_of(lax.rem(base + PART, COLS), 128), 128), pl.ds(384, 128)),
        )

    def depth_copy(d, n, send):
        sp = lax.rem(s + d, SPACE) if send else lax.rem(s + SPACE - d, SPACE)
        to = sp if send else s
        src, dst = depth_pieces(512 * to + 256 * (owned(to, tm) // 16))[n]
        return copy(depth.at[:, src], dr.at[rows(ROWS * (s if send else sp)), dst], dep_s.at[n, d], dep_r.at[n, d], at(tm, sp))

    for d in range(1, SPACE):
        for n in range(3):
            depth_copy(d, n, True).start()
    for src, dst in depth_pieces(512 * s + 256 * half):
        dr[rows(ROWS * s), dst] = depth[:, src]


    def two_copy(f, n):
        src, dst = et.at[f, rows(OWN * n, OWN), :], ex.at[chip, f, pl.ds(HALO, OWN), :]
        return copy(src, dst, two_s.at[f, n], two_r.at[f, chip], at(owner(s, 16 * k + n), s))

    for f in range(3):
        for d in range(1, SPACE):
            one_copy(f, lax.rem(s + SPACE - d, SPACE), False).wait_recv()
        for t in range(2):
            et[f, 128 * t : 128 * t + 128, :] = rt[f, :, 128 * t : 128 * t + 128].T

        @pl.loop(0, 16)
        def _(m, f=f):
            n = lax.rem(m + spot, 16)

            @pl.when((owner(s, 16 * k + n) != tm) & (chip < CHIPS - 1))
            def _():
                two_copy(f, n).start()

    @pl.when(half == k)
    def _():
        ex[chip, :, HALO : HALO + OWN, :] = et[:, rows(OWN * spot, OWN), :]

    spans = ((0, 2, 16), (2, 6, 8), (7, 10, 16), (10, 14, 8))

    def halo_copy(n, j, width):
        src, dst = (HALO + OWN - width, HALO - width) if n == 0 else (HALO, HALO + OWN)
        return copy(ex.at[j, :, pl.ds(src, width), :], ex.at[j, :, pl.ds(dst, width), :], halo_s.at[n, j], halo_r.at[n, j], nears[n])

    def middle_copy(n):
        return copy(vx.at[MIDDLE], middle.at[n], halo_s.at[n, 15], halo_r.at[n, 15], nears[n])

    def each_halo(j, act):
        for lo, hi, width in spans:
            @pl.when((j >= lo) & (j < hi))
            def _():
                for n in range(2):
                    act(halo_copy(n, j, width))

    for c in (0, 1, 2, 3, 5, 6, 4, 7, 9, 10, 11, 8, 13, 14, 12):
        @pl.when((chip != c) | (half != k))
        def _(c=c):
            for f in range(3):
                src, dst = et.at[f, rows(OWN * spot, OWN), :], ex.at[c, f, pl.ds(HALO, OWN), :]
                copy(src, dst, two_s.at[f, 0], two_r.at[f, c], at(c * 2 + half, s)).wait_recv()

        for lo, hi, width in spans:
            if lo <= c < hi:
                for n in range(2):
                    halo_copy(n, c, width).start()

    for d in range(1, SPACE):
        for n in range(3):
            depth_copy(d, n, False).wait_recv()
    for t in range(4):
        dt[128 * t : 128 * t + 128, :] = dr[:, 128 * t : 128 * t + 128].T


    def scanned(lo, hi, halo, state, send):
        count = OWN + 2 * halo
        d_own = dt[rows(128 - halo + OWN * spot, count), :]

        def stepped(state):
            h, u, v = state
            r = rates(
                h, u, v, d_own * u, d_own * v,
                lambda x: pltpu.roll(x, 1, 0), lambda x: pltpu.roll(x, count - 1, 0),
                lambda x: pltpu.roll(x, 1, 1), lambda x: pltpu.roll(x, 127, 1), lambda x: x,
            )
            return tuple(x + step_size * y for x, y in zip(state, r))

        def body(j, state):
            state = stepped(stepped(state))
            each_halo(j, lambda x: x.wait_recv())
            state = tuple(x + ex[j, f, HALO - halo : HALO + OWN + halo] for f, x in enumerate(state))
            for f in range(3):
                vx[j + 1, f] = state[f][halo : halo + OWN]

            if send:
                give_back(j + 1)
            return state

        return lax.fori_loop(lo, hi, body, state)

    def give_back(j):
        @pl.when((chip != j) | (half != k))
        def _():
            ret_copy(j).start()

    def ret_copy(j):
        return copy(vx.at[j], vt.at[:, rows(OWN * spot, OWN), :], ret_s.at[j], ret_r.at[spot], at(j * 2 + half, s))

    state = scanned(0, MIDDLE, HALO, (jnp.zeros((WIDE, 128), F32),) * 3, False)
    for n in range(2):
        middle_copy(n).start()

    @pl.loop(0, MIDDLE)
    def _(i):
        give_back(1 + lax.rem(chip + i, MIDDLE))

    for n in range(2):
        middle_copy(n).wait_recv()
    state = tuple(jnp.concatenate([middle[0, f], x[HALO : HALO + OWN], middle[1, f]], axis=0) for f, x in enumerate(state))
    state = scanned(MIDDLE, 11, HALO, state, True)
    scanned(11, CHIPS - 1, 8, tuple(x[8:40] for x in state), True)

    @pl.when(chip > 0)
    def _():
        @pl.when(half == k)
        def _():
            vt[:, rows(OWN * spot, OWN), :] = vx[chip]

        @pl.loop(0, 16)
        def _(n):
            t = owner(s, 16 * k + n)

            @pl.when(t != tm)
            def _():
                copy(vx.at[0], vt.at[:, rows(OWN * n, OWN), :], ret_s.at[0], ret_r.at[n], at(t, s)).wait_recv()

    low = lax.broadcasted_iota(jnp.int32, (8, 128), 0) < 4
    for f in range(3):
        for t in range(2):
            cols = slice(128 * t, 128 * t + 128)
            x = vt[f, cols, :].T
            for sp in range(SPACE):
                vr[sp, f, :ROWS, cols] = x[16 * sp : 16 * sp + 16]
                a, b = (16 * sp + 16) % 128, (16 * sp + 120) % 128
                vr[sp, f, ROWS:, cols] = jnp.where(low, x[a : a + 8], x[b : b + 8])

    def row_copy(sp, send):
        to, by = (sp, s) if send else (s, sp)
        return copy(vr.at[to], vout.at[:, :, block(by, k)], row_s.at[sp], row_r.at[by], at(tm, sp))

    def fin_copy(sp, send):
        cols = block(sp, k if send else 1 - k)
        return copy(vout.at[:, :, cols], vout.at[:, :, cols], fin_s.at[sp], fin_r.at[sp], partner)

    for d in range(1, SPACE):
        row_copy(lax.rem(s + d, SPACE), True).start()
    vout[:, :, block(s, k)] = vr[s]
    fin_copy(s, True).start()
    give.wait_recv()

    @pl.when(tm < 31)
    def _():
        for n in range(8):
            start_copy(n, tm_next).wait_send()

    for ns, buffer, back, spot_of in routes:
        @pl.when((z_place == spot_of) & (tm < 24))
        def _(ns=ns, buffer=buffer, back=back):
            for n in ns:
                pass_copy(n, buffer, ns[0], back + 1).wait_send()

    for n in range(4):
        for j in range(PAIRS):
            pack_copy(n, j, True).wait_send()
    for n in range(2):
        for j in range(PAIRS):
            q2_copy(n, j, True).wait_send()
            q3_copy(n, j, True).wait_send()

    @pl.when(k == 0)
    def _():
        for n in range(2, 4):
            for j in range(PAIRS):
                q3_copy(n, j, True).wait_send()

    give.wait_send()
    for i in range(COLS // CHUNK):
        item_copy(i).wait_send()
    for d in range(1, SPACE):
        for n in range(3):
            depth_copy(d, n, True).wait_send()
        for f in range(3):
            one_copy(f, lax.rem(s + d, SPACE), True).wait_send()

    @pl.loop(0, 16)
    def _(n):
        @pl.when((owner(s, 16 * k + n) != tm) & (chip < CHIPS - 1))
        def _():
            for f in range(3):
                two_copy(f, n).wait_send()

        each_halo(n, lambda x: x.wait_send())

    for n in range(2):
        middle_copy(n).wait_send()


    def finish(sp):
        base = pl.multiple_of(sp * CHUNK, CHUNK)
        cols = pl.ds(base, CHUNK)
        d = wide(lambda c: drow[:, c], base)

        def stepped(state):
            h, u, w = state
            r = rates(h, u, w, d * u, d * w, left, right, up, down, lambda x: x)
            return [x + step_size * y for x, y in zip(state, r)]

        state = [wide(lambda c, f=f: vout[f, :, c], base) for f in range(3)]
        a = stepped(state)
        b = stepped(a)
        for f in range(3):
            begin = inner(state[f])[:ROWS]
            ours = jnp.where(k == 0, boosted[f, :, cols], other[f, :, cols])
            y1 = ours + inner(a[f])[:ROWS]
            y2 = esum[f, :, cols] + inner(b[f])[:ROWS]
            start = jnp.where(k == 0, jnp.where(tm == 0, init[f, :, cols], begin), y1)
            end = jnp.where(k == 0, y1, y2)
            out[0, f, :, cols] = start
            out[1, f, :, cols] = partial[f, :, cols] + 0.5 * (start + end)
            out[2, f, :, cols] = end

    @pl.loop(1, SPACE)
    def _(d):
        sp = lax.rem(s + SPACE - d, SPACE)
        row_copy(sp, False).wait_recv()
        fin_copy(sp, True).start()
        fin_copy(lax.rem(sp + 1, SPACE), False).wait_recv()

        @pl.when(d >= 3)
        def _():
            finish(lax.rem(sp + 2, SPACE))

    fin_copy(lax.rem(s + 1, SPACE), False).wait_recv()

    @pl.loop(0, 3)
    def _(i):
        finish(lax.rem(s + 2 * SPACE - 6 - i, SPACE))

    for d in range(1, SPACE):
        row_copy(lax.rem(s + d, SPACE), True).wait_send()
    for sp in range(SPACE):
        fin_copy(sp, True).wait_send()

    @pl.loop(1, 16)
    def _(n):
        @pl.when((chip != n) | (half != k))
        def _():
            ret_copy(n).wait_send()


VM = pl.BlockSpec(memory_space=pltpu.VMEM)


def per_device(fine_nodes, init_state, mean_depth):
    points = fine_nodes[0].reshape(9, ROWS, COLS)

    def vm(*shape):
        return pltpu.VMEM(shape, F32)

    def sems(*shape):
        return [pltpu.SemaphoreType.DMA(shape)] * 2

    flat, ringed = vm(3, ROWS, COLS), vm(3, RING, COLS)
    out = pl.pallas_call(
        coarse_kernel,
        out_shape=jax.ShapeDtypeStruct((3, 3, ROWS, COLS), F32),
        in_specs=[pl.BlockSpec(memory_space=pltpu.HBM)] * 3,
        out_specs=VM,
        scratch_shapes=[
            flat, flat, flat, flat, ringed, vm(RING, COLS), vm(9, ROWS, COLS), flat, vm(ROWS, COLS),
            flat, flat, flat, vm(2, 8, FOLD), vm(2, 8, FOLD), vm(2, 8, FOLD), vm(2, 8, FOLD),
            ringed, ringed, flat, ringed, vm(2, 8, FOLD), vm(2, 8, FOLD), ringed, vm(4, 8, FOLD), vm(4, 8, FOLD),
            ringed, flat, flat, vm(2, 3, ROWS, COLS // 8), vm(2, 3, ROWS, COLS // 8), vm(2, 3, ROWS, COLS // 8),
            vm(3, 128, PART), vm(3, PART, 128), vm(128, 512), vm(512, 128),
            vm(CHIPS, 3, WIDE, 128), vm(CHIPS, 3, OWN, 128), vm(2, 3, OWN, 128), vm(3, PART, 128), vm(SPACE, 3, RING, PART),
            pltpu.SemaphoreType.DMA((5,)), *sems(8), *sems(8), *sems(4, 4), *sems(2, 4), *sems(4, 4), *sems(8), *sems(1), *sems(3, 8), *sems(3, 8), *sems(3, 16),
            *sems(2, 16), *sems(16), *sems(8), *sems(8),
        ],
        compiler_params=pltpu.CompilerParams(collective_id=0, has_side_effects=True, vmem_limit_bytes=40 << 20),
        name="sweep",
    )(*(pltpu.with_memory_space_constraint(x, pltpu.HBM) for x in (points, init_state, mean_depth)))
    return out[None]


def solution(mesh):
    placed = (P("tm", None, None, "space", None), P(None, "space", None), P("space", None))
    return jax.shard_map(
        per_device,
        mesh=mesh,
        in_specs=placed,
        out_specs=P("tm", None, None, "space", None),
        check_vma=False,
    )
```

```python
import functools

import jax
import jax.numpy as jnp
from jax import lax
from jax.experimental import pallas as pl
from jax.experimental.pallas import tpu as pltpu
from jax.sharding import PartitionSpec as P

MESH = pl.DeviceIdType.MESH
F32 = jnp.float32

step_size = 0.3
viscosity = 1.0 / 3.0
coriolis = 0.5
quad_near = 5.0 / 24.0
quad_mid = 1.0 / 3.0
quad_far = -1.0 / 24.0
half_step = 0.5 * step_size
start_share = -(half_step + step_size / 3.0)
one_share = 2.0 * step_size / 3.0
two_share = half_step - step_size / 3.0

ROWS = 16
COLS = 4096
SPACE = 8
CHIPS = 16
PART = 256
OWN = 16
HALO = 16
MIDDLE = 7
WIDE = OWN + 2 * HALO


def rates(h, u, v, de, dn, left, right, up, down, centre):
    nh, nu, nv = viscosity * h, viscosity * u, viscosity * v
    he, hn, hh = 0.5 * de, 0.5 * dn, 0.5 * h
    nhc, nuc, nvc = centre(nh), centre(nu), centre(nv)
    hr = right(nh - he) + left(nh + he) + down(centre(nh - hn)) + up(centre(nh + hn)) - 4.0 * nhc
    ur = right(nu - hh) + left(nu + hh) + down(nuc) + up(nuc) - 4.0 * nuc + coriolis * centre(v)
    vr = right(nv) + left(nv) + down(centre(nv - hh)) + up(centre(nv + hh)) - 4.0 * nvc - coriolis * centre(u)
    return hr, ur, vr


CHUNK = 512
RING = 24


def edges(base):
    if isinstance(base, int):
        lo, hi = (base - 128) % COLS, (base + CHUNK) % COLS
    else:
        lo = pl.multiple_of(lax.rem(base + COLS - 128, COLS), 128)
        hi = pl.multiple_of(lax.rem(base + CHUNK, COLS), 128)
    return pl.ds(lo, 128), pl.ds(base, CHUNK), pl.ds(hi, 128)


def wide(get, base):
    return jnp.concatenate([get(c) for c in edges(base)], axis=1)


def right(x):
    return pltpu.roll(x, x.shape[1] - 1, 1)


def left(x):
    return pltpu.roll(x, 1, 1)


def down(x):
    return pltpu.roll(x, RING - 1, 0)


def up(x):
    return pltpu.roll(x, 1, 0)


def inner(x):
    return x[:, 128 : 128 + CHUNK]


def ring_rates(q, depth, base):
    h, u, v = (wide(lambda c, f=f: q[f, :, c], base) for f in range(3))
    d = wide(lambda c: depth[:, c], base)
    return rates(h, u, v, d * u, d * v, lambda x: inner(left(x)), lambda x: inner(right(x)), up, down, inner)


def chunks(body):
    @pl.loop(0, COLS // CHUNK)
    def _(i):
        body(pl.multiple_of(i * CHUNK, CHUNK))


PAIRS = COLS // CHUNK // 2
FOLD = COLS // 2


def pairs(body):
    @pl.loop(0, PAIRS)
    def _(j):
        base = pl.multiple_of(j * CHUNK, CHUNK)
        body(j, pl.ds(base, CHUNK), [base, pl.multiple_of(base + FOLD, CHUNK)])


def pair(body, j):
    base = j * CHUNK
    body(j, pl.ds(base, CHUNK), [base, base + FOLD])


def sub_roll(x, by):
    by %= 8
    return x if by == 0 else pltpu.roll(x, by, 0)


def pack(parts, at):
    row = lax.broadcasted_iota(jnp.int32, parts[0].shape, 0)
    tile = sub_roll(parts[0], -at)
    for i in range(1, len(parts)):
        tile = jnp.where(row >= 2 * i, sub_roll(parts[i], 2 * i - at), tile)
    return tile


def place(parts, at):
    row = lax.broadcasted_iota(jnp.int32, parts[0].shape, 0)
    tile = sub_roll(parts[0], -at[0])
    for i in range(1, len(parts)):
        tile = jnp.where(row >= i, sub_roll(parts[i], i - at[i]), tile)
    return tile


def fold(first, second):
    row = lax.broadcasted_iota(jnp.int32, first.shape, 0)
    return jnp.where(row < 4, first, sub_roll(second, 4))


def unfold(after, before, i):
    row = lax.broadcasted_iota(jnp.int32, after.shape, 0)
    return jnp.where(row < 4, sub_roll(after, -i), sub_roll(before, 7 - i))


def unpack(after, before, i):
    row = lax.broadcasted_iota(jnp.int32, after.shape, 0)
    return jnp.where(row < 4, sub_roll(after, -2 * i), sub_roll(before, 6 - 2 * i))


def snake(n):
    z, x = n // 4, lax.rem(n, 4)
    return z * 4 + jnp.where(lax.rem(z, 2) == 0, x, 3 - x)


def turned(s, chip):
    return chip // 4 * 4 + lax.rem(chip + 2 * lax.rem(s, 2), 4)


def owner(s, i):
    o = jnp.where(lax.rem(s, 2) == 0, i, 31 - i)
    return turned(s, snake(o // 2)) * 2 + lax.rem(o, 2)


def owned(s, tm):
    o = snake(turned(s, tm // 2)) * 2 + lax.rem(tm, 2)
    return jnp.where(lax.rem(s, 2) == 0, o, 31 - o)


def coarse_kernel(
    points_hbm, init_hbm, depth_hbm,
    out,
    boosted, other, esum, partial, vout, vob, vh, drow, points, init, depth, s0, a1, a2, ps, pr, fs, fr, s0r, q1, s1, q2, q2s, q2r, q3, q3s, q3r, br, item, ritem, relay_a, relay_b, relay_c,
    rt, et, dr, dt, ex, vx, middle, vt, vr, vb,
    in_sem, st_s, st_r, rl_s, rl_r, pk_s, pk_r, q2_ss, q2_rs, q3_ss, q3_rs, it_s, it_r, oth_s, oth_r, one_s, one_r, dep_s, dep_r, two_s, two_r,
    halo_s, halo_r, ret_s, ret_r, row_s, row_r, fin_s, fin_r,
):
    tm = lax.axis_index("tm")
    s = lax.axis_index("space")
    chip, k = tm // 2, lax.rem(tm, 2)
    mine = owned(s, tm)
    half, spot = mine // 16, lax.rem(mine, 16)
    s_next, s_prev = lax.rem(s + 1, SPACE), lax.rem(s + SPACE - 1, SPACE)
    tm_next, tm_prev = lax.rem(tm + 1, 32), lax.rem(tm + 31, 32)
    first = jnp.where(tm == 0, 1.0, 0.0).astype(F32)

    def at(t, sp):
        return {"tm": t, "space": sp}

    def near(step):
        p = lax.rem(32 * s + mine + step + 256, 256)
        return at(owner(p // 32, lax.rem(p, 32)), p // 32)

    partner = at(chip * 2 + 1 - k, s)
    nears = [near(1), near(-1)]

    loads = [pltpu.make_async_copy(points_hbm.at[3 * m : 3 * m + 3], points.at[3 * m : 3 * m + 3], in_sem.at[m]) for m in range(3)]
    loads += [pltpu.make_async_copy(init_hbm, init, in_sem.at[3]), pltpu.make_async_copy(depth_hbm, depth, in_sem.at[4])]
    for n in (2, 0, 1, 4, 3):
        loads[n].start()
    vt[...] = jnp.zeros_like(vt)
    barrier = pltpu.get_barrier_semaphore()
    z, x = tm // 8, lax.rem(tm // 2, 4)
    peers = [
        at(lax.rem(z + dz, 4) * 8 + lax.rem(x + dx, 4) * 2 + c, s)
        for dz in (2, 1, 3, 0) for dx in (2, 1, 3, 0) for c in range(2) if dz or dx
    ] + [partner]
    peers += [at(tm, lax.rem(s + d, SPACE)) for d in range(1, SPACE)]
    peers += [at(t, sp) for t in (tm_next, tm_prev) for sp in (s_next, s_prev)]
    peers += nears
    for p in peers:
        pl.semaphore_signal(barrier, inc=1, device_id=p, device_id_type=MESH)
    pl.semaphore_wait(barrier, len(peers))

    def copy(src, dst, ss, rs, dev):
        return pltpu.make_async_remote_copy(src_ref=src, dst_ref=dst, send_sem=ss, recv_sem=rs, device_id=dev, device_id_type=MESH)

    def block(sp, kk):
        return pl.ds(pl.multiple_of(512 * sp + 256 * kk, PART), PART)

    def rows(start, n=ROWS):
        return pl.ds(pl.multiple_of(start, 8), n)

    loads[2].wait()

    z_place = lax.rem(tm, 8)
    far_end = (z_place == 7) & (tm < 31)
    PIECE = COLS // 8
    direct = range(0, 2)
    routes = ((range(2, 4), relay_a, 6, 1), (range(4, 6), relay_b, 2, 5), (range(6, 8), relay_c, 4, 3))

    def piece(n):
        return pl.ds(PIECE * n, PIECE)

    def start_copy(n, to):
        return copy(points.at[6:9, :, piece(n)], s0.at[:, :, piece(n)], st_s.at[n], st_r.at[n], at(to, s))

    def via_copy(n, buffer, first_piece, to):
        return copy(points.at[6:9, :, piece(n)], buffer.at[n - first_piece], st_s.at[n], rl_r.at[n], at(to, s))

    def pass_copy(n, buffer, first_piece, ahead):
        return copy(buffer.at[n - first_piece], s0.at[:, :, piece(n)], rl_s.at[n], st_r.at[n], at(lax.rem(tm + ahead, 32), s))

    @pl.when((tm < 31) & (z_place != 7))
    def _():
        for n in (0, 4, 1, 5, 2, 6, 3, 7):
            start_copy(n, tm_next).start()

    @pl.when(far_end)
    def _():
        for ns, buffer, back, _ in routes:
            for n in ns:
                via_copy(n, buffer, ns[0], lax.rem(tm + 32 - back, 32)).start()

    for n in (0, 1, 4, 3):
        loads[n].wait()

    def pack_copy(n, j, send):
        up_down = lax.rem(s + (1 if (n % 2 == 0) == send else SPACE - 1), SPACE)
        slot = tm if n < 2 else (tm_next if send else tm_prev)
        cols = pl.ds(j * CHUNK, CHUNK) if isinstance(j, int) else pl.ds(pl.multiple_of(j * CHUNK, CHUNK), CHUNK)
        src, dst = (ps, pr) if n < 2 else (fs, fr)
        return copy(src.at[n % 2, :, cols], dst.at[n % 2, :, cols], pk_s.at[n, j], pk_r.at[n, j], at(slot, up_down))

    def prepare(j, folded, bases):
        tiles = [[], []], [[], []]
        for base in bases:
            cols = pl.ds(base, CHUNK)
            top, bottom = [], []
            for f in range(3):
                p0, p1, p2 = (points[3 * m + f, :, cols] for m in range(3))
                x = (step_size * quad_near - half_step) * p0 + (step_size * quad_mid) * p1 + (step_size * quad_far) * p2
                y = (step_size * quad_far) * p0 + (step_size * quad_mid - half_step) * p1 + (step_size * quad_near) * p2
                a1[f, :, cols] = x
                a2[f, :, cols] = y
                top.append(x[:8])
                bottom.append(x[8:])
            for n, (parts, tile, row, inside) in enumerate(((bottom, 8, 7, 6), (top, 0, 0, 1))):
                d = depth[tile : tile + 8, cols]
                ends = [
                    jnp.where(tm == 31, init[f, tile : tile + 8, cols], points[6 + f, tile : tile + 8, cols]) for f in range(3)
                ]
                tiles[0][n].append(place(parts + [d], [row] * 4))
                tiles[1][n].append(place(ends + [d], [row] * 3 + [inside]))
        for n in range(2):
            ps[n, :, folded] = fold(*tiles[0][n])
            fs[n, :, folded] = fold(*tiles[1][n])
        for n in range(2, 4):
            pack_copy(n, j, True).start()

    pairs(prepare)

    @pl.when(far_end)
    def _():
        for n in direct:
            start_copy(n, tm_next).start()

    for n in range(2):
        for j in range(PAIRS):
            pack_copy(n, j, True).start()

    for ns, buffer, back, spot_of in routes:
        @pl.when((z_place == spot_of) & (tm < 24))
        def _(ns=ns, buffer=buffer, back=back):
            for n in ns:
                via_copy(n, buffer, ns[0], lax.rem(tm + back, 32)).wait_recv()
                pass_copy(n, buffer, ns[0], back + 1).start()

    for n in range(4):
        for j in range(PAIRS):
            pack_copy(n, j, False).wait_recv()

    def ringed(j, folded, bases):
        row = lax.broadcasted_iota(jnp.int32, (8, CHUNK), 0)
        for h, base in enumerate(bases):
            cols = pl.ds(base, CHUNK)
            pa, pb, fa, fb = pr[1, :, folded], pr[0, :, folded], fr[1, :, folded], fr[0, :, folded]
            i = 4 * h + 3
            d = jnp.where(row < 4, sub_roll(fa, 1 - i), sub_roll(fb, 6 - i))
            d = jnp.where((row == 0) | (row == 7), unfold(pa, pb, i), d)
            drow[:, cols] = jnp.concatenate([depth[:, cols], d], axis=0)
            for f in range(3):
                main = jnp.where(tm == 0, init[f, :, cols], s0[f, :, cols])
                x = jnp.concatenate([main, unfold(fa, fb, 4 * h + f)], axis=0)
                y = jnp.concatenate([a1[f, :, cols], unfold(pa, pb, 4 * h + f)], axis=0)
                s0r[f, :, cols] = x
                q1[f, :, cols] = half_step * x + y

    def q2_copy(n, j, send):
        up_down = lax.rem(s + (1 if (n == 0) == send else SPACE - 1), SPACE)
        cols = pl.ds(j * CHUNK, CHUNK) if isinstance(j, int) else pl.ds(pl.multiple_of(j * CHUNK, CHUNK), CHUNK)
        return copy(q2s.at[n, :, cols], q2r.at[n, :, cols], q2_ss.at[n, j], q2_rs.at[n, j], at(tm, up_down))

    def one(j, folded, bases):
        tiles = [[], []]
        for base in bases:
            cols = pl.ds(base, CHUNK)
            r = ring_rates(q1, drow, base)
            q = []
            for f in range(3):
                x = s0r[f, :ROWS, cols] + r[f][:ROWS]
                s1[f, :, cols] = x
                q.append(half_step * x + a2[f, :, cols])
                q2[f, :ROWS, cols] = q[f]
            tiles[0].append(place([x[8:] for x in q], [7] * 3))
            tiles[1].append(place([x[:8] for x in q], [0] * 3))
        for n in range(2):
            q2s[n, :, folded] = fold(*tiles[n])
            q2_copy(n, j, True).start()

    for j in range(PAIRS):
        @pl.when(tm > 0)
        def _(j=j):
            start_copy(j, tm_prev).wait_recv()
            start_copy(j + PAIRS, tm_prev).wait_recv()

        pair(ringed, j)
        if j >= 2:
            pair(one, j - 1)
    pair(one, 3)
    pair(one, 0)

    def q3_copy(n, j, send):
        up_down = lax.rem(s + (1 if (n % 2 == 0) == send else SPACE - 1), SPACE)
        cols = pl.ds(j * CHUNK, CHUNK) if isinstance(j, int) else pl.ds(pl.multiple_of(j * CHUNK, CHUNK), CHUNK)
        return copy(q3s.at[n, :, cols], q3r.at[n, :, cols], q3_ss.at[n, j], q3_rs.at[n, j], at(tm, up_down))

    def two(j, folded, bases):
        for n in range(2):
            q2_copy(n, j, False).wait_recv()
        tiles = [[], [], [], []]
        for h, base in enumerate(bases):
            cols = pl.ds(base, CHUNK)
            for f in range(3):
                q2[f, ROWS:, cols] = unfold(q2r[1, :, folded], q2r[0, :, folded], 4 * h + f)
            r = ring_rates(q2, drow, base)
            top, bottom = [], []
            for f in range(3):
                x, y = s0r[f, :ROWS, cols], s1[f, :, cols]
                z = y + r[f][:ROWS]
                partial[f, :, cols] = y - 0.5 * (x + z)
                q = (step_size * first + start_share) * x + one_share * y + two_share * z
                q3[f, :ROWS, cols] = q
                top.append(q[:8])
                bottom.append(q[8:])
            for n, (parts, row) in enumerate(((bottom, 7), (top, 0), (bottom, 6), (top, 1))):
                tiles[n].append(place(parts, [row] * 3))
        for n in range(4):
            q3s[n, :, folded] = fold(*tiles[n])
        for n in range(2):
            q3_copy(n, j, True).start()

        @pl.when(k == 0)
        def _():
            for n in range(2, 4):
                q3_copy(n, j, True).start()

    for j in (1, 2, 3, 0):
        pair(two, j)

    def q3_rows(j, folded, bases):
        for n in range(2):
            q3_copy(n, j, False).wait_recv()

        @pl.when(k == 0)
        def _():
            for n in range(2, 4):
                q3_copy(n, j, False).wait_recv()

        row = lax.broadcasted_iota(jnp.int32, (8, CHUNK), 0)
        for h, base in enumerate(bases):
            for f in range(3):
                i = 4 * h + f
                near_rows = unfold(q3r[1, :, folded], q3r[0, :, folded], i)
                far_rows = jnp.where(row < 4, sub_roll(q3r[3, :, folded], 1 - i), sub_roll(q3r[2, :, folded], 6 - i))
                q3[f, ROWS:, pl.ds(base, CHUNK)] = jnp.where((row == 0) | (row == 7), near_rows, far_rows)

    def three(j, folded, bases):
        for base in bases:
            cols = pl.ds(base, CHUNK)
            r = ring_rates(q3, drow, base)
            for f in range(3):
                x = r[f] + first * s0r[f, :, cols]
                br[f, :, cols] = x
                boosted[f, :, cols] = x[:ROWS]

    pair(q3_rows, 1)
    pair(q3_rows, 2)
    pair(q3_rows, 3)
    pair(three, 2)
    pair(q3_rows, 0)
    for j in (3, 0, 1):
        pair(three, j)
    give = copy(boosted, other, oth_s.at[0], oth_r.at[0], partner)

    def item_copy(i):
        cols = pl.ds(pl.multiple_of(i * CHUNK, CHUNK), CHUNK)
        return copy(item.at[:, :, cols], ritem.at[:, :, cols], it_s.at[i], it_r.at[i], partner)

    @pl.loop(0, COLS // CHUNK)
    def _(i):
        base = pl.multiple_of(i * CHUNK, CHUNK)
        cols = pl.ds(base, CHUNK)
        r = ring_rates(br, drow, base)
        for f in range(3):
            item[f, :, cols] = jnp.where(k == 0, boosted[f, :, cols] + step_size * r[f][:ROWS], boosted[f, :, cols])
        item_copy(i).start()

    give.start()

    def one_copy(f, sp, send):
        to, by = (sp, s) if send else (s, sp)
        n = to if send else by
        return copy(esum.at[f, :, block(to, k)], rt.at[f, rows(ROWS * by), :], one_s.at[f, n], one_r.at[f, by], at(tm, sp))

    for i in range(COLS // CHUNK):
        item_copy(i).wait_recv()

    def summed(base):
        cols = pl.ds(base, CHUNK)
        for f in range(3):
            esum[f, :, cols] = item[f, :, cols] + ritem[f, :, cols]

    chunks(summed)
    for f in range(3):
        for d in range(1, SPACE):
            one_copy(f, lax.rem(s + d, SPACE), True).start()
    rt[:, rows(ROWS * s), :] = esum[:, :, block(s, k)]

    def depth_pieces(base):
        return (
            (pl.ds(pl.multiple_of(base, 128), PART), pl.ds(128, PART)),
            (pl.ds(pl.multiple_of(lax.rem(base + COLS - 128, COLS), 128), 128), pl.ds(0, 128)),
            (pl.ds(pl.multiple_of(lax.rem(base + PART, COLS), 128), 128), pl.ds(384, 128)),
        )

    def depth_copy(d, n, send):
        sp = lax.rem(s + d, SPACE) if send else lax.rem(s + SPACE - d, SPACE)
        to = sp if send else s
        src, dst = depth_pieces(512 * to + 256 * (owned(to, tm) // 16))[n]
        return copy(depth.at[:, src], dr.at[rows(ROWS * (s if send else sp)), dst], dep_s.at[n, d], dep_r.at[n, d], at(tm, sp))

    for d in range(1, SPACE):
        for n in range(3):
            depth_copy(d, n, True).start()
    for src, dst in depth_pieces(512 * s + 256 * half):
        dr[rows(ROWS * s), dst] = depth[:, src]


    def two_copy(f, n):
        src, dst = et.at[f, rows(OWN * n, OWN), :], ex.at[chip, f, pl.ds(HALO, OWN), :]
        return copy(src, dst, two_s.at[f, n], two_r.at[f, chip], at(owner(s, 16 * k + n), s))

    for f in range(3):
        for d in range(1, SPACE):
            one_copy(f, lax.rem(s + SPACE - d, SPACE), False).wait_recv()
        for t in range(2):
            et[f, 128 * t : 128 * t + 128, :] = rt[f, :, 128 * t : 128 * t + 128].T

        @pl.loop(0, 16)
        def _(m, f=f):
            n = lax.rem(m + spot, 16)

            @pl.when((owner(s, 16 * k + n) != tm) & (chip < CHIPS - 1))
            def _():
                two_copy(f, n).start()

    @pl.when(half == k)
    def _():
        ex[chip, :, HALO : HALO + OWN, :] = et[:, rows(OWN * spot, OWN), :]

    spans = ((0, 2, 16), (2, 6, 8), (7, 10, 16), (10, 14, 8))

    def halo_copy(n, j, width):
        src, dst = (HALO + OWN - width, HALO - width) if n == 0 else (HALO, HALO + OWN)
        return copy(ex.at[j, :, pl.ds(src, width), :], ex.at[j, :, pl.ds(dst, width), :], halo_s.at[n, j], halo_r.at[n, j], nears[n])

    def middle_copy(n):
        return copy(vx.at[MIDDLE], middle.at[n], halo_s.at[n, 15], halo_r.at[n, 15], nears[n])

    def each_halo(j, act):
        for lo, hi, width in spans:
            @pl.when((j >= lo) & (j < hi))
            def _():
                for n in range(2):
                    act(halo_copy(n, j, width))

    for c in (0, 1, 2, 3, 5, 6, 4, 7, 9, 10, 11, 8, 13, 14, 12):
        @pl.when((chip != c) | (half != k))
        def _(c=c):
            for f in range(3):
                src, dst = et.at[f, rows(OWN * spot, OWN), :], ex.at[c, f, pl.ds(HALO, OWN), :]
                copy(src, dst, two_s.at[f, 0], two_r.at[f, c], at(c * 2 + half, s)).wait_recv()

        for lo, hi, width in spans:
            if lo <= c < hi:
                for n in range(2):
                    halo_copy(n, c, width).start()

    for d in range(1, SPACE):
        for n in range(3):
            depth_copy(d, n, False).wait_recv()
    for t in range(4):
        dt[128 * t : 128 * t + 128, :] = dr[:, 128 * t : 128 * t + 128].T


    def scanned(lo, hi, halo, state, send):
        count = OWN + 2 * halo
        d_own = dt[rows(128 - halo + OWN * spot, count), :]

        def stepped(state):
            h, u, v = state
            r = rates(
                h, u, v, d_own * u, d_own * v,
                lambda x: pltpu.roll(x, 1, 0), lambda x: pltpu.roll(x, count - 1, 0),
                lambda x: pltpu.roll(x, 1, 1), lambda x: pltpu.roll(x, 127, 1), lambda x: x,
            )
            return tuple(x + step_size * y for x, y in zip(state, r))

        def body(j, state):
            state = stepped(stepped(state))
            each_halo(j, lambda x: x.wait_recv())
            state = tuple(x + ex[j, f, HALO - halo : HALO + OWN + halo] for f, x in enumerate(state))
            for f in range(3):
                vx[j + 1, f] = state[f][halo : halo + OWN]

            if send:
                give_back(j + 1)
            return state

        return lax.fori_loop(lo, hi, body, state)

    def give_back(j):
        @pl.when((chip != j) | (half != k))
        def _():
            ret_copy(j).start()

    def ret_copy(j):
        return copy(vx.at[j], vt.at[:, rows(OWN * spot, OWN), :], ret_s.at[j], ret_r.at[spot], at(j * 2 + half, s))

    state = scanned(0, MIDDLE, HALO, (jnp.zeros((WIDE, 128), F32),) * 3, False)
    for n in range(2):
        middle_copy(n).start()

    @pl.loop(0, MIDDLE)
    def _(i):
        give_back(1 + lax.rem(chip + i, MIDDLE))

    for n in range(2):
        middle_copy(n).wait_recv()
    state = tuple(jnp.concatenate([middle[0, f], x[HALO : HALO + OWN], middle[1, f]], axis=0) for f, x in enumerate(state))
    state = scanned(MIDDLE, 11, HALO, state, True)
    scanned(11, CHIPS - 1, 8, tuple(x[8:40] for x in state), True)

    @pl.when(chip > 0)
    def _():
        @pl.when(half == k)
        def _():
            vt[:, rows(OWN * spot, OWN), :] = vx[chip]

        @pl.loop(0, 16)
        def _(n):
            t = owner(s, 16 * k + n)

            @pl.when(t != tm)
            def _():
                copy(vx.at[0], vt.at[:, rows(OWN * n, OWN), :], ret_s.at[0], ret_r.at[n], at(t, s)).wait_recv()

    tile_row = lax.broadcasted_iota(jnp.int32, (8, 128), 0)
    turned_back = [[vt[f, 128 * t : 128 * t + 128, :].T for t in range(2)] for f in range(3)]

    def around(x, sp):
        a, b = (16 * sp + 16) % 128, (16 * sp + 120) % 128
        return jnp.where(tile_row < 2, x[a : a + 8], pltpu.roll(x[b : b + 8], 4, 0))

    def stack(x, y):
        return jnp.where(tile_row < 4, x, pltpu.roll(y, 4, 0))

    for sp in range(SPACE):
        for t in range(2):
            cols = slice(128 * t, 128 * t + 128)
            for f in range(3):
                vr[sp, 16 * f : 16 * f + 16, cols] = turned_back[f][t][16 * sp : 16 * sp + 16]
            vr[sp, 48:, cols] = stack(around(turned_back[0][t], sp), around(turned_back[1][t], sp))
        vb[sp] = stack(around(turned_back[2][0], sp), around(turned_back[2][1], sp))

    def side(sp, kk):
        return pl.ds(pl.multiple_of(256 * sp + 128 * kk, 128), 128)

    def row_copies(sp, send):
        to, by = (sp, s) if send else (s, sp)
        return (
            copy(vr.at[to], vout.at[:, block(by, k)], row_s.at[0, sp], row_r.at[0, by], at(tm, sp)),
            copy(vb.at[to], vob.at[:, side(by, k)], row_s.at[1, sp], row_r.at[1, by], at(tm, sp)),
        )

    def fin_copies(sp, send):
        kk = k if send else 1 - k
        cols, beside = block(sp, kk), side(sp, kk)
        return (
            copy(vout.at[:, cols], vout.at[:, cols], fin_s.at[0, sp], fin_r.at[0, sp], partner),
            copy(vob.at[:, beside], vob.at[:, beside], fin_s.at[1, sp], fin_r.at[1, sp], partner),
        )

    for d in range(1, SPACE):
        for c in row_copies(lax.rem(s + d, SPACE), True):
            c.start()
    vout[:, block(s, k)] = vr[s]
    vob[:, side(s, k)] = vb[s]
    for c in fin_copies(s, True):
        c.start()
    give.wait_recv()

    @pl.when(tm < 31)
    def _():
        for n in range(8):
            start_copy(n, tm_next).wait_send()

    for ns, buffer, back, spot_of in routes:
        @pl.when((z_place == spot_of) & (tm < 24))
        def _(ns=ns, buffer=buffer, back=back):
            for n in ns:
                pass_copy(n, buffer, ns[0], back + 1).wait_send()

    for n in range(4):
        for j in range(PAIRS):
            pack_copy(n, j, True).wait_send()
    for n in range(2):
        for j in range(PAIRS):
            q2_copy(n, j, True).wait_send()
            q3_copy(n, j, True).wait_send()

    @pl.when(k == 0)
    def _():
        for n in range(2, 4):
            for j in range(PAIRS):
                q3_copy(n, j, True).wait_send()

    give.wait_send()
    for i in range(COLS // CHUNK):
        item_copy(i).wait_send()
    for d in range(1, SPACE):
        for n in range(3):
            depth_copy(d, n, True).wait_send()
        for f in range(3):
            one_copy(f, lax.rem(s + d, SPACE), True).wait_send()

    @pl.loop(0, 16)
    def _(n):
        @pl.when((owner(s, 16 * k + n) != tm) & (chip < CHIPS - 1))
        def _():
            for f in range(3):
                two_copy(f, n).wait_send()

        each_halo(n, lambda x: x.wait_send())

    for n in range(2):
        middle_copy(n).wait_send()


    def spread(sp):
        cols = pl.ds(pl.multiple_of(sp * CHUNK, CHUNK), CHUNK)
        row = lax.broadcasted_iota(jnp.int32, (8, CHUNK), 0)
        x = vout[48:, cols]
        y = pltpu.roll(x, 4, 0)
        vh[0, :, cols] = jnp.where(row < 4, x, y)
        vh[1, :, cols] = jnp.where(row < 4, y, x)
        for kk in range(2):
            x = vob[:, side(sp, kk)]
            y = pltpu.roll(x, 4, 0)
            for t, z in enumerate((jnp.where(tile_row < 4, x, y), jnp.where(tile_row < 4, y, x))):
                vh[2, :, pl.ds(pl.multiple_of(512 * sp + 256 * kk + 128 * t, 128), 128)] = z

    def finish(sp):
        base = pl.multiple_of(sp * CHUNK, CHUNK)
        cols = pl.ds(base, CHUNK)
        d = wide(lambda c: drow[:, c], base)

        def stepped(state):
            h, u, w = state
            r = rates(h, u, w, d * u, d * w, left, right, up, down, lambda x: x)
            return [x + step_size * y for x, y in zip(state, r)]

        state = [
            wide(lambda c, f=f: jnp.concatenate([vout[16 * f : 16 * f + 16, c], vh[f, :, c]], axis=0), base) for f in range(3)
        ]
        a = stepped(state)
        b = stepped(a)
        for f in range(3):
            begin = inner(state[f])[:ROWS]
            ours = jnp.where(k == 0, boosted[f, :, cols], other[f, :, cols])
            y1 = ours + inner(a[f])[:ROWS]
            y2 = esum[f, :, cols] + inner(b[f])[:ROWS]
            start = jnp.where(k == 0, jnp.where(tm == 0, init[f, :, cols], begin), y1)
            end = jnp.where(k == 0, y1, y2)
            out[0, f, :, cols] = start
            out[1, f, :, cols] = partial[f, :, cols] + 0.5 * (start + end)
            out[2, f, :, cols] = end

    @pl.loop(1, SPACE)
    def _(d):
        sp = lax.rem(s + SPACE - d, SPACE)
        for c in row_copies(sp, False):
            c.wait_recv()
        for c in fin_copies(sp, True):
            c.start()
        for c in fin_copies(lax.rem(sp + 1, SPACE), False):
            c.wait_recv()
        spread(lax.rem(sp + 1, SPACE))

        @pl.when(d >= 3)
        def _():
            finish(lax.rem(sp + 2, SPACE))

    for c in fin_copies(lax.rem(s + 1, SPACE), False):
        c.wait_recv()
    spread(lax.rem(s + 1, SPACE))

    @pl.loop(0, 3)
    def _(i):
        finish(lax.rem(s + 2 * SPACE - 6 - i, SPACE))

    for d in range(1, SPACE):
        for c in row_copies(lax.rem(s + d, SPACE), True):
            c.wait_send()
    for sp in range(SPACE):
        for c in fin_copies(sp, True):
            c.wait_send()

    @pl.loop(1, 16)
    def _(n):
        @pl.when((chip != n) | (half != k))
        def _():
            ret_copy(n).wait_send()


VM = pl.BlockSpec(memory_space=pltpu.VMEM)


def per_device(fine_nodes, init_state, mean_depth):
    points = fine_nodes[0].reshape(9, ROWS, COLS)

    def vm(*shape):
        return pltpu.VMEM(shape, F32)

    def sems(*shape):
        return [pltpu.SemaphoreType.DMA(shape)] * 2

    flat, ringed = vm(3, ROWS, COLS), vm(3, RING, COLS)
    out = pl.pallas_call(
        coarse_kernel,
        out_shape=jax.ShapeDtypeStruct((3, 3, ROWS, COLS), F32),
        in_specs=[pl.BlockSpec(memory_space=pltpu.HBM)] * 3,
        out_specs=VM,
        scratch_shapes=[
            flat, flat, flat, flat, vm(56, COLS), vm(8, FOLD), vm(3, 8, COLS), vm(RING, COLS), vm(9, ROWS, COLS), flat, vm(ROWS, COLS),
            flat, flat, flat, vm(2, 8, FOLD), vm(2, 8, FOLD), vm(2, 8, FOLD), vm(2, 8, FOLD),
            ringed, ringed, flat, ringed, vm(2, 8, FOLD), vm(2, 8, FOLD), ringed, vm(4, 8, FOLD), vm(4, 8, FOLD),
            ringed, flat, flat, vm(2, 3, ROWS, COLS // 8), vm(2, 3, ROWS, COLS // 8), vm(2, 3, ROWS, COLS // 8),
            vm(3, 128, PART), vm(3, PART, 128), vm(128, 512), vm(512, 128),
            vm(CHIPS, 3, WIDE, 128), vm(CHIPS, 3, OWN, 128), vm(2, 3, OWN, 128), vm(3, PART, 128), vm(SPACE, 56, PART), vm(SPACE, 8, 128),
            pltpu.SemaphoreType.DMA((5,)), *sems(8), *sems(8), *sems(4, 4), *sems(2, 4), *sems(4, 4), *sems(8), *sems(1), *sems(3, 8), *sems(3, 8), *sems(3, 16),
            *sems(2, 16), *sems(16), *sems(2, 8), *sems(2, 8),
        ],
        compiler_params=pltpu.CompilerParams(collective_id=0, has_side_effects=True, vmem_limit_bytes=40 << 20),
        name="sweep",
    )(*(pltpu.with_memory_space_constraint(x, pltpu.HBM) for x in (points, init_state, mean_depth)))
    return out[None]


def solution(mesh):
    placed = (P("tm", None, None, "space", None), P(None, "space", None), P("space", None))
    return jax.shard_map(
        per_device,
        mesh=mesh,
        in_specs=placed,
        out_specs=P("tm", None, None, "space", None),
        check_vma=False,
    )
```

```python
import functools

import jax
import jax.numpy as jnp
from jax import lax
from jax.experimental import pallas as pl
from jax.experimental.pallas import tpu as pltpu
from jax.sharding import PartitionSpec as P

MESH = pl.DeviceIdType.MESH
F32 = jnp.float32

step_size = 0.3
viscosity = 1.0 / 3.0
coriolis = 0.5
quad_near = 5.0 / 24.0
quad_mid = 1.0 / 3.0
quad_far = -1.0 / 24.0
half_step = 0.5 * step_size
start_share = -(half_step + step_size / 3.0)
one_share = 2.0 * step_size / 3.0
two_share = half_step - step_size / 3.0

ROWS = 16
COLS = 4096
SPACE = 8
CHIPS = 16
PART = 256
OWN = 16
HALO = 16
MIDDLE = 7
WIDE = OWN + 2 * HALO


def rates(h, u, v, de, dn, left, right, up, down, centre):
    nh, nu, nv = viscosity * h, viscosity * u, viscosity * v
    he, hn, hh = 0.5 * de, 0.5 * dn, 0.5 * h
    nhc, nuc, nvc = centre(nh), centre(nu), centre(nv)
    hr = right(nh - he) + left(nh + he) + down(centre(nh - hn)) + up(centre(nh + hn)) - 4.0 * nhc
    ur = right(nu - hh) + left(nu + hh) + down(nuc) + up(nuc) - 4.0 * nuc + coriolis * centre(v)
    vr = right(nv) + left(nv) + down(centre(nv - hh)) + up(centre(nv + hh)) - 4.0 * nvc - coriolis * centre(u)
    return hr, ur, vr


CHUNK = 512
RING = 24


def edges(base):
    if isinstance(base, int):
        lo, hi = (base - 128) % COLS, (base + CHUNK) % COLS
    else:
        lo = pl.multiple_of(lax.rem(base + COLS - 128, COLS), 128)
        hi = pl.multiple_of(lax.rem(base + CHUNK, COLS), 128)
    return pl.ds(lo, 128), pl.ds(base, CHUNK), pl.ds(hi, 128)


def wide(get, base):
    return jnp.concatenate([get(c) for c in edges(base)], axis=1)


def right(x):
    return pltpu.roll(x, x.shape[1] - 1, 1)


def left(x):
    return pltpu.roll(x, 1, 1)


def down(x):
    return pltpu.roll(x, RING - 1, 0)


def up(x):
    return pltpu.roll(x, 1, 0)


def inner(x):
    return x[:, 128 : 128 + CHUNK]


def ring_rates(q, depth, base):
    h, u, v = (wide(lambda c, f=f: q[f, :, c], base) for f in range(3))
    d = wide(lambda c: depth[:, c], base)
    return rates(h, u, v, d * u, d * v, lambda x: inner(left(x)), lambda x: inner(right(x)), up, down, inner)


def chunks(body):
    @pl.loop(0, COLS // CHUNK)
    def _(i):
        body(pl.multiple_of(i * CHUNK, CHUNK))


PAIRS = COLS // CHUNK // 2
FOLD = COLS // 2


def pairs(body):
    @pl.loop(0, PAIRS)
    def _(j):
        base = pl.multiple_of(j * CHUNK, CHUNK)
        body(j, pl.ds(base, CHUNK), [base, pl.multiple_of(base + FOLD, CHUNK)])


def pair(body, j):
    base = j * CHUNK
    body(j, pl.ds(base, CHUNK), [base, base + FOLD])


def sub_roll(x, by):
    by %= 8
    return x if by == 0 else pltpu.roll(x, by, 0)


def pack(parts, at):
    row = lax.broadcasted_iota(jnp.int32, parts[0].shape, 0)
    tile = sub_roll(parts[0], -at)
    for i in range(1, len(parts)):
        tile = jnp.where(row >= 2 * i, sub_roll(parts[i], 2 * i - at), tile)
    return tile


def place(parts, at):
    row = lax.broadcasted_iota(jnp.int32, parts[0].shape, 0)
    tile = sub_roll(parts[0], -at[0])
    for i in range(1, len(parts)):
        tile = jnp.where(row >= i, sub_roll(parts[i], i - at[i]), tile)
    return tile


def fold(first, second):
    row = lax.broadcasted_iota(jnp.int32, first.shape, 0)
    return jnp.where(row < 4, first, sub_roll(second, 4))


def unfold(after, before, i):
    row = lax.broadcasted_iota(jnp.int32, after.shape, 0)
    return jnp.where(row < 4, sub_roll(after, -i), sub_roll(before, 7 - i))


def unpack(after, before, i):
    row = lax.broadcasted_iota(jnp.int32, after.shape, 0)
    return jnp.where(row < 4, sub_roll(after, -2 * i), sub_roll(before, 6 - 2 * i))


def snake(n):
    z, x = n // 4, lax.rem(n, 4)
    return z * 4 + jnp.where(lax.rem(z, 2) == 0, x, 3 - x)


def turned(s, chip):
    return chip // 4 * 4 + lax.rem(chip + 2 * lax.rem(s, 2), 4)


def owner(s, i):
    o = jnp.where(lax.rem(s, 2) == 0, i, 31 - i)
    return turned(s, snake(o // 2)) * 2 + lax.rem(o, 2)


def owned(s, tm):
    o = snake(turned(s, tm // 2)) * 2 + lax.rem(tm, 2)
    return jnp.where(lax.rem(s, 2) == 0, o, 31 - o)


def coarse_kernel(
    points_hbm, init_hbm, depth_hbm,
    out,
    boosted, other, esum, partial, vout, vob, vh, drow, points, init, depth, s0, a1, a2, ps, pr, fs, fr, s0r, q1, s1, q2, q2s, q2r, q3, q3s, q3r, br, item, ritem, relay_a, relay_b, relay_c,
    rt, et, dr, dt, ex, vx, middle, vt, vr, vb,
    in_sem, st_s, st_r, rl_s, rl_r, pk_s, pk_r, q2_ss, q2_rs, q3_ss, q3_rs, it_s, it_r, oth_s, oth_r, one_s, one_r, dep_s, dep_r, two_s, two_r,
    halo_s, halo_r, ret_s, ret_r, row_s, row_r, fin_s, fin_r,
):
    tm = lax.axis_index("tm")
    s = lax.axis_index("space")
    chip, k = tm // 2, lax.rem(tm, 2)
    mine = owned(s, tm)
    half, spot = mine // 16, lax.rem(mine, 16)
    s_next, s_prev = lax.rem(s + 1, SPACE), lax.rem(s + SPACE - 1, SPACE)
    tm_next, tm_prev = lax.rem(tm + 1, 32), lax.rem(tm + 31, 32)
    first = jnp.where(tm == 0, 1.0, 0.0).astype(F32)

    def at(t, sp):
        return {"tm": t, "space": sp}

    def near(step):
        p = lax.rem(32 * s + mine + step + 256, 256)
        return at(owner(p // 32, lax.rem(p, 32)), p // 32)

    partner = at(chip * 2 + 1 - k, s)
    nears = [near(1), near(-1)]

    loads = [pltpu.make_async_copy(points_hbm.at[3 * m : 3 * m + 3], points.at[3 * m : 3 * m + 3], in_sem.at[m]) for m in range(3)]
    loads += [pltpu.make_async_copy(init_hbm, init, in_sem.at[3]), pltpu.make_async_copy(depth_hbm, depth, in_sem.at[4])]
    for n in (2, 0, 1, 4, 3):
        loads[n].start()
    vt[...] = jnp.zeros_like(vt)
    barrier = pltpu.get_barrier_semaphore()
    z, x = tm // 8, lax.rem(tm // 2, 4)
    peers = [
        at(lax.rem(z + dz, 4) * 8 + lax.rem(x + dx, 4) * 2 + c, s)
        for dz in (2, 1, 3, 0) for dx in (2, 1, 3, 0) for c in range(2) if dz or dx
    ] + [partner]
    peers += [at(tm, lax.rem(s + d, SPACE)) for d in range(1, SPACE)]
    peers += [at(t, sp) for t in (tm_next, tm_prev) for sp in (s_next, s_prev)]
    peers += nears
    for p in peers:
        pl.semaphore_signal(barrier, inc=1, device_id=p, device_id_type=MESH)
    pl.semaphore_wait(barrier, len(peers))

    def copy(src, dst, ss, rs, dev):
        return pltpu.make_async_remote_copy(src_ref=src, dst_ref=dst, send_sem=ss, recv_sem=rs, device_id=dev, device_id_type=MESH)

    def block(sp, kk):
        return pl.ds(pl.multiple_of(512 * sp + 256 * kk, PART), PART)

    def rows(start, n=ROWS):
        return pl.ds(pl.multiple_of(start, 8), n)

    loads[2].wait()

    z_place = lax.rem(tm, 8)
    far_end = (z_place == 7) & (tm < 31)
    PIECE = COLS // 8
    direct = range(0, 2)
    routes = ((range(2, 4), relay_a, 6, 1), (range(4, 6), relay_b, 2, 5), (range(6, 8), relay_c, 4, 3))

    def piece(n):
        return pl.ds(PIECE * n, PIECE)

    def start_copy(n, to):
        return copy(points.at[6:9, :, piece(n)], s0.at[:, :, piece(n)], st_s.at[n], st_r.at[n], at(to, s))

    def via_copy(n, buffer, first_piece, to):
        return copy(points.at[6:9, :, piece(n)], buffer.at[n - first_piece], st_s.at[n], rl_r.at[n], at(to, s))

    def pass_copy(n, buffer, first_piece, ahead):
        return copy(buffer.at[n - first_piece], s0.at[:, :, piece(n)], rl_s.at[n], st_r.at[n], at(lax.rem(tm + ahead, 32), s))

    @pl.when((tm < 31) & (z_place != 7))
    def _():
        for n in (0, 4, 1, 5, 2, 6, 3, 7):
            start_copy(n, tm_next).start()

    @pl.when(far_end)
    def _():
        for ns, buffer, back, _ in routes:
            for n in ns:
                via_copy(n, buffer, ns[0], lax.rem(tm + 32 - back, 32)).start()

    for n in (0, 1, 4, 3):
        loads[n].wait()

    def pack_copy(n, j, send):
        up_down = lax.rem(s + (1 if (n % 2 == 0) == send else SPACE - 1), SPACE)
        slot = tm if n < 2 else (tm_next if send else tm_prev)
        cols = pl.ds(j * CHUNK, CHUNK) if isinstance(j, int) else pl.ds(pl.multiple_of(j * CHUNK, CHUNK), CHUNK)
        src, dst = (ps, pr) if n < 2 else (fs, fr)
        return copy(src.at[n % 2, :, cols], dst.at[n % 2, :, cols], pk_s.at[n, j], pk_r.at[n, j], at(slot, up_down))

    def prepare(j, folded, bases):
        tiles = [[], []], [[], []]
        for base in bases:
            cols = pl.ds(base, CHUNK)
            top, bottom = [], []
            for f in range(3):
                p0, p1, p2 = (points[3 * m + f, :, cols] for m in range(3))
                x = (step_size * quad_near - half_step) * p0 + (step_size * quad_mid) * p1 + (step_size * quad_far) * p2
                y = (step_size * quad_far) * p0 + (step_size * quad_mid - half_step) * p1 + (step_size * quad_near) * p2
                a1[f, :, cols] = x
                a2[f, :, cols] = y
                top.append(x[:8])
                bottom.append(x[8:])
            for n, (parts, tile, row, inside) in enumerate(((bottom, 8, 7, 6), (top, 0, 0, 1))):
                d = depth[tile : tile + 8, cols]
                ends = [
                    jnp.where(tm == 31, init[f, tile : tile + 8, cols], points[6 + f, tile : tile + 8, cols]) for f in range(3)
                ]
                tiles[0][n].append(place(parts + [d], [row] * 4))
                tiles[1][n].append(place(ends + [d], [row] * 3 + [inside]))
        for n in range(2):
            ps[n, :, folded] = fold(*tiles[0][n])
            fs[n, :, folded] = fold(*tiles[1][n])
        for n in range(2, 4):
            pack_copy(n, j, True).start()

    pairs(prepare)

    @pl.when(far_end)
    def _():
        for n in direct:
            start_copy(n, tm_next).start()

    for n in range(2):
        for j in range(PAIRS):
            pack_copy(n, j, True).start()

    for ns, buffer, back, spot_of in routes:
        @pl.when((z_place == spot_of) & (tm < 24))
        def _(ns=ns, buffer=buffer, back=back):
            for n in ns:
                via_copy(n, buffer, ns[0], lax.rem(tm + back, 32)).wait_recv()
                pass_copy(n, buffer, ns[0], back + 1).start()

    for n in range(4):
        for j in range(PAIRS):
            pack_copy(n, j, False).wait_recv()

    def ringed(j, folded, bases):
        row = lax.broadcasted_iota(jnp.int32, (8, CHUNK), 0)
        for h, base in enumerate(bases):
            cols = pl.ds(base, CHUNK)
            pa, pb, fa, fb = pr[1, :, folded], pr[0, :, folded], fr[1, :, folded], fr[0, :, folded]
            i = 4 * h + 3
            d = jnp.where(row < 4, sub_roll(fa, 1 - i), sub_roll(fb, 6 - i))
            d = jnp.where((row == 0) | (row == 7), unfold(pa, pb, i), d)
            drow[:, cols] = jnp.concatenate([depth[:, cols], d], axis=0)
            for f in range(3):
                main = jnp.where(tm == 0, init[f, :, cols], s0[f, :, cols])
                x = jnp.concatenate([main, unfold(fa, fb, 4 * h + f)], axis=0)
                y = jnp.concatenate([a1[f, :, cols], unfold(pa, pb, 4 * h + f)], axis=0)
                s0r[f, :, cols] = x
                q1[f, :, cols] = half_step * x + y

    def q2_copy(n, j, send):
        up_down = lax.rem(s + (1 if (n == 0) == send else SPACE - 1), SPACE)
        cols = pl.ds(j * CHUNK, CHUNK) if isinstance(j, int) else pl.ds(pl.multiple_of(j * CHUNK, CHUNK), CHUNK)
        return copy(q2s.at[n, :, cols], q2r.at[n, :, cols], q2_ss.at[n, j], q2_rs.at[n, j], at(tm, up_down))

    def one(j, folded, bases):
        tiles = [[], []]
        for base in bases:
            cols = pl.ds(base, CHUNK)
            r = ring_rates(q1, drow, base)
            q = []
            for f in range(3):
                x = s0r[f, :ROWS, cols] + r[f][:ROWS]
                s1[f, :, cols] = x
                q.append(half_step * x + a2[f, :, cols])
                q2[f, :ROWS, cols] = q[f]
            tiles[0].append(place([x[8:] for x in q], [7] * 3))
            tiles[1].append(place([x[:8] for x in q], [0] * 3))
        for n in range(2):
            q2s[n, :, folded] = fold(*tiles[n])
            q2_copy(n, j, True).start()

    for j in range(PAIRS):
        @pl.when(tm > 0)
        def _(j=j):
            start_copy(j, tm_prev).wait_recv()
            start_copy(j + PAIRS, tm_prev).wait_recv()

        pair(ringed, j)
        if j >= 2:
            pair(one, j - 1)
    pair(one, 3)
    pair(one, 0)

    def q3_copy(n, j, send):
        up_down = lax.rem(s + (1 if (n % 2 == 0) == send else SPACE - 1), SPACE)
        cols = pl.ds(j * CHUNK, CHUNK) if isinstance(j, int) else pl.ds(pl.multiple_of(j * CHUNK, CHUNK), CHUNK)
        return copy(q3s.at[n, :, cols], q3r.at[n, :, cols], q3_ss.at[n, j], q3_rs.at[n, j], at(tm, up_down))

    def two(j, folded, bases):
        for n in range(2):
            q2_copy(n, j, False).wait_recv()
        tiles = [[], [], [], []]
        for h, base in enumerate(bases):
            cols = pl.ds(base, CHUNK)
            for f in range(3):
                q2[f, ROWS:, cols] = unfold(q2r[1, :, folded], q2r[0, :, folded], 4 * h + f)
            r = ring_rates(q2, drow, base)
            top, bottom = [], []
            for f in range(3):
                x, y = s0r[f, :ROWS, cols], s1[f, :, cols]
                z = y + r[f][:ROWS]
                partial[f, :, cols] = y - 0.5 * (x + z)
                q = (step_size * first + start_share) * x + one_share * y + two_share * z
                q3[f, :ROWS, cols] = q
                top.append(q[:8])
                bottom.append(q[8:])
            for n, (parts, row) in enumerate(((bottom, 7), (top, 0), (bottom, 6), (top, 1))):
                tiles[n].append(place(parts, [row] * 3))
        for n in range(4):
            q3s[n, :, folded] = fold(*tiles[n])
        for n in range(2):
            q3_copy(n, j, True).start()

        @pl.when(k == 0)
        def _():
            for n in range(2, 4):
                q3_copy(n, j, True).start()

    for j in (1, 2, 3, 0):
        pair(two, j)

    def q3_rows(j, folded, bases):
        for n in range(2):
            q3_copy(n, j, False).wait_recv()

        @pl.when(k == 0)
        def _():
            for n in range(2, 4):
                q3_copy(n, j, False).wait_recv()

        row = lax.broadcasted_iota(jnp.int32, (8, CHUNK), 0)
        for h, base in enumerate(bases):
            for f in range(3):
                i = 4 * h + f
                near_rows = unfold(q3r[1, :, folded], q3r[0, :, folded], i)
                far_rows = jnp.where(row < 4, sub_roll(q3r[3, :, folded], 1 - i), sub_roll(q3r[2, :, folded], 6 - i))
                q3[f, ROWS:, pl.ds(base, CHUNK)] = jnp.where((row == 0) | (row == 7), near_rows, far_rows)

    def three(j, folded, bases):
        for base in bases:
            cols = pl.ds(base, CHUNK)
            r = ring_rates(q3, drow, base)
            for f in range(3):
                x = r[f] + first * s0r[f, :, cols]
                br[f, :, cols] = x
                boosted[f, :, cols] = x[:ROWS]

    pair(q3_rows, 1)
    pair(q3_rows, 2)
    pair(q3_rows, 3)
    pair(three, 2)
    pair(q3_rows, 0)
    for j in (3, 0, 1):
        pair(three, j)
    give = copy(boosted, other, oth_s.at[0], oth_r.at[0], partner)

    def item_copy(i):
        cols = pl.ds(pl.multiple_of(i * CHUNK, CHUNK), CHUNK)
        return copy(item.at[:, :, cols], ritem.at[:, :, cols], it_s.at[i], it_r.at[i], partner)

    @pl.loop(0, COLS // CHUNK)
    def _(i):
        base = pl.multiple_of(i * CHUNK, CHUNK)
        cols = pl.ds(base, CHUNK)
        r = ring_rates(br, drow, base)
        for f in range(3):
            item[f, :, cols] = jnp.where(k == 0, boosted[f, :, cols] + step_size * r[f][:ROWS], boosted[f, :, cols])
        item_copy(i).start()

    give.start()

    def one_copy(f, sp, send):
        to, by = (sp, s) if send else (s, sp)
        n = to if send else by
        return copy(esum.at[f, :, block(to, k)], rt.at[f, rows(ROWS * by), :], one_s.at[f, n], one_r.at[f, by], at(tm, sp))

    @pl.loop(0, COLS // CHUNK)
    def _(i):
        item_copy(i).wait_recv()
        cols = pl.ds(pl.multiple_of(i * CHUNK, CHUNK), CHUNK)
        for f in range(3):
            esum[f, :, cols] = item[f, :, cols] + ritem[f, :, cols]

    for f in range(3):
        for d in range(1, SPACE):
            one_copy(f, lax.rem(s + d, SPACE), True).start()
    rt[:, rows(ROWS * s), :] = esum[:, :, block(s, k)]

    def depth_pieces(base):
        return (
            (pl.ds(pl.multiple_of(base, 128), PART), pl.ds(128, PART)),
            (pl.ds(pl.multiple_of(lax.rem(base + COLS - 128, COLS), 128), 128), pl.ds(0, 128)),
            (pl.ds(pl.multiple_of(lax.rem(base + PART, COLS), 128), 128), pl.ds(384, 128)),
        )

    def depth_copy(d, n, send):
        sp = lax.rem(s + d, SPACE) if send else lax.rem(s + SPACE - d, SPACE)
        to = sp if send else s
        src, dst = depth_pieces(512 * to + 256 * (owned(to, tm) // 16))[n]
        return copy(depth.at[:, src], dr.at[rows(ROWS * (s if send else sp)), dst], dep_s.at[n, d], dep_r.at[n, d], at(tm, sp))

    for d in range(1, SPACE):
        for n in range(3):
            depth_copy(d, n, True).start()
    for src, dst in depth_pieces(512 * s + 256 * half):
        dr[rows(ROWS * s), dst] = depth[:, src]


    def two_copy(f, n):
        src, dst = et.at[f, rows(OWN * n, OWN), :], ex.at[chip, f, pl.ds(HALO, OWN), :]
        return copy(src, dst, two_s.at[f, n], two_r.at[f, chip], at(owner(s, 16 * k + n), s))

    for f in range(3):
        for d in range(1, SPACE):
            one_copy(f, lax.rem(s + SPACE - d, SPACE), False).wait_recv()
        for t in range(2):
            et[f, 128 * t : 128 * t + 128, :] = rt[f, :, 128 * t : 128 * t + 128].T

        @pl.loop(0, 16)
        def _(m, f=f):
            n = lax.rem(m + spot, 16)

            @pl.when((owner(s, 16 * k + n) != tm) & (chip < CHIPS - 1))
            def _():
                two_copy(f, n).start()

    @pl.when(half == k)
    def _():
        ex[chip, :, HALO : HALO + OWN, :] = et[:, rows(OWN * spot, OWN), :]

    spans = ((0, 2, 16), (2, 6, 8), (7, 10, 16), (10, 14, 8))

    def halo_copy(n, j, width):
        src, dst = (HALO + OWN - width, HALO - width) if n == 0 else (HALO, HALO + OWN)
        return copy(ex.at[j, :, pl.ds(src, width), :], ex.at[j, :, pl.ds(dst, width), :], halo_s.at[n, j], halo_r.at[n, j], nears[n])

    def middle_copy(n):
        return copy(vx.at[MIDDLE], middle.at[n], halo_s.at[n, 15], halo_r.at[n, 15], nears[n])

    def each_halo(j, act):
        for lo, hi, width in spans:
            @pl.when((j >= lo) & (j < hi))
            def _():
                for n in range(2):
                    act(halo_copy(n, j, width))

    for c in (0, 1, 2, 3, 5, 6, 4, 7, 9, 10, 11, 8, 13, 14, 12):
        @pl.when((chip != c) | (half != k))
        def _(c=c):
            for f in range(3):
                src, dst = et.at[f, rows(OWN * spot, OWN), :], ex.at[c, f, pl.ds(HALO, OWN), :]
                copy(src, dst, two_s.at[f, 0], two_r.at[f, c], at(c * 2 + half, s)).wait_recv()

        for lo, hi, width in spans:
            if lo <= c < hi:
                for n in range(2):
                    halo_copy(n, c, width).start()

    for d in range(1, SPACE):
        for n in range(3):
            depth_copy(d, n, False).wait_recv()
    for t in range(4):
        dt[128 * t : 128 * t + 128, :] = dr[:, 128 * t : 128 * t + 128].T


    def scanned(lo, hi, halo, state, send):
        count = OWN + 2 * halo
        d_own = dt[rows(128 - halo + OWN * spot, count), :]

        def stepped(state):
            h, u, v = state
            r = rates(
                h, u, v, d_own * u, d_own * v,
                lambda x: pltpu.roll(x, 1, 0), lambda x: pltpu.roll(x, count - 1, 0),
                lambda x: pltpu.roll(x, 1, 1), lambda x: pltpu.roll(x, 127, 1), lambda x: x,
            )
            return tuple(x + step_size * y for x, y in zip(state, r))

        def body(j, state):
            state = stepped(stepped(state))
            each_halo(j, lambda x: x.wait_recv())
            state = tuple(x + ex[j, f, HALO - halo : HALO + OWN + halo] for f, x in enumerate(state))
            for f in range(3):
                vx[j + 1, f] = state[f][halo : halo + OWN]

            if send:
                give_back(j + 1)
            return state

        return lax.fori_loop(lo, hi, body, state)

    def give_back(j):
        @pl.when((chip != j) | (half != k))
        def _():
            ret_copy(j).start()

    def ret_copy(j):
        return copy(vx.at[j], vt.at[:, rows(OWN * spot, OWN), :], ret_s.at[j], ret_r.at[spot], at(j * 2 + half, s))

    state = scanned(0, MIDDLE, HALO, (jnp.zeros((WIDE, 128), F32),) * 3, False)
    for n in range(2):
        middle_copy(n).start()

    @pl.loop(0, MIDDLE)
    def _(i):
        give_back(1 + lax.rem(chip + i, MIDDLE))

    for n in range(2):
        middle_copy(n).wait_recv()
    state = tuple(jnp.concatenate([middle[0, f], x[HALO : HALO + OWN], middle[1, f]], axis=0) for f, x in enumerate(state))
    state = scanned(MIDDLE, 11, HALO, state, True)
    scanned(11, CHIPS - 1, 8, tuple(x[8:40] for x in state), True)

    @pl.when((chip > 0) & (half == k))
    def _():
        vt[:, rows(OWN * spot, OWN), :] = vx[chip]

    tile_row = lax.broadcasted_iota(jnp.int32, (8, 128), 0)
    def around(x, sp):
        a, b = (16 * sp + 16) % 128, (16 * sp + 120) % 128
        return jnp.where(tile_row < 2, x[a : a + 8], pltpu.roll(x[b : b + 8], 4, 0))

    def stack(x, y):
        return jnp.where(tile_row < 4, x, pltpu.roll(y, 4, 0))

    def half_block(sp, t):
        return pl.ds(pl.multiple_of(512 * sp + 256 * k + 128 * t, 128), 128)

    def side(sp, kk):
        return pl.ds(pl.multiple_of(256 * sp + 128 * kk, 128), 128)

    def row_copies(sp, send):
        to, by = (sp, s) if send else (s, sp)
        return (
            *(copy(vr.at[t, to], vout.at[:, half_block(by, t)], row_s.at[t, sp], row_r.at[t, by], at(tm, sp)) for t in range(2)),
            copy(vb.at[to], vob.at[:, side(by, k)], row_s.at[2, sp], row_r.at[2, by], at(tm, sp)),
        )

    def fin_copies(sp, send):
        kk = k if send else 1 - k
        cols, beside = block(sp, kk), side(sp, kk)
        return (
            copy(vout.at[:, cols], vout.at[:, cols], fin_s.at[0, sp], fin_r.at[0, sp], partner),
            copy(vob.at[:, beside], vob.at[:, beside], fin_s.at[1, sp], fin_r.at[1, sp], partner),
        )

    for t in range(2):
        @pl.when(chip > 0)
        def _(t=t):
            @pl.loop(8 * t, 8 * t + 8)
            def _(n):
                frm = owner(s, 16 * k + n)

                @pl.when(frm != tm)
                def _():
                    copy(vx.at[0], vt.at[:, rows(OWN * n, OWN), :], ret_s.at[0], ret_r.at[n], at(frm, s)).wait_recv()

        xs = [vt[f, 128 * t : 128 * t + 128, :].T for f in range(3)]
        for sp in range(SPACE):
            for f in range(3):
                vr[t, sp, 16 * f : 16 * f + 16, :] = xs[f][16 * sp : 16 * sp + 16]
            vr[t, sp, 48:, :] = stack(around(xs[0], sp), around(xs[1], sp))
        if t == 1:
            other_half = vt[2, :128, :].T
            for sp in range(SPACE):
                vb[sp] = stack(around(other_half, sp), around(xs[2], sp))
        for d in range(1, SPACE):
            for c in row_copies(lax.rem(s + d, SPACE), True)[t : 1 if t == 0 else 3]:
                c.start()
        vout[:, half_block(s, t)] = vr[t, s]
    vob[:, side(s, k)] = vb[s]
    for c in fin_copies(s, True):
        c.start()
    give.wait_recv()

    @pl.when(tm < 31)
    def _():
        for n in range(8):
            start_copy(n, tm_next).wait_send()

    for ns, buffer, back, spot_of in routes:
        @pl.when((z_place == spot_of) & (tm < 24))
        def _(ns=ns, buffer=buffer, back=back):
            for n in ns:
                pass_copy(n, buffer, ns[0], back + 1).wait_send()

    for n in range(4):
        for j in range(PAIRS):
            pack_copy(n, j, True).wait_send()
    for n in range(2):
        for j in range(PAIRS):
            q2_copy(n, j, True).wait_send()
            q3_copy(n, j, True).wait_send()

    @pl.when(k == 0)
    def _():
        for n in range(2, 4):
            for j in range(PAIRS):
                q3_copy(n, j, True).wait_send()

    give.wait_send()
    for i in range(COLS // CHUNK):
        item_copy(i).wait_send()
    for d in range(1, SPACE):
        for n in range(3):
            depth_copy(d, n, True).wait_send()
        for f in range(3):
            one_copy(f, lax.rem(s + d, SPACE), True).wait_send()

    @pl.loop(0, 16)
    def _(n):
        @pl.when((owner(s, 16 * k + n) != tm) & (chip < CHIPS - 1))
        def _():
            for f in range(3):
                two_copy(f, n).wait_send()

        each_halo(n, lambda x: x.wait_send())

    for n in range(2):
        middle_copy(n).wait_send()


    def spread(sp):
        cols = pl.ds(pl.multiple_of(sp * CHUNK, CHUNK), CHUNK)
        row = lax.broadcasted_iota(jnp.int32, (8, CHUNK), 0)
        x = vout[48:, cols]
        y = pltpu.roll(x, 4, 0)
        vh[0, :, cols] = jnp.where(row < 4, x, y)
        vh[1, :, cols] = jnp.where(row < 4, y, x)
        for kk in range(2):
            x = vob[:, side(sp, kk)]
            y = pltpu.roll(x, 4, 0)
            for t, z in enumerate((jnp.where(tile_row < 4, x, y), jnp.where(tile_row < 4, y, x))):
                vh[2, :, pl.ds(pl.multiple_of(512 * sp + 256 * kk + 128 * t, 128), 128)] = z

    def finish(sp):
        base = pl.multiple_of(sp * CHUNK, CHUNK)
        cols = pl.ds(base, CHUNK)
        d = wide(lambda c: drow[:, c], base)

        def stepped(state):
            h, u, w = state
            r = rates(h, u, w, d * u, d * w, left, right, up, down, lambda x: x)
            return [x + step_size * y for x, y in zip(state, r)]

        state = [
            wide(lambda c, f=f: jnp.concatenate([vout[16 * f : 16 * f + 16, c], vh[f, :, c]], axis=0), base) for f in range(3)
        ]
        a = stepped(state)
        b = stepped(a)
        for f in range(3):
            begin = inner(state[f])[:ROWS]
            ours = jnp.where(k == 0, boosted[f, :, cols], other[f, :, cols])
            y1 = ours + inner(a[f])[:ROWS]
            y2 = esum[f, :, cols] + inner(b[f])[:ROWS]
            start = jnp.where(k == 0, jnp.where(tm == 0, init[f, :, cols], begin), y1)
            end = jnp.where(k == 0, y1, y2)
            out[0, f, :, cols] = start
            out[1, f, :, cols] = partial[f, :, cols] + 0.5 * (start + end)
            out[2, f, :, cols] = end

    @pl.loop(1, SPACE)
    def _(d):
        sp = lax.rem(s + SPACE - d, SPACE)
        for c in row_copies(sp, False):
            c.wait_recv()
        for c in fin_copies(sp, True):
            c.start()
        for c in fin_copies(lax.rem(sp + 1, SPACE), False):
            c.wait_recv()
        spread(lax.rem(sp + 1, SPACE))

        @pl.when(d >= 3)
        def _():
            finish(lax.rem(sp + 2, SPACE))

    for c in fin_copies(lax.rem(s + 1, SPACE), False):
        c.wait_recv()
    spread(lax.rem(s + 1, SPACE))

    @pl.loop(0, 3)
    def _(i):
        finish(lax.rem(s + 2 * SPACE - 6 - i, SPACE))

    for d in range(1, SPACE):
        for c in row_copies(lax.rem(s + d, SPACE), True):
            c.wait_send()
    for sp in range(SPACE):
        for c in fin_copies(sp, True):
            c.wait_send()

    @pl.loop(1, 16)
    def _(n):
        @pl.when((chip != n) | (half != k))
        def _():
            ret_copy(n).wait_send()


VM = pl.BlockSpec(memory_space=pltpu.VMEM)


def per_device(fine_nodes, init_state, mean_depth):
    points = fine_nodes[0].reshape(9, ROWS, COLS)

    def vm(*shape):
        return pltpu.VMEM(shape, F32)

    def sems(*shape):
        return [pltpu.SemaphoreType.DMA(shape)] * 2

    flat, ringed = vm(3, ROWS, COLS), vm(3, RING, COLS)
    out = pl.pallas_call(
        coarse_kernel,
        out_shape=jax.ShapeDtypeStruct((3, 3, ROWS, COLS), F32),
        in_specs=[pl.BlockSpec(memory_space=pltpu.HBM)] * 3,
        out_specs=VM,
        scratch_shapes=[
            flat, flat, flat, flat, vm(56, COLS), vm(8, FOLD), vm(3, 8, COLS), vm(RING, COLS), vm(9, ROWS, COLS), flat, vm(ROWS, COLS),
            flat, flat, flat, vm(2, 8, FOLD), vm(2, 8, FOLD), vm(2, 8, FOLD), vm(2, 8, FOLD),
            ringed, ringed, flat, ringed, vm(2, 8, FOLD), vm(2, 8, FOLD), ringed, vm(4, 8, FOLD), vm(4, 8, FOLD),
            ringed, flat, flat, vm(2, 3, ROWS, COLS // 8), vm(2, 3, ROWS, COLS // 8), vm(2, 3, ROWS, COLS // 8),
            vm(3, 128, PART), vm(3, PART, 128), vm(128, 512), vm(512, 128),
            vm(CHIPS, 3, WIDE, 128), vm(CHIPS, 3, OWN, 128), vm(2, 3, OWN, 128), vm(3, PART, 128), vm(2, SPACE, 56, 128), vm(SPACE, 8, 128),
            pltpu.SemaphoreType.DMA((5,)), *sems(8), *sems(8), *sems(4, 4), *sems(2, 4), *sems(4, 4), *sems(8), *sems(1), *sems(3, 8), *sems(3, 8), *sems(3, 16),
            *sems(2, 16), *sems(16), *sems(3, 8), *sems(2, 8),
        ],
        compiler_params=pltpu.CompilerParams(collective_id=0, has_side_effects=True, vmem_limit_bytes=40 << 20),
        name="sweep",
    )(*(pltpu.with_memory_space_constraint(x, pltpu.HBM) for x in (points, init_state, mean_depth)))
    return out[None]


def solution(mesh):
    placed = (P("tm", None, None, "space", None), P(None, "space", None), P("space", None))
    return jax.shard_map(
        per_device,
        mesh=mesh,
        in_specs=placed,
        out_specs=P("tm", None, None, "space", None),
        check_vma=False,
    )
```

```python
import functools

import jax
import jax.numpy as jnp
from jax import lax
from jax.experimental import pallas as pl
from jax.experimental.pallas import tpu as pltpu
from jax.sharding import PartitionSpec as P

MESH = pl.DeviceIdType.MESH
F32 = jnp.float32

step_size = 0.3
viscosity = 1.0 / 3.0
coriolis = 0.5
quad_near = 5.0 / 24.0
quad_mid = 1.0 / 3.0
quad_far = -1.0 / 24.0
half_step = 0.5 * step_size
start_share = -(half_step + step_size / 3.0)
one_share = 2.0 * step_size / 3.0
two_share = half_step - step_size / 3.0

ROWS = 16
COLS = 4096
SPACE = 8
CHIPS = 16
PART = 256
OWN = 16
HALO = 16
MIDDLE = 7
WIDE = OWN + 2 * HALO


def rates(h, u, v, de, dn, left, right, up, down, centre):
    nh, nu, nv = viscosity * h, viscosity * u, viscosity * v
    he, hn, hh = 0.5 * de, 0.5 * dn, 0.5 * h
    nhc, nuc, nvc = centre(nh), centre(nu), centre(nv)
    hr = right(nh - he) + left(nh + he) + down(centre(nh - hn)) + up(centre(nh + hn)) - 4.0 * nhc
    ur = right(nu - hh) + left(nu + hh) + down(nuc) + up(nuc) - 4.0 * nuc + coriolis * centre(v)
    vr = right(nv) + left(nv) + down(centre(nv - hh)) + up(centre(nv + hh)) - 4.0 * nvc - coriolis * centre(u)
    return hr, ur, vr


CHUNK = 512
RING = 24


def edges(base):
    if isinstance(base, int):
        lo, hi = (base - 128) % COLS, (base + CHUNK) % COLS
    else:
        lo = pl.multiple_of(lax.rem(base + COLS - 128, COLS), 128)
        hi = pl.multiple_of(lax.rem(base + CHUNK, COLS), 128)
    return pl.ds(lo, 128), pl.ds(base, CHUNK), pl.ds(hi, 128)


def wide(get, base):
    return jnp.concatenate([get(c) for c in edges(base)], axis=1)


def right(x):
    return pltpu.roll(x, x.shape[1] - 1, 1)


def left(x):
    return pltpu.roll(x, 1, 1)


def down(x):
    return pltpu.roll(x, RING - 1, 0)


def up(x):
    return pltpu.roll(x, 1, 0)


def inner(x):
    return x[:, 128 : 128 + CHUNK]


def ring_rates(q, depth, base):
    h, u, v = (wide(lambda c, f=f: q[f, :, c], base) for f in range(3))
    d = wide(lambda c: depth[:, c], base)
    return rates(h, u, v, d * u, d * v, lambda x: inner(left(x)), lambda x: inner(right(x)), up, down, inner)


def chunks(body):
    @pl.loop(0, COLS // CHUNK)
    def _(i):
        body(pl.multiple_of(i * CHUNK, CHUNK))


PAIRS = COLS // CHUNK // 2
FOLD = COLS // 2


def pairs(body):
    @pl.loop(0, PAIRS)
    def _(j):
        base = pl.multiple_of(j * CHUNK, CHUNK)
        body(j, pl.ds(base, CHUNK), [base, pl.multiple_of(base + FOLD, CHUNK)])


def pair(body, j):
    base = j * CHUNK
    body(j, pl.ds(base, CHUNK), [base, base + FOLD])


def sub_roll(x, by):
    by %= 8
    return x if by == 0 else pltpu.roll(x, by, 0)


def pack(parts, at):
    row = lax.broadcasted_iota(jnp.int32, parts[0].shape, 0)
    tile = sub_roll(parts[0], -at)
    for i in range(1, len(parts)):
        tile = jnp.where(row >= 2 * i, sub_roll(parts[i], 2 * i - at), tile)
    return tile


def place(parts, at):
    row = lax.broadcasted_iota(jnp.int32, parts[0].shape, 0)
    tile = sub_roll(parts[0], -at[0])
    for i in range(1, len(parts)):
        tile = jnp.where(row >= i, sub_roll(parts[i], i - at[i]), tile)
    return tile


def fold(first, second):
    row = lax.broadcasted_iota(jnp.int32, first.shape, 0)
    return jnp.where(row < 4, first, sub_roll(second, 4))


def unfold(after, before, i):
    row = lax.broadcasted_iota(jnp.int32, after.shape, 0)
    return jnp.where(row < 4, sub_roll(after, -i), sub_roll(before, 7 - i))


def unpack(after, before, i):
    row = lax.broadcasted_iota(jnp.int32, after.shape, 0)
    return jnp.where(row < 4, sub_roll(after, -2 * i), sub_roll(before, 6 - 2 * i))


def snake(n):
    z, x = n // 4, lax.rem(n, 4)
    return z * 4 + jnp.where(lax.rem(z, 2) == 0, x, 3 - x)


def turned(s, chip):
    return chip // 4 * 4 + lax.rem(chip + 2 * lax.rem(s, 2), 4)


def owner(s, i):
    o = jnp.where(lax.rem(s, 2) == 0, i, 31 - i)
    return turned(s, snake(o // 2)) * 2 + lax.rem(o, 2)


def owned(s, tm):
    o = snake(turned(s, tm // 2)) * 2 + lax.rem(tm, 2)
    return jnp.where(lax.rem(s, 2) == 0, o, 31 - o)


def coarse_kernel(
    points_hbm, init_hbm, depth_hbm,
    out,
    boosted, other, esum, partial, vout, vob, vh, drow, points, init, depth, s0, a1, a2, ps, pr, fs, fr, s0r, q1, s1, q2, q2s, q2r, q3, q3s, q3r, br, item, ritem, relay_a, relay_b, relay_c,
    rt, et, dr, dt, ex, vx, middle, vt, vr, vb,
    in_sem, st_s, st_r, rl_s, rl_r, pk_s, pk_r, q2_ss, q2_rs, q3_ss, q3_rs, it_s, it_r, oth_s, oth_r, one_s, one_r, dep_s, dep_r, two_s, two_r,
    halo_s, halo_r, ret_s, ret_r, row_s, row_r, fin_s, fin_r,
):
    tm = lax.axis_index("tm")
    s = lax.axis_index("space")
    chip, k = tm // 2, lax.rem(tm, 2)
    mine = owned(s, tm)
    half, spot = mine // 16, lax.rem(mine, 16)
    s_next, s_prev = lax.rem(s + 1, SPACE), lax.rem(s + SPACE - 1, SPACE)
    tm_next, tm_prev = lax.rem(tm + 1, 32), lax.rem(tm + 31, 32)
    first = jnp.where(tm == 0, 1.0, 0.0).astype(F32)

    def at(t, sp):
        return {"tm": t, "space": sp}

    def near(step):
        p = lax.rem(32 * s + mine + step + 256, 256)
        return at(owner(p // 32, lax.rem(p, 32)), p // 32)

    partner = at(chip * 2 + 1 - k, s)
    nears = [near(1), near(-1)]

    loads = [pltpu.make_async_copy(points_hbm.at[3 * m : 3 * m + 3], points.at[3 * m : 3 * m + 3], in_sem.at[m]) for m in range(3)]
    loads += [pltpu.make_async_copy(init_hbm, init, in_sem.at[3]), pltpu.make_async_copy(depth_hbm, depth, in_sem.at[4])]
    for n in (2, 0, 1, 4, 3):
        loads[n].start()
    vt[...] = jnp.zeros_like(vt)
    barrier = pltpu.get_barrier_semaphore()
    z, x = tm // 8, lax.rem(tm // 2, 4)
    peers = [
        at(lax.rem(z + dz, 4) * 8 + lax.rem(x + dx, 4) * 2 + c, s)
        for dz in (2, 1, 3, 0) for dx in (2, 1, 3, 0) for c in range(2) if dz or dx
    ] + [partner]
    peers += [at(tm, lax.rem(s + d, SPACE)) for d in range(1, SPACE)]
    peers += [at(t, sp) for t in (tm_next, tm_prev) for sp in (s_next, s_prev)]
    peers += nears
    for p in peers:
        pl.semaphore_signal(barrier, inc=1, device_id=p, device_id_type=MESH)
    pl.semaphore_wait(barrier, len(peers))

    def copy(src, dst, ss, rs, dev):
        return pltpu.make_async_remote_copy(src_ref=src, dst_ref=dst, send_sem=ss, recv_sem=rs, device_id=dev, device_id_type=MESH)

    def block(sp, kk):
        return pl.ds(pl.multiple_of(512 * sp + 256 * kk, PART), PART)

    def rows(start, n=ROWS):
        return pl.ds(pl.multiple_of(start, 8), n)

    loads[2].wait()

    z_place = lax.rem(tm, 8)
    far_end = (z_place == 7) & (tm < 31)
    PIECE = COLS // 8
    direct = range(0, 2)
    routes = ((range(2, 4), relay_a, 6, 1), (range(4, 6), relay_b, 2, 5), (range(6, 8), relay_c, 4, 3))

    def piece(n):
        return pl.ds(PIECE * n, PIECE)

    def start_copy(n, to):
        return copy(points.at[6:9, :, piece(n)], s0.at[:, :, piece(n)], st_s.at[n], st_r.at[n], at(to, s))

    def via_copy(n, buffer, first_piece, to):
        return copy(points.at[6:9, :, piece(n)], buffer.at[n - first_piece], st_s.at[n], rl_r.at[n], at(to, s))

    def pass_copy(n, buffer, first_piece, ahead):
        return copy(buffer.at[n - first_piece], s0.at[:, :, piece(n)], rl_s.at[n], st_r.at[n], at(lax.rem(tm + ahead, 32), s))

    @pl.when((tm < 31) & (z_place != 7))
    def _():
        for n in (0, 4, 1, 5, 2, 6, 3, 7):
            start_copy(n, tm_next).start()

    @pl.when(far_end)
    def _():
        for ns, buffer, back, _ in routes:
            for n in ns:
                via_copy(n, buffer, ns[0], lax.rem(tm + 32 - back, 32)).start()

    for n in (0, 1, 4, 3):
        loads[n].wait()

    def pack_copy(n, j, send):
        up_down = lax.rem(s + (1 if (n % 2 == 0) == send else SPACE - 1), SPACE)
        slot = tm if n < 2 else (tm_next if send else tm_prev)
        cols = pl.ds(j * CHUNK, CHUNK) if isinstance(j, int) else pl.ds(pl.multiple_of(j * CHUNK, CHUNK), CHUNK)
        src, dst = (ps, pr) if n < 2 else (fs, fr)
        return copy(src.at[n % 2, :, cols], dst.at[n % 2, :, cols], pk_s.at[n, j], pk_r.at[n, j], at(slot, up_down))

    def prepare(j, folded, bases):
        tiles = [[], []], [[], []]
        for base in bases:
            cols = pl.ds(base, CHUNK)
            top, bottom = [], []
            for f in range(3):
                p0, p1, p2 = (points[3 * m + f, :, cols] for m in range(3))
                x = (step_size * quad_near - half_step) * p0 + (step_size * quad_mid) * p1 + (step_size * quad_far) * p2
                y = (step_size * quad_far) * p0 + (step_size * quad_mid - half_step) * p1 + (step_size * quad_near) * p2
                a1[f, :, cols] = x
                a2[f, :, cols] = y
                top.append(x[:8])
                bottom.append(x[8:])
            for n, (parts, tile, row, inside) in enumerate(((bottom, 8, 7, 6), (top, 0, 0, 1))):
                d = depth[tile : tile + 8, cols]
                ends = [
                    jnp.where(tm == 31, init[f, tile : tile + 8, cols], points[6 + f, tile : tile + 8, cols]) for f in range(3)
                ]
                tiles[0][n].append(place(parts + [d], [row] * 4))
                tiles[1][n].append(place(ends + [d], [row] * 3 + [inside]))
        for n in range(2):
            ps[n, :, folded] = fold(*tiles[0][n])
            fs[n, :, folded] = fold(*tiles[1][n])
        for n in range(2, 4):
            pack_copy(n, j, True).start()

    pairs(prepare)

    @pl.when(far_end)
    def _():
        for n in direct:
            start_copy(n, tm_next).start()

    for n in range(2):
        for j in range(PAIRS):
            pack_copy(n, j, True).start()

    for ns, buffer, back, spot_of in routes:
        @pl.when((z_place == spot_of) & (tm < 24))
        def _(ns=ns, buffer=buffer, back=back):
            for n in ns:
                via_copy(n, buffer, ns[0], lax.rem(tm + back, 32)).wait_recv()
                pass_copy(n, buffer, ns[0], back + 1).start()

    for n in range(4):
        for j in range(PAIRS):
            pack_copy(n, j, False).wait_recv()

    def ringed(j, folded, bases):
        row = lax.broadcasted_iota(jnp.int32, (8, CHUNK), 0)
        for h, base in enumerate(bases):
            cols = pl.ds(base, CHUNK)
            pa, pb, fa, fb = pr[1, :, folded], pr[0, :, folded], fr[1, :, folded], fr[0, :, folded]
            i = 4 * h + 3
            d = jnp.where(row < 4, sub_roll(fa, 1 - i), sub_roll(fb, 6 - i))
            d = jnp.where((row == 0) | (row == 7), unfold(pa, pb, i), d)
            drow[:, cols] = jnp.concatenate([depth[:, cols], d], axis=0)
            for f in range(3):
                main = jnp.where(tm == 0, init[f, :, cols], s0[f, :, cols])
                x = jnp.concatenate([main, unfold(fa, fb, 4 * h + f)], axis=0)
                y = jnp.concatenate([a1[f, :, cols], unfold(pa, pb, 4 * h + f)], axis=0)
                s0r[f, :, cols] = x
                q1[f, :, cols] = half_step * x + y

    def q2_copy(n, j, send):
        up_down = lax.rem(s + (1 if (n == 0) == send else SPACE - 1), SPACE)
        cols = pl.ds(j * CHUNK, CHUNK) if isinstance(j, int) else pl.ds(pl.multiple_of(j * CHUNK, CHUNK), CHUNK)
        return copy(q2s.at[n, :, cols], q2r.at[n, :, cols], q2_ss.at[n, j], q2_rs.at[n, j], at(tm, up_down))

    def one(j, folded, bases):
        tiles = [[], []]
        for base in bases:
            cols = pl.ds(base, CHUNK)
            r = ring_rates(q1, drow, base)
            q = []
            for f in range(3):
                x = s0r[f, :ROWS, cols] + r[f][:ROWS]
                s1[f, :, cols] = x
                q.append(half_step * x + a2[f, :, cols])
                q2[f, :ROWS, cols] = q[f]
            tiles[0].append(place([x[8:] for x in q], [7] * 3))
            tiles[1].append(place([x[:8] for x in q], [0] * 3))
        for n in range(2):
            q2s[n, :, folded] = fold(*tiles[n])
            q2_copy(n, j, True).start()

    for j in range(PAIRS):
        @pl.when(tm > 0)
        def _(j=j):
            start_copy(j, tm_prev).wait_recv()
            start_copy(j + PAIRS, tm_prev).wait_recv()

        pair(ringed, j)
        if j >= 2:
            pair(one, j - 1)
    pair(one, 3)
    pair(one, 0)

    def q3_copy(n, j, send):
        up_down = lax.rem(s + (1 if (n % 2 == 0) == send else SPACE - 1), SPACE)
        cols = pl.ds(j * CHUNK, CHUNK) if isinstance(j, int) else pl.ds(pl.multiple_of(j * CHUNK, CHUNK), CHUNK)
        return copy(q3s.at[n, :, cols], q3r.at[n, :, cols], q3_ss.at[n, j], q3_rs.at[n, j], at(tm, up_down))

    def two(j, folded, bases):
        for n in range(2):
            q2_copy(n, j, False).wait_recv()
        tiles = [[], [], [], []]
        for h, base in enumerate(bases):
            cols = pl.ds(base, CHUNK)
            for f in range(3):
                q2[f, ROWS:, cols] = unfold(q2r[1, :, folded], q2r[0, :, folded], 4 * h + f)
            r = ring_rates(q2, drow, base)
            top, bottom = [], []
            for f in range(3):
                x, y = s0r[f, :ROWS, cols], s1[f, :, cols]
                z = y + r[f][:ROWS]
                partial[f, :, cols] = y - 0.5 * (x + z)
                q = (step_size * first + start_share) * x + one_share * y + two_share * z
                q3[f, :ROWS, cols] = q
                top.append(q[:8])
                bottom.append(q[8:])
            for n, (parts, row) in enumerate(((bottom, 7), (top, 0), (bottom, 6), (top, 1))):
                tiles[n].append(place(parts, [row] * 3))
        for n in range(4):
            q3s[n, :, folded] = fold(*tiles[n])
        for n in range(2):
            q3_copy(n, j, True).start()

        @pl.when(k == 0)
        def _():
            for n in range(2, 4):
                q3_copy(n, j, True).start()

    for j in (1, 2, 3, 0):
        pair(two, j)

    def q3_rows(j, folded, bases):
        for n in range(2):
            q3_copy(n, j, False).wait_recv()

        @pl.when(k == 0)
        def _():
            for n in range(2, 4):
                q3_copy(n, j, False).wait_recv()

        row = lax.broadcasted_iota(jnp.int32, (8, CHUNK), 0)
        for h, base in enumerate(bases):
            for f in range(3):
                i = 4 * h + f
                near_rows = unfold(q3r[1, :, folded], q3r[0, :, folded], i)
                far_rows = jnp.where(row < 4, sub_roll(q3r[3, :, folded], 1 - i), sub_roll(q3r[2, :, folded], 6 - i))
                q3[f, ROWS:, pl.ds(base, CHUNK)] = jnp.where((row == 0) | (row == 7), near_rows, far_rows)

    def three(j, folded, bases):
        for base in bases:
            cols = pl.ds(base, CHUNK)
            r = ring_rates(q3, drow, base)
            for f in range(3):
                x = r[f] + first * s0r[f, :, cols]
                br[f, :, cols] = x
                boosted[f, :, cols] = x[:ROWS]

    pair(q3_rows, 1)
    pair(q3_rows, 2)
    pair(q3_rows, 3)
    pair(three, 2)
    pair(q3_rows, 0)
    for j in (3, 0, 1):
        pair(three, j)
    give = copy(boosted, other, oth_s.at[0], oth_r.at[0], partner)

    def item_copy(i):
        cols = pl.ds(pl.multiple_of(i * CHUNK, CHUNK), CHUNK)
        return copy(item.at[:, :, cols], ritem.at[:, :, cols], it_s.at[i], it_r.at[i], partner)

    @pl.loop(0, COLS // CHUNK)
    def _(i):
        base = pl.multiple_of(i * CHUNK, CHUNK)
        cols = pl.ds(base, CHUNK)
        r = ring_rates(br, drow, base)
        for f in range(3):
            item[f, :, cols] = jnp.where(k == 0, boosted[f, :, cols] + step_size * r[f][:ROWS], boosted[f, :, cols])
        item_copy(i).start()

    give.start()

    def one_copy(f, sp, send):
        to, by = (sp, s) if send else (s, sp)
        n = to if send else by
        return copy(esum.at[f, :, block(to, k)], rt.at[f, rows(ROWS * by), :], one_s.at[f, n], one_r.at[f, by], at(tm, sp))

    @pl.loop(0, COLS // CHUNK)
    def _(i):
        item_copy(i).wait_recv()
        cols = pl.ds(pl.multiple_of(i * CHUNK, CHUNK), CHUNK)
        for f in range(3):
            esum[f, :, cols] = item[f, :, cols] + ritem[f, :, cols]

    for f in range(3):
        for d in range(1, SPACE):
            one_copy(f, lax.rem(s + d, SPACE), True).start()
    rt[:, rows(ROWS * s), :] = esum[:, :, block(s, k)]

    def depth_pieces(sp):
        i = owned(sp, tm)
        tile = 4 * sp + 2 * (i // 16) + lax.rem(i, 16) // 8 + jnp.where(lax.rem(i, 8) == 0, -1, 0)
        return [(pl.ds(pl.multiple_of(lax.rem(tile + 32 + n, 32) * 128, 128), 128), pl.ds(128 * n, 128)) for n in range(2)]

    def depth_copy(d, n, send):
        sp = lax.rem(s + d, SPACE) if send else lax.rem(s + SPACE - d, SPACE)
        to = sp if send else s
        src, dst = depth_pieces(to)[n]
        return copy(depth.at[:, src], dr.at[rows(ROWS * (s if send else sp)), dst], dep_s.at[n, d], dep_r.at[n, d], at(tm, sp))

    for d in range(1, SPACE):
        for n in range(2):
            depth_copy(d, n, True).start()
    for src, dst in depth_pieces(s):
        dr[rows(ROWS * s), dst] = depth[:, src]


    def two_copy(f, n):
        src, dst = et.at[f, rows(OWN * n, OWN), :], ex.at[chip, f, pl.ds(HALO, OWN), :]
        return copy(src, dst, two_s.at[f, n], two_r.at[f, chip], at(owner(s, 16 * k + n), s))

    for f in range(3):
        for d in range(1, SPACE):
            one_copy(f, lax.rem(s + SPACE - d, SPACE), False).wait_recv()
        for t in range(2):
            et[f, 128 * t : 128 * t + 128, :] = rt[f, :, 128 * t : 128 * t + 128].T

        @pl.loop(0, 16)
        def _(m, f=f):
            n = lax.rem(m + spot, 16)

            @pl.when((owner(s, 16 * k + n) != tm) & (chip < CHIPS - 1))
            def _():
                two_copy(f, n).start()

    @pl.when(half == k)
    def _():
        ex[chip, :, HALO : HALO + OWN, :] = et[:, rows(OWN * spot, OWN), :]

    spans = ((0, 2, 16), (2, 6, 8), (7, 10, 16), (10, 14, 8))

    def halo_copy(n, j, width):
        src, dst = (HALO + OWN - width, HALO - width) if n == 0 else (HALO, HALO + OWN)
        return copy(ex.at[j, :, pl.ds(src, width), :], ex.at[j, :, pl.ds(dst, width), :], halo_s.at[n, j], halo_r.at[n, j], nears[n])

    def middle_copy(n):
        return copy(vx.at[MIDDLE], middle.at[n], halo_s.at[n, 15], halo_r.at[n, 15], nears[n])

    def each_halo(j, act):
        for lo, hi, width in spans:
            @pl.when((j >= lo) & (j < hi))
            def _():
                for n in range(2):
                    act(halo_copy(n, j, width))

    for c in (0, 1, 2, 3, 4, 5, 6, 7, 8, 9, 10, 11, 12, 13, 14):
        @pl.when((chip != c) | (half != k))
        def _(c=c):
            for f in range(3):
                src, dst = et.at[f, rows(OWN * spot, OWN), :], ex.at[c, f, pl.ds(HALO, OWN), :]
                copy(src, dst, two_s.at[f, 0], two_r.at[f, c], at(c * 2 + half, s)).wait_recv()

        for lo, hi, width in spans:
            if lo <= c < hi:
                for n in range(2):
                    halo_copy(n, c, width).start()

    for d in range(1, SPACE):
        for n in range(2):
            depth_copy(d, n, False).wait_recv()
    for t in range(2):
        dt[128 * t : 128 * t + 128, :] = dr[:, 128 * t : 128 * t + 128].T


    def scanned(lo, hi, halo, state, send):
        count = OWN + 2 * halo
        d_own = dt[rows(jnp.where(lax.rem(spot, 8) == 0, 128, OWN * lax.rem(spot, 8)) - halo, count), :]

        def stepped(state):
            h, u, v = state
            r = rates(
                h, u, v, d_own * u, d_own * v,
                lambda x: pltpu.roll(x, 1, 0), lambda x: pltpu.roll(x, count - 1, 0),
                lambda x: pltpu.roll(x, 1, 1), lambda x: pltpu.roll(x, 127, 1), lambda x: x,
            )
            return tuple(x + step_size * y for x, y in zip(state, r))

        def body(j, state):
            state = stepped(stepped(state))
            each_halo(j, lambda x: x.wait_recv())
            state = tuple(x + ex[j, f, HALO - halo : HALO + OWN + halo] for f, x in enumerate(state))
            for f in range(3):
                vx[j + 1, f] = state[f][halo : halo + OWN]

            if send:
                give_back(j + 1)
            return state

        return lax.fori_loop(lo, hi, body, state)

    def give_back(j):
        @pl.when((chip != j) | (half != k))
        def _():
            ret_copy(j).start()

    def ret_copy(j):
        return copy(vx.at[j], vt.at[:, rows(OWN * spot, OWN), :], ret_s.at[j], ret_r.at[spot], at(j * 2 + half, s))

    state = scanned(0, MIDDLE, HALO, (jnp.zeros((WIDE, 128), F32),) * 3, False)
    for n in range(2):
        middle_copy(n).start()

    @pl.loop(0, MIDDLE)
    def _(i):
        give_back(1 + lax.rem(chip + i, MIDDLE))

    for n in range(2):
        middle_copy(n).wait_recv()
    state = tuple(jnp.concatenate([middle[0, f], x[HALO : HALO + OWN], middle[1, f]], axis=0) for f, x in enumerate(state))
    state = scanned(MIDDLE, 11, HALO, state, True)
    scanned(11, CHIPS - 1, 8, tuple(x[8:40] for x in state), True)

    @pl.when((chip > 0) & (half == k))
    def _():
        vt[:, rows(OWN * spot, OWN), :] = vx[chip]

    tile_row = lax.broadcasted_iota(jnp.int32, (8, 128), 0)
    def around(x, sp):
        a, b = (16 * sp + 16) % 128, (16 * sp + 120) % 128
        return jnp.where(tile_row < 2, x[a : a + 8], pltpu.roll(x[b : b + 8], 4, 0))

    def stack(x, y):
        return jnp.where(tile_row < 4, x, pltpu.roll(y, 4, 0))

    def half_block(sp, t):
        return pl.ds(pl.multiple_of(512 * sp + 256 * k + 128 * t, 128), 128)

    def side(sp, kk):
        return pl.ds(pl.multiple_of(256 * sp + 128 * kk, 128), 128)

    def row_copies(sp, send):
        to, by = (sp, s) if send else (s, sp)
        return (
            *(copy(vr.at[t, to], vout.at[:, half_block(by, t)], row_s.at[t, sp], row_r.at[t, by], at(tm, sp)) for t in range(2)),
            copy(vb.at[to], vob.at[:, side(by, k)], row_s.at[2, sp], row_r.at[2, by], at(tm, sp)),
        )

    def fin_copies(sp, send):
        kk = k if send else 1 - k
        cols, beside = block(sp, kk), side(sp, kk)
        return (
            copy(vout.at[:, cols], vout.at[:, cols], fin_s.at[0, sp], fin_r.at[0, sp], partner),
            copy(vob.at[:, beside], vob.at[:, beside], fin_s.at[1, sp], fin_r.at[1, sp], partner),
        )

    for t in range(2):
        @pl.when(chip > 0)
        def _(t=t):
            @pl.loop(8 * t, 8 * t + 8)
            def _(n):
                frm = owner(s, 16 * k + n)

                @pl.when(frm != tm)
                def _():
                    copy(vx.at[0], vt.at[:, rows(OWN * n, OWN), :], ret_s.at[0], ret_r.at[n], at(frm, s)).wait_recv()

        xs = [vt[f, 128 * t : 128 * t + 128, :].T for f in range(3)]
        for sp in range(SPACE):
            for f in range(3):
                vr[t, sp, 16 * f : 16 * f + 16, :] = xs[f][16 * sp : 16 * sp + 16]
            vr[t, sp, 48:, :] = stack(around(xs[0], sp), around(xs[1], sp))
        if t == 1:
            other_half = vt[2, :128, :].T
            for sp in range(SPACE):
                vb[sp] = stack(around(other_half, sp), around(xs[2], sp))
        for d in range(1, SPACE):
            for c in row_copies(lax.rem(s + d, SPACE), True)[t : 1 if t == 0 else 3]:
                c.start()
        vout[:, half_block(s, t)] = vr[t, s]
    vob[:, side(s, k)] = vb[s]
    for c in fin_copies(s, True):
        c.start()
    give.wait_recv()

    @pl.when(tm < 31)
    def _():
        for n in range(8):
            start_copy(n, tm_next).wait_send()

    for ns, buffer, back, spot_of in routes:
        @pl.when((z_place == spot_of) & (tm < 24))
        def _(ns=ns, buffer=buffer, back=back):
            for n in ns:
                pass_copy(n, buffer, ns[0], back + 1).wait_send()

    for n in range(4):
        for j in range(PAIRS):
            pack_copy(n, j, True).wait_send()
    for n in range(2):
        for j in range(PAIRS):
            q2_copy(n, j, True).wait_send()
            q3_copy(n, j, True).wait_send()

    @pl.when(k == 0)
    def _():
        for n in range(2, 4):
            for j in range(PAIRS):
                q3_copy(n, j, True).wait_send()

    give.wait_send()
    for i in range(COLS // CHUNK):
        item_copy(i).wait_send()
    for d in range(1, SPACE):
        for n in range(2):
            depth_copy(d, n, True).wait_send()
        for f in range(3):
            one_copy(f, lax.rem(s + d, SPACE), True).wait_send()

    @pl.loop(0, 16)
    def _(n):
        @pl.when((owner(s, 16 * k + n) != tm) & (chip < CHIPS - 1))
        def _():
            for f in range(3):
                two_copy(f, n).wait_send()

        each_halo(n, lambda x: x.wait_send())

    for n in range(2):
        middle_copy(n).wait_send()


    def spread(sp):
        cols = pl.ds(pl.multiple_of(sp * CHUNK, CHUNK), CHUNK)
        row = lax.broadcasted_iota(jnp.int32, (8, CHUNK), 0)
        x = vout[48:, cols]
        y = pltpu.roll(x, 4, 0)
        vh[0, :, cols] = jnp.where(row < 4, x, y)
        vh[1, :, cols] = jnp.where(row < 4, y, x)
        for kk in range(2):
            x = vob[:, side(sp, kk)]
            y = pltpu.roll(x, 4, 0)
            for t, z in enumerate((jnp.where(tile_row < 4, x, y), jnp.where(tile_row < 4, y, x))):
                vh[2, :, pl.ds(pl.multiple_of(512 * sp + 256 * kk + 128 * t, 128), 128)] = z

    def finish(sp):
        base = pl.multiple_of(sp * CHUNK, CHUNK)
        cols = pl.ds(base, CHUNK)
        d = wide(lambda c: drow[:, c], base)

        def stepped(state):
            h, u, w = state
            r = rates(h, u, w, d * u, d * w, left, right, up, down, lambda x: x)
            return [x + step_size * y for x, y in zip(state, r)]

        state = [
            wide(lambda c, f=f: jnp.concatenate([vout[16 * f : 16 * f + 16, c], vh[f, :, c]], axis=0), base) for f in range(3)
        ]
        a = stepped(state)
        b = stepped(a)
        for f in range(3):
            begin = inner(state[f])[:ROWS]
            ours = jnp.where(k == 0, boosted[f, :, cols], other[f, :, cols])
            y1 = ours + inner(a[f])[:ROWS]
            y2 = esum[f, :, cols] + inner(b[f])[:ROWS]
            start = jnp.where(k == 0, jnp.where(tm == 0, init[f, :, cols], begin), y1)
            end = jnp.where(k == 0, y1, y2)
            out[0, f, :, cols] = start
            out[1, f, :, cols] = partial[f, :, cols] + 0.5 * (start + end)
            out[2, f, :, cols] = end

    @pl.loop(1, SPACE)
    def _(d):
        sp = lax.rem(s + SPACE - d, SPACE)
        for c in row_copies(sp, False):
            c.wait_recv()
        for c in fin_copies(sp, True):
            c.start()
        for c in fin_copies(lax.rem(sp + 1, SPACE), False):
            c.wait_recv()
        spread(lax.rem(sp + 1, SPACE))

        @pl.when(d >= 3)
        def _():
            finish(lax.rem(sp + 2, SPACE))

    for c in fin_copies(lax.rem(s + 1, SPACE), False):
        c.wait_recv()
    spread(lax.rem(s + 1, SPACE))

    @pl.loop(0, 3)
    def _(i):
        finish(lax.rem(s + 2 * SPACE - 6 - i, SPACE))

    for d in range(1, SPACE):
        for c in row_copies(lax.rem(s + d, SPACE), True):
            c.wait_send()
    for sp in range(SPACE):
        for c in fin_copies(sp, True):
            c.wait_send()

    @pl.loop(1, 16)
    def _(n):
        @pl.when((chip != n) | (half != k))
        def _():
            ret_copy(n).wait_send()


VM = pl.BlockSpec(memory_space=pltpu.VMEM)


def per_device(fine_nodes, init_state, mean_depth):
    points = fine_nodes[0].reshape(9, ROWS, COLS)

    def vm(*shape):
        return pltpu.VMEM(shape, F32)

    def sems(*shape):
        return [pltpu.SemaphoreType.DMA(shape)] * 2

    flat, ringed = vm(3, ROWS, COLS), vm(3, RING, COLS)
    out = pl.pallas_call(
        coarse_kernel,
        out_shape=jax.ShapeDtypeStruct((3, 3, ROWS, COLS), F32),
        in_specs=[pl.BlockSpec(memory_space=pltpu.HBM)] * 3,
        out_specs=VM,
        scratch_shapes=[
            flat, flat, flat, flat, vm(56, COLS), vm(8, FOLD), vm(3, 8, COLS), vm(RING, COLS), vm(9, ROWS, COLS), flat, vm(ROWS, COLS),
            flat, flat, flat, vm(2, 8, FOLD), vm(2, 8, FOLD), vm(2, 8, FOLD), vm(2, 8, FOLD),
            ringed, ringed, flat, ringed, vm(2, 8, FOLD), vm(2, 8, FOLD), ringed, vm(4, 8, FOLD), vm(4, 8, FOLD),
            ringed, flat, flat, vm(2, 3, ROWS, COLS // 8), vm(2, 3, ROWS, COLS // 8), vm(2, 3, ROWS, COLS // 8),
            vm(3, 128, PART), vm(3, PART, 128), vm(128, 256), vm(256, 128),
            vm(CHIPS, 3, WIDE, 128), vm(CHIPS, 3, OWN, 128), vm(2, 3, OWN, 128), vm(3, PART, 128), vm(2, SPACE, 56, 128), vm(SPACE, 8, 128),
            pltpu.SemaphoreType.DMA((5,)), *sems(8), *sems(8), *sems(4, 4), *sems(2, 4), *sems(4, 4), *sems(8), *sems(1), *sems(3, 8), *sems(3, 8), *sems(3, 16),
            *sems(2, 16), *sems(16), *sems(3, 8), *sems(2, 8),
        ],
        compiler_params=pltpu.CompilerParams(collective_id=0, has_side_effects=True, vmem_limit_bytes=40 << 20),
        name="sweep",
    )(*(pltpu.with_memory_space_constraint(x, pltpu.HBM) for x in (points, init_state, mean_depth)))
    return out[None]


def solution(mesh):
    placed = (P("tm", None, None, "space", None), P(None, "space", None), P("space", None))
    return jax.shard_map(
        per_device,
        mesh=mesh,
        in_specs=placed,
        out_specs=P("tm", None, None, "space", None),
        check_vma=False,
    )
```
